32 devices in a mesh: dp: 8 (over y, x, core), mp: 4 (over z).
Axes of the slice: x: 2, y: 2, z: 4, core: 2. Of those that a mesh axis runs over, the one named last changes fastest.
Arguments:
- frames: bfloat16 [24576, 768], P(('dp', 'mp')), may hold values from -6 to 6
- w_qkv: bfloat16 [3, 768, 768], P(None, 'dp', 'mp'), may hold values from -0.21875 to 0.21875
- b_qv: bfloat16 [2, 768], P(None, ('mp', 'dp')), may hold values from -1.5 to 1.5
- w_out: bfloat16 [768, 768], P('mp', 'dp'), may hold values from -4 to 4
- b_out: float32 [768], P(('dp', 'mp')), may hold values from -1.5 to 1.5
- ln1_gain: float32 [768], P(('dp', 'mp')), may hold values from 0.5 to 1.5
- ln1_bias: float32 [768], P(('dp', 'mp')), may hold values from -1.5 to 1.5
- w_ff1: bfloat16 [768, 3072], P('dp', 'mp'), may hold values from -0.21875 to 0.21875
- b_ff1: bfloat16 [3072], P(('mp', 'dp')), may hold values from -1.5 to 1.5
- w_ff2: bfloat16 [3072, 768], P('mp', 'dp'), may hold values from -0.109375 to 0.109375
- b_ff2: float32 [768], P(('dp', 'mp')), may hold values from -1.5 to 1.5
- ln2_gain: float32 [768], P(('dp', 'mp')), may hold values from 0.5 to 1.5
- ln2_bias: float32 [768], P(('dp', 'mp')), may hold values from -1.5 to 1.5
- cotangent: bfloat16 [24576, 768], P(('dp', 'mp')), may hold values from -6 to 6
- clip_lengths: int32 [16], replicated, may hold values from 384 to 1536, as said below
- clip_slot: int32 [16], replicated, may hold values from 0 to 15, each once
Outputs:
- layer_out: bfloat16 [24576, 768], P(('dp', 'mp'))
- grad_frames: float32 [24576, 768], P(('dp', 'mp'))
- grad_w_qkv: float32 [3, 768, 768], P(None, 'dp', 'mp')
- grad_b_qv: float32 [2, 768], P(None, ('mp', 'dp'))
- grad_w_out: float32 [768, 768], P('mp', 'dp')
- grad_b_out: float32 [768], P(('dp', 'mp'))
- grad_ln1_gain: float32 [768], P(('dp', 'mp'))
- grad_ln1_bias: float32 [768], P(('dp', 'mp'))
- grad_w_ff1: float32 [768, 3072], P('dp', 'mp')
- grad_b_ff1: float32 [3072], P(('mp', 'dp'))
- grad_w_ff2: float32 [3072, 768], P('mp', 'dp')
- grad_b_ff2: float32 [768], P(('dp', 'mp'))
- grad_ln2_gain: float32 [768], P(('dp', 'mp'))
- grad_ln2_bias: float32 [768], P(('dp', 'mp'))
The draws below stay inside these ranges and needn't reach their ends.
Inputs may be any that keep to these rules, and one draw needn't show every extreme that they name: `clip_lengths`: frames of each clip; the longest clips fill a whole slot of 1536. A permutation: clip c fills slot clip_slot[c].
All inputs are finite; a program needn't handle non-finite values.
Results may differ from the reference program's by a relative error of at most 0.02.
Values may be sent and summed in bfloat16 or wider, within the bound.
A program may use at most 192 MiB of HBM per device.

```python
import jax
import jax.numpy as jnp
from jax import lax

D = 768
HEAD = 64
FF = 3072
SLOT = 1536
NCLIPS = 16
TOKENS = 24576
N_MP = 4


def draw_clip_lengths(key, part):
    short_key = jax.random.fold_in(key, 11)
    order_key = jax.random.fold_in(key, 12)
    short = jax.random.randint(short_key, (NCLIPS,), SLOT // 4, 3 * SLOT // 4)
    order = jax.random.permutation(order_key, NCLIPS)
    return jnp.where(order < max(1, NCLIPS // 8), SLOT, short).astype(jnp.int32)


def with_spikes(drawn, stream_key, source, target, shards_of, factor):
    owner, partner = [(jnp.arange(drawn.shape[position]) // (drawn.shape[position] // shards_of)).reshape([-1 if axis == position else 1 for axis in range(drawn.ndim)]) for position in (source, target)]
    chosen = jax.random.permutation(stream_key, shards_of)[partner]
    strong = (owner == chosen) | (owner == (partner + shards_of // 2) % shards_of)
    return jnp.where(strong, factor * drawn, drawn)


def levels(key, shape, cuts, smallest, high):
    level, own = 1.0, jax.random.fold_in(key, 6)
    for position, parts in cuts:
        steps = jnp.exp(jax.random.uniform(jax.random.fold_in(own, position), (parts,), jnp.float32, smallest / len(cuts), high / len(cuts)))
        level = level * jnp.repeat(steps, shape[position] // parts).reshape([-1 if axis == position else 1 for axis in range(len(shape))])
    return level


def normal_values(key, dims, deviation, most, pieces=(), kind=jnp.bfloat16):
    level = levels(key, dims, pieces, -0.22, 0.18) if pieces else 1.0
    drawn = jax.random.normal(key, dims, jnp.float32) * deviation * level
    return jnp.minimum(jnp.maximum(drawn, -most), most).astype(kind)


def bell_draw_with(rng, extent, width, most, cuts, heavy, kind=jnp.bfloat16):
    drawn = width * jax.random.normal(rng, extent, jnp.float32)
    if cuts:
        drawn = drawn * levels(rng, extent, cuts, -0.22, 0.18)
    return jnp.clip(with_spikes(drawn, jax.random.fold_in(rng, 3), *heavy), -most, most).astype(kind)


def setup_inputs(seed: int = 0) -> dict:
    key_of = jax.random.split(jax.random.key(seed), 17)
    return {
        "frames": bell_draw_with(key_of[0], (TOKENS, D), 1.0, 6.0, ((0, 32),), (0, 1, 32, 2.75)),
        "w_qkv": normal_values(key_of[1], (3, D, D), D ** -0.5, 0.21875, ((1, 8), (2, 4))),
        "b_qv": normal_values(key_of[2], (2, D), 0.3, 1.5, ((1, 32),)),
        "w_out": normal_values(key_of[3], (D, D), (4 * D // SLOT) ** -0.5, 4.0, ((0, 4), (1, 8))),
        "b_out": normal_values(key_of[4], (D,), 0.3, 1.5, ((0, 32),), jnp.float32),
        "ln1_gain": jnp.clip(1.0 + 0.1 * jax.random.normal(key_of[5], (D,), jnp.float32), 0.5, 1.5),
        "ln1_bias": normal_values(key_of[6], (D,), 0.3, 1.5, ((0, 32),), jnp.float32),
        "w_ff1": normal_values(key_of[7], (D, FF), D ** -0.5, 0.21875, ((0, 8), (1, 4))),
        "b_ff1": normal_values(key_of[8], (FF,), 0.3, 1.5, ((0, 32),)),
        "w_ff2": normal_values(key_of[9], (FF, D), FF ** -0.5, 0.109375, ((0, 4), (1, 8))),
        "b_ff2": normal_values(key_of[10], (D,), 0.3, 1.5, ((0, 32),), jnp.float32),
        "ln2_gain": jnp.clip(1.0 + 0.1 * jax.random.normal(key_of[11], (D,), jnp.float32), 0.5, 1.5),
        "ln2_bias": normal_values(key_of[12], (D,), 0.3, 1.5, ((0, 32),), jnp.float32),
        "cotangent": bell_draw_with(key_of[13], (TOKENS, D), 1.0, 6.0, ((0, 32),), (0, 1, 32, 2.75)),
        "clip_lengths": draw_clip_lengths(jax.random.fold_in(key_of[16], 71), 0),
        "clip_slot": jax.random.permutation(key_of[15], NCLIPS).astype(jnp.int32),
    }


EPS = 1e-05

@jax.custom_vjp
def low(v):
    return lax.optimization_barrier(v.astype(jnp.bfloat16)).astype(jnp.float32)

@jax.custom_vjp
def low_back(v):
    return v

def low_keep(v):
    return (low(v), None)

def low_pass(kept, grad):
    return (grad,)

def back_keep(v):
    return (v, None)

def back_low(kept, grad):
    return (low(grad),)
low.defvjp(low_keep, low_pass)
low_back.defvjp(back_keep, back_low)

def product(left, right):
    return jnp.dot(left, right, precision=lax.Precision.HIGHEST, preferred_element_type=jnp.float32)

def normalize(field, gain, shift):
    mean = lax.optimization_barrier(jnp.mean(field, axis=-1, keepdims=True))
    centred = field - mean
    spread = lax.optimization_barrier(jnp.mean(centred * centred, axis=-1, keepdims=True))
    return centred * lax.rsqrt(spread + EPS) * gain + shift

def attend(query, keys, values, slot_length):
    heads = query.shape[1] // HEAD
    shape = (-1, SLOT, heads, HEAD)

    def one_slot(items):
        query_slot, keys_slot, values_slot, length = items
        scores = jnp.einsum('qhd,khd->hqk', query_slot, keys_slot, precision=lax.Precision.HIGHEST) * 0.125
        scores = low_back(scores)
        valid = jnp.arange(SLOT) < length
        scores = jnp.where(valid[None, None, :], scores, -1e+30)
        peak = lax.optimization_barrier(jnp.max(scores, axis=-1, keepdims=True))
        exps = jnp.exp(scores - peak)
        weights = low(exps / lax.optimization_barrier(jnp.sum(exps, axis=-1, keepdims=True)))
        context = jnp.einsum('hqk,khd->qhd', weights, values_slot, precision=lax.Precision.HIGHEST)
        return low_back(low(context))
    result = lax.map(jax.checkpoint(one_slot), (query.reshape(shape), keys.reshape(shape), values.reshape(shape), slot_length))
    return result.reshape(-1, heads * HEAD)

def layer(frames, w_qkv, b_qv, w_out, b_out, ln1_gain, ln1_bias, w_ff1, b_ff1, w_ff2, b_ff2, ln2_gain, ln2_bias, slot_length):
    head_width = D // N_MP
    unit_width = FF // N_MP
    branch_one = jnp.zeros(frames.shape, jnp.float32)
    for member in range(N_MP):
        first = member * head_width
        last = first + head_width
        frames_member = low_back(frames)
        query = low_back(low(product(frames_member, w_qkv[0][:, first:last]) + b_qv[0, first:last]))
        keys = low_back(low(product(frames_member, w_qkv[1][:, first:last])))
        values = low_back(low(product(frames_member, w_qkv[2][:, first:last]) + b_qv[1, first:last]))
        context = attend(query, keys, values, slot_length)
        branch_one = branch_one + low(product(context, w_out[first:last, :]))
    pre_one = low_back(branch_one) + b_out + frames
    middle = normalize(pre_one, ln1_gain, ln1_bias)
    middle_low = low(middle)
    branch_two = jnp.zeros(frames.shape, jnp.float32)
    for member in range(N_MP):
        first = member * unit_width
        last = first + unit_width
        middle_member = low_back(middle_low)
        hidden = low_back(product(middle_member, w_ff1[:, first:last]) + b_ff1[first:last])
        active = low(jax.nn.gelu(hidden, approximate=False))
        branch_two = branch_two + low(product(active, w_ff2[first:last, :]))
    pre_two = low_back(branch_two) + b_ff2 + middle
    return normalize(pre_two, ln2_gain, ln2_bias)

def reference(frames, w_qkv, b_qv, w_out, b_out, ln1_gain, ln1_bias, w_ff1, b_ff1, w_ff2, b_ff2, ln2_gain, ln2_bias, cotangent, clip_lengths, clip_slot):
    slot_ids = jnp.arange(NCLIPS).astype(jnp.int32)
    slot_length = lax.optimization_barrier(jnp.sum(jnp.where(clip_slot[None, :] == slot_ids[:, None], clip_lengths[None, :], 0), axis=1)).astype(jnp.int32)
    params = (frames, w_qkv, b_qv, w_out, b_out, ln1_gain, ln1_bias, w_ff1, b_ff1, w_ff2, b_ff2, ln2_gain, ln2_bias)
    params = tuple((item.astype(jnp.float32) for item in params))

    def forward(*values):
        return layer(*values, slot_length)
    output, pullback = jax.vjp(forward, *params)
    grads = pullback(cotangent.astype(jnp.float32))
    return (output.astype(jnp.bfloat16), grads[0], grads[1], grads[2], grads[3], grads[4], grads[5], grads[6], grads[7], grads[8], grads[9], grads[10], grads[11], grads[12])
```

```python
import functools

import jax
import jax.numpy as jnp
from jax import lax
from jax.experimental import pallas as pl
from jax.experimental.pallas import tpu as pltpu
from jax.sharding import PartitionSpec as P

HEAD = 64
SLOT = 1536
EPS = 1e-05
SCALE = 0.125
MASKED = -1e30
BOTH = ("dp", "mp")
F32 = jnp.float32
BF16 = jnp.bfloat16
NN = (((1,), (0,)), ((), ()))
NT = (((1,), (1,)), ((), ()))


def mul(left, right, dims=NN):
    return lax.dot_general(left, right, dims, preferred_element_type=F32)


def lanes(shape):
    return lax.broadcasted_iota(jnp.int32, shape, 1)


def three_parts(value):
    high = value.astype(BF16).astype(F32)
    rest = value - high
    middle = rest.astype(BF16).astype(F32)
    return high, middle, rest - middle


def head_block(value, place):
    block = value[:, 128 * (place // 2) : 128 * (place // 2) + 128]
    return pltpu.roll(block, HEAD, 1) if place % 2 else block


def pair(low, high):
    return jnp.where(lanes(low.shape) < HEAD, low, pltpu.roll(high, HEAD, 1))


def norm_parts(field):
    mean = jnp.mean(field, axis=-1, keepdims=True)
    centred = field - mean
    spread = jnp.mean(centred * centred, axis=-1, keepdims=True)
    inverse = lax.rsqrt(spread + EPS)
    return centred * inverse, inverse


def norm_back(grad, scaled, inverse, gain):
    inner = grad * gain
    return inverse * (
        inner
        - jnp.mean(inner, axis=-1, keepdims=True)
        - scaled * jnp.mean(inner * scaled, axis=-1, keepdims=True)
    )


def weight(ref, first, last):
    return ref[:, 0, :, first:last].reshape(ref.shape[0] * ref.shape[2], last - first)


def attend_kernel(
    valid_ref, own_ref, other_ref, w_ref, qv_bias_ref, out_bias_ref, pre_ref, ctx_ref, q_ref, k_ref, v_ref
):
    group, groups = pl.program_id(0), pl.num_programs(0)
    rows = own_ref.shape[0]
    bias = qv_bias_ref[0]
    projected = mul(own_ref[...], weight(w_ref, 0, 640)) + bias
    projected_other = mul(other_ref[...], weight(w_ref, 128, 640)) + bias[:, 128:]
    lane = lanes((rows, 128))
    row = lax.broadcasted_iota(jnp.int32, (rows, 128), 0)
    contexts = []
    for head in range(3):
        query = jnp.where(
            lane < HEAD, head_block(projected, head).astype(BF16).astype(F32) * SCALE, jnp.where(lane == HEAD, 1.0, 0.0)
        )
        for half, (source, shift) in enumerate(((projected, 0), (projected_other, 2))):
            mask = jnp.where(row < valid_ref[half], 0.0, MASKED)
            tail = jnp.where(lane == HEAD, mask, jnp.where(lane < HEAD + 4, 1.0, 0.0))
            keys = jnp.where(lane < HEAD, head_block(source, 3 + head - shift), tail)
            values = jnp.where(
                lane < HEAD, head_block(source, 6 + head - shift), jnp.where(lane < HEAD + 3, 1.0, 0.0)
            )
            k_ref[head, half * rows : (half + 1) * rows, :] = keys.astype(BF16)
            v_ref[head, half * rows : (half + 1) * rows, :] = values.astype(BF16)
        step = 256
        pieces = []
        for first in range(0, rows, step):
            query_here = query[first : first + step]
            scores = mul(query_here.astype(BF16), k_ref[head], NT)
            peak = jnp.max(scores, axis=1, keepdims=True)
            exps = jnp.exp(scores - peak).astype(BF16)
            mixed = mul(exps, v_ref[head])
            lane_here = lanes((step, 128))
            total = jnp.sum(jnp.where(lane_here == HEAD, mixed, 0.0), axis=1, keepdims=True)
            pieces.append(mixed / total)
            high, middle, low = three_parts(-(peak + jnp.log(total)))
            kept = jnp.where(
                lane_here == HEAD + 1,
                high,
                jnp.where(lane_here == HEAD + 2, middle, jnp.where(lane_here == HEAD + 3, low, query_here)),
            )
            q_ref[head, first : first + step, :] = kept.astype(BF16)
        contexts.append(jnp.concatenate(pieces, axis=0))
    first_half = jnp.where(lane < HEAD, 0.0, pltpu.roll(contexts[0], HEAD, 1)).astype(BF16)
    second_half = pair(contexts[1], contexts[2]).astype(BF16)
    ctx_ref[0, :, 0:128] = first_half
    ctx_ref[0, :, 128:256] = second_half
    part = mul(ctx_ref[0], weight(w_ref, 512, 768), NT)

    @pl.when(group == 0)
    def _():
        pre_ref[...] = part + (out_bias_ref[...] + own_ref[...].astype(F32))

    @pl.when(group > 0)
    def _():
        pre_ref[...] += part


def attend(valid, own, other, weights, qv_bias, out_bias):
    rows, width = own.shape
    groups = weights.shape[1]
    whole = lambda g: (0, 0)
    by_group = lambda g: (g, 0, 0)
    flops = groups * (2 * 2 * rows * width * 640 + 3 * 4 * rows * SLOT * 128)
    return pl.pallas_call(
        attend_kernel,
        name="attend",
        grid=(groups,),
        in_specs=[
            pl.BlockSpec(memory_space=pltpu.SMEM),
            pl.BlockSpec((rows, width), whole),
            pl.BlockSpec((rows, width), whole),
            pl.BlockSpec((weights.shape[0], 1) + weights.shape[2:], lambda g: (0, g, 0, 0)),
            pl.BlockSpec((1, 1, 640), by_group),
            pl.BlockSpec((1, width), whole),
        ],
        out_specs=[
            pl.BlockSpec((rows, width), whole),
            pl.BlockSpec((1, rows, 256), by_group),
            pl.BlockSpec((3, rows, 128), by_group),
            pl.BlockSpec((3, SLOT, 128), by_group),
            pl.BlockSpec((3, SLOT, 128), by_group),
        ],
        out_shape=[
            jax.ShapeDtypeStruct((rows, width), F32),
            jax.ShapeDtypeStruct((groups, rows, 256), BF16),
            jax.ShapeDtypeStruct((3 * groups, rows, 128), BF16),
            jax.ShapeDtypeStruct((3 * groups, SLOT, 128), BF16),
            jax.ShapeDtypeStruct((3 * groups, SLOT, 128), BF16),
        ],
        cost_estimate=pl.CostEstimate(flops=4 * flops, bytes_accessed=24 << 20, transcendentals=12 * rows * SLOT),
        compiler_params=pltpu.CompilerParams(vmem_limit_bytes=60 << 20),
    )(valid, own, other, weights, qv_bias, out_bias)


def up_kernel(pre_ref, gain_ref, shift_ref, w_ref, bias_ref, hidden_ref, active_ref, low_ref, low_t_ref):
    @pl.when(pl.program_id(0) == 0)
    def _():
        scaled, _ = norm_parts(pre_ref[...])
        low = (scaled * gain_ref[...] + shift_ref[...]).astype(BF16)
        low_ref[...] = low
        low_t_ref[...] = low.T

    hidden = mul(low_ref[...], weight(w_ref, 0, w_ref.shape[3])) + bias_ref[0]
    hidden_ref[0] = hidden
    active_ref[0] = (hidden * (0.5 * (1.0 + lax.erf(hidden * 0.7071067811865476)))).astype(BF16)


def up(pre, gain, shift, weights, bias):
    rows, width = pre.shape
    groups, units = weights.shape[1], weights.shape[3]
    whole = lambda g: (0, 0)
    by_group = lambda g: (g, 0, 0)
    return pl.pallas_call(
        up_kernel,
        name="up",
        grid=(groups,),
        in_specs=[
            pl.BlockSpec((rows, width), whole),
            pl.BlockSpec((1, width), whole),
            pl.BlockSpec((1, width), whole),
            pl.BlockSpec((weights.shape[0], 1) + weights.shape[2:], lambda g: (0, g, 0, 0)),
            pl.BlockSpec((1, 1, units), by_group),
        ],
        out_specs=[
            pl.BlockSpec((1, rows, units), by_group),
            pl.BlockSpec((1, rows, units), by_group),
            pl.BlockSpec((rows, width), whole),
            pl.BlockSpec((width, rows), whole),
        ],
        out_shape=[
            jax.ShapeDtypeStruct((groups, rows, units), F32),
            jax.ShapeDtypeStruct((groups, rows, units), BF16),
            jax.ShapeDtypeStruct((rows, width), BF16),
            jax.ShapeDtypeStruct((width, rows), BF16),
        ],
        cost_estimate=pl.CostEstimate(
            flops=2 * groups * rows * width * units, bytes_accessed=24 << 20, transcendentals=groups * rows * units
        ),
        compiler_params=pltpu.CompilerParams(vmem_limit_bytes=60 << 20),
    )(pre, gain, shift, weights, bias)


def down_kernel(
    groups,
    pre_ref,
    cot_ref,
    vec_ref,
    active_ref,
    hidden_ref,
    w2_ref,
    w1_ref,
    low_t_ref,
    out_ref,
    grad_pre_ref,
    grad_low_ref,
    grad_low_t_ref,
    grad_w2_ref,
    grad_w1_ref,
    sums_ref,
    up_bias_ref,
    total_ref,
    upper_ref,
    upper_low_ref,
    upper_low_t_ref,
):
    step = pl.program_id(0)

    @pl.when(step < groups)
    def _():
        part = mul(active_ref[0], weight(w2_ref, 0, w2_ref.shape[3]), NT)

        @pl.when(step == 0)
        def _():
            total_ref[...] = part

        @pl.when(step > 0)
        def _():
            total_ref[...] += part

    @pl.when(step == groups - 1)
    def _():
        gain_one, shift_one = vec_ref[1:2], vec_ref[2:3]
        down_bias, gain_two, shift_two = vec_ref[3:4], vec_ref[4:5], vec_ref[5:6]
        middle = norm_parts(pre_ref[...])[0] * gain_one + shift_one
        scaled, inverse = norm_parts(total_ref[...] + down_bias + middle)
        out_ref[...] = (scaled * gain_two + shift_two).astype(BF16)
        cotangent = cot_ref[...].astype(F32)
        grad = norm_back(cotangent, scaled, inverse, gain_two)
        sums_ref[4:5] = jnp.sum(cotangent * scaled, axis=0, keepdims=True)
        sums_ref[5:6] = jnp.sum(cotangent, axis=0, keepdims=True)
        sums_ref[3:4] = jnp.sum(grad, axis=0, keepdims=True)
        upper_ref[...] = grad
        low = grad.astype(BF16)
        upper_low_ref[...] = low
        upper_low_t_ref[...] = low.T

    @pl.when(step >= groups)
    def _():
        grad_active = mul(upper_low_ref[...], weight(w2_ref, 0, w2_ref.shape[3]))
        hidden = hidden_ref[0]
        cdf = 0.5 * (1.0 + lax.erf(hidden * 0.7071067811865476))
        slope = cdf + hidden * jnp.exp(-0.5 * hidden * hidden) * 0.3989422804014327
        grad_hidden = (grad_active * slope).astype(BF16)
        up_bias_ref[0] = jnp.sum(grad_hidden.astype(F32), axis=0, keepdims=True)
        shape = grad_w2_ref.shape
        grad_w2_ref[...] = mul(upper_low_t_ref[...], active_ref[0]).astype(BF16).reshape(shape)
        grad_w1_ref[...] = mul(low_t_ref[...], grad_hidden).astype(BF16).reshape(shape)
        part = mul(grad_hidden, weight(w1_ref, 0, w1_ref.shape[3]), NT)

        @pl.when(step == groups)
        def _():
            total_ref[...] = part

        @pl.when(step > groups)
        def _():
            total_ref[...] += part

    @pl.when(step == 2 * groups - 1)
    def _():
        scaled, inverse = norm_parts(pre_ref[...])
        grad_middle = upper_ref[...] + total_ref[...]
        grad = norm_back(grad_middle, scaled, inverse, vec_ref[1:2])
        sums_ref[1:2] = jnp.sum(grad_middle * scaled, axis=0, keepdims=True)
        sums_ref[2:3] = jnp.sum(grad_middle, axis=0, keepdims=True)
        sums_ref[0:1] = jnp.sum(grad, axis=0, keepdims=True)
        sums_ref[6:8] = jnp.zeros_like(sums_ref[6:8])
        grad_pre_ref[...] = grad
        low = grad.astype(BF16)
        grad_low_ref[...] = low
        grad_low_t_ref[...] = low.T


def down(pre, cotangent, vectors, active, hidden, w2, w1, low_t):
    rows, width = pre.shape
    groups, units = w2.shape[1], w2.shape[3]
    whole = lambda s: (0, 0)
    both = lambda s: (lax.rem(s, groups), 0, 0)
    late = lambda s: (jnp.maximum(s - groups, 0), 0, 0)
    block = (w2.shape[0], 1) + w2.shape[2:]
    w_both = lambda s: (0, lax.rem(s, groups), 0, 0)
    w_late = lambda s: (0, jnp.maximum(s - groups, 0), 0, 0)
    return pl.pallas_call(
        functools.partial(down_kernel, groups),
        name="down",
        grid=(2 * groups,),
        in_specs=[
            pl.BlockSpec((rows, width), whole),
            pl.BlockSpec((rows, width), whole),
            pl.BlockSpec((8, width), whole),
            pl.BlockSpec((1, rows, units), both),
            pl.BlockSpec((1, rows, units), late),
            pl.BlockSpec(block, w_both),
            pl.BlockSpec(block, w_late),
            pl.BlockSpec((width, rows), whole),
        ],
        out_specs=[
            pl.BlockSpec((rows, width), whole),
            pl.BlockSpec((rows, width), whole),
            pl.BlockSpec((rows, width), whole),
            pl.BlockSpec((width, rows), whole),
            pl.BlockSpec(block, w_late),
            pl.BlockSpec(block, w_late),
            pl.BlockSpec((8, width), whole),
            pl.BlockSpec((1, 1, units), late),
        ],
        out_shape=[
            jax.ShapeDtypeStruct((rows, width), BF16),
            jax.ShapeDtypeStruct((rows, width), F32),
            jax.ShapeDtypeStruct((rows, width), BF16),
            jax.ShapeDtypeStruct((width, rows), BF16),
            jax.ShapeDtypeStruct(w2.shape, BF16),
            jax.ShapeDtypeStruct(w1.shape, BF16),
            jax.ShapeDtypeStruct((8, width), F32),
            jax.ShapeDtypeStruct((groups, 1, units), F32),
        ],
        scratch_shapes=[
            pltpu.VMEM((rows, width), F32),
            pltpu.VMEM((rows, width), F32),
            pltpu.VMEM((rows, width), BF16),
            pltpu.VMEM((width, rows), BF16),
        ],
        cost_estimate=pl.CostEstimate(
            flops=10 * groups * rows * width * units, bytes_accessed=48 << 20, transcendentals=groups * rows * units
        ),
        compiler_params=pltpu.CompilerParams(vmem_limit_bytes=63 << 20),
    )(pre, cotangent, vectors, active, hidden, w2, w1, low_t)


def attend_back_kernel(
    grad_ref,
    grad_t_ref,
    own_t_ref,
    other_t_ref,
    w_ref,
    ctx_ref,
    q_ref,
    k_ref,
    v_ref,
    grad_w_ref,
    grad_own_ref,
    grad_other_ref,
    sums_ref,
    other_total_ref,
):
    group, groups = pl.program_id(0), pl.num_programs(0)
    rows = grad_ref.shape[0]
    step = 256
    grad_context = mul(grad_ref[...], weight(w_ref, 512, 768)).astype(BF16).astype(F32)
    lane = lanes((rows, 128))
    grads = []
    for head in range(3):
        place = 1 + head
        grad_head = head_block(grad_context, place)
        context = head_block(ctx_ref[0].astype(F32), place)
        delta = jnp.sum(jnp.where(lane < HEAD, grad_head * context, 0.0), axis=1, keepdims=True)
        high, middle, low = three_parts(-delta)
        tail = jnp.where(
            lane == HEAD, high, jnp.where(lane == HEAD + 1, middle, jnp.where(lane == HEAD + 2, low, 0.0))
        )
        grad_head = jnp.where(lane < HEAD, grad_head, tail).astype(BF16)
        keys_t = k_ref[head].T
        grad_query = []
        grad_keys = grad_values = None
        for first in range(0, rows, step):
            query_here = q_ref[head, first : first + step, :]
            grad_here = grad_head[first : first + step]
            weights = jnp.exp(mul(k_ref[head], query_here, NT))
            grad_scores = (weights * mul(v_ref[head], grad_here, NT)).astype(BF16)
            values_part = mul(weights.astype(BF16), grad_here)
            keys_part = mul(grad_scores, query_here)
            grad_values = values_part if grad_values is None else grad_values + values_part
            grad_keys = keys_part if grad_keys is None else grad_keys + keys_part
            grad_query.append(mul(keys_t, grad_scores))
        grad_query = jnp.concatenate(grad_query, axis=1).T * SCALE
        grads.append((grad_query, grad_keys, grad_values))
    (q0, k0, v0), (q1, k1, v1), (q2, k2, v2) = grads
    blank = jnp.zeros((rows, 128), F32)
    own = jnp.concatenate(
        [
            pair(q0, q1),
            pair(q2, k0[:rows]),
            pair(k1[:rows], k2[:rows]),
            pair(v0[:rows], v1[:rows]),
            pair(v2[:rows], blank),
        ],
        axis=1,
    )
    other = jnp.concatenate(
        [pair(blank, k0[rows:]), pair(k1[rows:], k2[rows:]), pair(v0[rows:], v1[rows:]), pair(v2[rows:], blank)],
        axis=1,
    )
    own_sum = jnp.sum(own, axis=0, keepdims=True)
    other_sum = jnp.sum(other, axis=0, keepdims=True)
    sums_ref[0, :, 0:128] = own_sum[:, 0:128]
    sums_ref[0, :, 128:640] = own_sum[:, 128:] + other_sum
    own, other = own.astype(BF16), other.astype(BF16)
    grad_w = mul(own_t_ref[...], own)
    grad_w_other = mul(other_t_ref[...], other)
    grad_out = mul(grad_t_ref[...], ctx_ref[0])
    shape = (grad_w_ref.shape[0], 1, grad_w_ref.shape[2])
    grad_w_ref[:, :, :, 0:128] = grad_w[:, 0:128].astype(BF16).reshape(shape + (128,))
    grad_w_ref[:, :, :, 128:512] = (grad_w[:, 128:512] + grad_w_other[:, 0:384]).astype(BF16).reshape(shape + (384,))
    grad_w_ref[:, :, :, 512:640] = (
        (grad_w[:, 512:640] + grad_w_other[:, 384:512] + grad_out[:, 0:128]).astype(BF16).reshape(shape + (128,))
    )
    grad_w_ref[:, :, :, 640:768] = grad_out[:, 128:256].astype(BF16).reshape(shape + (128,))
    own_part = mul(own, weight(w_ref, 0, 640), NT)
    other_part = mul(other, weight(w_ref, 128, 640), NT)

    @pl.when(group == 0)
    def _():
        grad_own_ref[...] = own_part
        other_total_ref[...] = other_part

    @pl.when(group > 0)
    def _():
        grad_own_ref[...] += own_part
        other_total_ref[...] += other_part

    @pl.when(group == groups - 1)
    def _():
        grad_other_ref[...] = other_total_ref[...].astype(BF16)


def attend_back(grad, grad_t, own_t, other_t, weights, ctx, query, keys, values):
    rows, width = grad.shape
    groups = weights.shape[1]
    whole = lambda g: (0, 0)
    by_group = lambda g: (g, 0, 0)
    block = pl.BlockSpec((weights.shape[0], 1) + weights.shape[2:], lambda g: (0, g, 0, 0))
    flops = groups * (3 * 2 * rows * width * 640 + 3 * 10 * rows * SLOT * 128)
    return pl.pallas_call(
        attend_back_kernel,
        name="attend_back",
        grid=(groups,),
        in_specs=[
            pl.BlockSpec((rows, width), whole),
            pl.BlockSpec((width, rows), whole),
            pl.BlockSpec((width, rows), whole),
            pl.BlockSpec((width, rows), whole),
            block,
            pl.BlockSpec((1, rows, 256), by_group),
            pl.BlockSpec((3, rows, 128), by_group),
            pl.BlockSpec((3, SLOT, 128), by_group),
            pl.BlockSpec((3, SLOT, 128), by_group),
        ],
        out_specs=[
            block,
            pl.BlockSpec((rows, width), whole),
            pl.BlockSpec((rows, width), whole),
            pl.BlockSpec((1, 1, 640), by_group),
        ],
        out_shape=[
            jax.ShapeDtypeStruct(weights.shape, BF16),
            jax.ShapeDtypeStruct((rows, width), F32),
            jax.ShapeDtypeStruct((rows, width), BF16),
            jax.ShapeDtypeStruct((groups, 1, 640), F32),
        ],
        scratch_shapes=[pltpu.VMEM((rows, width), F32)],
        cost_estimate=pl.CostEstimate(flops=4 * flops, bytes_accessed=32 << 20, transcendentals=12 * rows * SLOT),
        compiler_params=pltpu.CompilerParams(vmem_limit_bytes=63 << 20),
    )(grad, grad_t, own_t, other_t, weights, ctx, query, keys, values)


def gather(local):
    return lax.all_gather(local, BOTH, axis=0, tiled=True)


def scatter(partial):
    return lax.psum_scatter(partial, BOTH, scatter_dimension=0, tiled=True)


def body(
    frames,
    w_qkv,
    b_qv,
    w_out,
    b_out,
    ln1_gain,
    ln1_bias,
    w_ff1,
    b_ff1,
    w_ff2,
    b_ff2,
    ln2_gain,
    ln2_bias,
    cotangent,
    clip_lengths,
    clip_slot,
):
    n_dp, n_mp = lax.axis_size("dp"), lax.axis_size("mp")
    rows, width = frames.shape
    part = w_ff1.shape[0]
    shape = (n_dp, n_mp, part, w_ff1.shape[1])
    share = b_out.shape[0]

    partner = [(m, m ^ 1) for m in range(n_mp)]
    other = lax.ppermute(frames, "mp", partner)
    packed = jnp.concatenate([w_qkv[0], w_qkv[1], w_qkv[2], w_out.T], axis=1)
    w_attn = gather(packed).reshape(shape)
    w1 = gather(w_ff1).reshape(shape)
    w2 = gather(w_ff2.T).reshape(shape)
    small = jnp.concatenate(
        [b_out, ln1_gain, ln1_bias, b_ff2, ln2_gain, ln2_bias, b_qv.reshape(-1).astype(F32), b_ff1.astype(F32)]
    )[None]
    small = gather(small)
    vectors = small[:, : 6 * share].reshape(n_dp * n_mp, 6, share).transpose(1, 0, 2).reshape(6, width)
    vectors = jnp.concatenate([vectors, jnp.zeros((2, width), F32)])
    ordered = small.reshape(n_dp, n_mp, -1).transpose(1, 0, 2)
    qv = ordered[:, :, 6 * share : 8 * share].reshape(n_mp, n_dp, 2, share).transpose(0, 2, 1, 3)
    qv = qv.reshape(n_mp, 2, 1, n_dp * share)
    heads_width = n_dp * share
    qv_bias = jnp.concatenate(
        [qv[:, 0], jnp.zeros((n_mp, 1, heads_width), F32), qv[:, 1], jnp.zeros((n_mp, 1, HEAD), F32)], axis=2
    )
    up_bias = ordered[:, :, 8 * share :].reshape(n_mp, 1, -1)

    index = lax.axis_index("dp") * n_mp + lax.axis_index("mp")
    slot = index // (SLOT // rows)
    half = index % (SLOT // rows)
    length = jnp.sum(jnp.where(clip_slot == slot, clip_lengths, 0))
    valid = jnp.stack([length - half * rows, length - (1 - half) * rows]).astype(jnp.int32)

    pre_one, ctx, query, keys, values = attend(valid, frames, other, w_attn, qv_bias, vectors[0:1])
    hidden, active, low, low_t = up(pre_one, vectors[1:2], vectors[2:3], w1, up_bias)
    output, grad_pre, grad_low, grad_low_t, grad_w2, grad_w1, sums, grad_up_bias = down(
        pre_one, cotangent, vectors, active, hidden, w2, w1, low_t
    )
    flat = (n_dp * n_mp * part, shape[3])
    done_w2 = scatter(grad_w2.reshape(flat))
    done_w1 = scatter(grad_w1.reshape(flat))
    grad_w, grad_own, grad_other, head_sums = attend_back(
        grad_low, grad_low_t, frames.T, other.T, w_attn, ctx, query, keys, values
    )
    returned = lax.ppermute(grad_other, "mp", partner)
    done_w = scatter(grad_w.reshape(flat)).astype(F32)
    grad_input = grad_pre + grad_own + returned.astype(F32)

    sums = sums[:6].reshape(6, n_dp * n_mp, share).transpose(1, 0, 2).reshape(n_dp * n_mp, 6 * share)
    head_sums = jnp.concatenate(
        [head_sums[:, :, :heads_width], head_sums[:, :, 2 * heads_width : 3 * heads_width]], axis=1
    )
    head_sums = head_sums.reshape(n_mp, 2, n_dp, share).transpose(2, 0, 1, 3).reshape(n_dp * n_mp, 2 * share)
    unit_sums = grad_up_bias.reshape(n_mp, n_dp, -1).transpose(1, 0, 2).reshape(n_dp * n_mp, -1)
    small = scatter(jnp.concatenate([sums, head_sums, unit_sums], axis=1))[0]
    (d_out_bias, d_gain1, d_shift1, d_down_bias, d_gain2, d_shift2) = [
        small[i * share : (i + 1) * share] for i in range(6)
    ]
    d_qv = small[6 * share : 8 * share].reshape(2, share)
    d_up_bias = small[8 * share :]
    d_qkv = jnp.stack([done_w[:, i * heads_width : (i + 1) * heads_width] for i in range(3)])
    return (
        output,
        grad_input,
        d_qkv,
        d_qv,
        done_w[:, 3 * heads_width :].T,
        d_out_bias,
        d_gain1,
        d_shift1,
        done_w1.astype(F32),
        d_up_bias,
        done_w2.astype(F32).T,
        d_down_bias,
        d_gain2,
        d_shift2,
    )


def solution(mesh):
    rows, vector, group_vector = P(BOTH, None), P(BOTH), P(("mp", "dp"))
    qkv, qv, out, up_spec = P(None, "dp", "mp"), P(None, ("mp", "dp")), P("mp", "dp"), P("dp", "mp")
    weights = (qkv, qv, out, vector, vector, vector, up_spec, group_vector, out, vector, vector, vector)
    return jax.shard_map(
        body,
        mesh=mesh,
        in_specs=(rows,) + weights + (rows, P(), P()),
        out_specs=(rows, rows) + weights,
        check_vma=False,
    )
```

```python
import functools

import jax
import jax.numpy as jnp
from jax import lax
from jax.experimental import pallas as pl
from jax.experimental.pallas import tpu as pltpu
from jax.sharding import PartitionSpec as P

HEAD = 64
SLOT = 1536
EPS = 1e-05
SCALE = 0.125
MASKED = -1e30
BOTH = ("dp", "mp")
F32 = jnp.float32
BF16 = jnp.bfloat16
MESH = pl.DeviceIdType.MESH
NN = (((1,), (0,)), ((), ()))
NT = (((1,), (1,)), ((), ()))


def mul(left, right, dims=NN):
    return lax.dot_general(left, right, dims, preferred_element_type=F32)


def lanes(shape):
    return lax.broadcasted_iota(jnp.int32, shape, 1)


def three_parts(value):
    high = value.astype(BF16).astype(F32)
    rest = value - high
    middle = rest.astype(BF16).astype(F32)
    return high, middle, rest - middle


def head_block(value, place):
    block = value[:, 128 * (place // 2) : 128 * (place // 2) + 128]
    return pltpu.roll(block, HEAD, 1) if place % 2 else block


def pair(low, high):
    return jnp.where(lanes(low.shape) < HEAD, low, pltpu.roll(high, HEAD, 1))


def norm_parts(field):
    mean = jnp.mean(field, axis=-1, keepdims=True)
    centred = field - mean
    spread = jnp.mean(centred * centred, axis=-1, keepdims=True)
    inverse = lax.rsqrt(spread + EPS)
    return centred * inverse, inverse


def norm_back(grad, scaled, inverse, gain):
    inner = grad * gain
    return inverse * (
        inner
        - jnp.mean(inner, axis=-1, keepdims=True)
        - scaled * jnp.mean(inner * scaled, axis=-1, keepdims=True)
    )


def weight(ref, first, last):
    return ref[:, 0, :, first:last].reshape(ref.shape[0] * ref.shape[2], last - first)


def attend_kernel(
    valid_ref, own_ref, other_ref, w_ref, qv_bias_ref, out_bias_ref, pre_ref, ctx_ref, q_ref, k_ref, v_ref
):
    group, groups = pl.program_id(0), pl.num_programs(0)
    rows = own_ref.shape[0]
    bias = qv_bias_ref[0]
    projected = mul(own_ref[...], weight(w_ref, 0, 640)) + bias
    projected_other = mul(other_ref[...], weight(w_ref, 128, 640)) + bias[:, 128:]
    lane = lanes((rows, 128))
    row = lax.broadcasted_iota(jnp.int32, (rows, 128), 0)
    contexts = []
    for head in range(3):
        query = jnp.where(
            lane < HEAD, head_block(projected, head).astype(BF16).astype(F32) * SCALE, jnp.where(lane == HEAD, 1.0, 0.0)
        )
        for half, (source, shift) in enumerate(((projected, 0), (projected_other, 2))):
            mask = jnp.where(row < valid_ref[half], 0.0, MASKED)
            tail = jnp.where(lane == HEAD, mask, jnp.where(lane < HEAD + 4, 1.0, 0.0))
            keys = jnp.where(lane < HEAD, head_block(source, 3 + head - shift), tail)
            values = jnp.where(
                lane < HEAD, head_block(source, 6 + head - shift), jnp.where(lane < HEAD + 3, 1.0, 0.0)
            )
            k_ref[head, half * rows : (half + 1) * rows, :] = keys.astype(BF16)
            v_ref[head, half * rows : (half + 1) * rows, :] = values.astype(BF16)
        step = 256
        pieces = []
        for first in range(0, rows, step):
            query_here = query[first : first + step]
            scores = mul(query_here.astype(BF16), k_ref[head], NT)
            peak = jnp.max(scores, axis=1, keepdims=True)
            exps = jnp.exp(scores - peak).astype(BF16)
            mixed = mul(exps, v_ref[head])
            lane_here = lanes((step, 128))
            total = jnp.sum(jnp.where(lane_here == HEAD, mixed, 0.0), axis=1, keepdims=True)
            pieces.append(mixed / total)
            high, middle, low = three_parts(-(peak + jnp.log(total)))
            kept = jnp.where(
                lane_here == HEAD + 1,
                high,
                jnp.where(lane_here == HEAD + 2, middle, jnp.where(lane_here == HEAD + 3, low, query_here)),
            )
            q_ref[head, first : first + step, :] = kept.astype(BF16)
        contexts.append(jnp.concatenate(pieces, axis=0))
    first_half = jnp.where(lane < HEAD, 0.0, pltpu.roll(contexts[0], HEAD, 1)).astype(BF16)
    second_half = pair(contexts[1], contexts[2]).astype(BF16)
    ctx_ref[0, :, 0:128] = first_half
    ctx_ref[0, :, 128:256] = second_half
    part = mul(ctx_ref[0], weight(w_ref, 512, 768), NT)

    @pl.when(group == 0)
    def _():
        pre_ref[...] = part + (out_bias_ref[...] + own_ref[...].astype(F32))

    @pl.when(group > 0)
    def _():
        pre_ref[...] += part


def attend(valid, own, other, weights, qv_bias, out_bias):
    rows, width = own.shape
    groups = weights.shape[1]
    whole = lambda g: (0, 0)
    by_group = lambda g: (g, 0, 0)
    flops = groups * (2 * 2 * rows * width * 640 + 3 * 4 * rows * SLOT * 128)
    return pl.pallas_call(
        attend_kernel,
        name="attend",
        grid=(groups,),
        in_specs=[
            pl.BlockSpec(memory_space=pltpu.SMEM),
            pl.BlockSpec((rows, width), whole),
            pl.BlockSpec((rows, width), whole),
            pl.BlockSpec((weights.shape[0], 1) + weights.shape[2:], lambda g: (0, g, 0, 0)),
            pl.BlockSpec((1, 1, 640), by_group),
            pl.BlockSpec((1, width), whole),
        ],
        out_specs=[
            pl.BlockSpec((rows, width), whole),
            pl.BlockSpec((1, rows, 256), by_group),
            pl.BlockSpec((3, rows, 128), by_group),
            pl.BlockSpec((3, SLOT, 128), by_group),
            pl.BlockSpec((3, SLOT, 128), by_group),
        ],
        out_shape=[
            jax.ShapeDtypeStruct((rows, width), F32),
            jax.ShapeDtypeStruct((groups, rows, 256), BF16),
            jax.ShapeDtypeStruct((3 * groups, rows, 128), BF16),
            jax.ShapeDtypeStruct((3 * groups, SLOT, 128), BF16),
            jax.ShapeDtypeStruct((3 * groups, SLOT, 128), BF16),
        ],
        cost_estimate=pl.CostEstimate(flops=4 * flops, bytes_accessed=24 << 20, transcendentals=12 * rows * SLOT),
        compiler_params=pltpu.CompilerParams(vmem_limit_bytes=60 << 20),
    )(valid, own, other, weights, qv_bias, out_bias)


def up_kernel(pre_ref, gain_ref, shift_ref, w_ref, bias_ref, hidden_ref, active_ref, low_ref, low_t_ref):
    @pl.when(pl.program_id(0) == 0)
    def _():
        scaled, _ = norm_parts(pre_ref[...])
        low = (scaled * gain_ref[...] + shift_ref[...]).astype(BF16)
        low_ref[...] = low
        low_t_ref[...] = low.T

    hidden = mul(low_ref[...], weight(w_ref, 0, w_ref.shape[3])) + bias_ref[0]
    hidden_ref[0] = hidden
    active_ref[0] = (hidden * (0.5 * (1.0 + lax.erf(hidden * 0.7071067811865476)))).astype(BF16)


def up(pre, gain, shift, weights, bias):
    rows, width = pre.shape
    groups, units = weights.shape[1], weights.shape[3]
    whole = lambda g: (0, 0)
    by_group = lambda g: (g, 0, 0)
    return pl.pallas_call(
        up_kernel,
        name="up",
        grid=(groups,),
        in_specs=[
            pl.BlockSpec((rows, width), whole),
            pl.BlockSpec((1, width), whole),
            pl.BlockSpec((1, width), whole),
            pl.BlockSpec((weights.shape[0], 1) + weights.shape[2:], lambda g: (0, g, 0, 0)),
            pl.BlockSpec((1, 1, units), by_group),
        ],
        out_specs=[
            pl.BlockSpec((1, rows, units), by_group),
            pl.BlockSpec((1, rows, units), by_group),
            pl.BlockSpec((rows, width), whole),
            pl.BlockSpec((width, rows), whole),
        ],
        out_shape=[
            jax.ShapeDtypeStruct((groups, rows, units), F32),
            jax.ShapeDtypeStruct((groups, rows, units), BF16),
            jax.ShapeDtypeStruct((rows, width), BF16),
            jax.ShapeDtypeStruct((width, rows), BF16),
        ],
        cost_estimate=pl.CostEstimate(
            flops=2 * groups * rows * width * units, bytes_accessed=24 << 20, transcendentals=groups * rows * units
        ),
        compiler_params=pltpu.CompilerParams(vmem_limit_bytes=60 << 20),
    )(pre, gain, shift, weights, bias)


def down_kernel(
    groups,
    pre_ref,
    cot_ref,
    vec_ref,
    active_ref,
    hidden_ref,
    w2_ref,
    w1_ref,
    low_t_ref,
    out_ref,
    grad_pre_ref,
    grad_low_ref,
    grad_low_t_ref,
    grad_w2_ref,
    grad_w1_ref,
    sums_ref,
    up_bias_ref,
    total_ref,
    upper_ref,
    upper_low_ref,
    upper_low_t_ref,
):
    step = pl.program_id(0)

    @pl.when(step < groups)
    def _():
        part = mul(active_ref[0], weight(w2_ref, 0, w2_ref.shape[3]), NT)

        @pl.when(step == 0)
        def _():
            total_ref[...] = part

        @pl.when(step > 0)
        def _():
            total_ref[...] += part

    @pl.when(step == groups - 1)
    def _():
        gain_one, shift_one = vec_ref[1:2], vec_ref[2:3]
        down_bias, gain_two, shift_two = vec_ref[3:4], vec_ref[4:5], vec_ref[5:6]
        middle = norm_parts(pre_ref[...])[0] * gain_one + shift_one
        scaled, inverse = norm_parts(total_ref[...] + down_bias + middle)
        out_ref[...] = (scaled * gain_two + shift_two).astype(BF16)
        cotangent = cot_ref[...].astype(F32)
        grad = norm_back(cotangent, scaled, inverse, gain_two)
        sums_ref[4:5] = jnp.sum(cotangent * scaled, axis=0, keepdims=True)
        sums_ref[5:6] = jnp.sum(cotangent, axis=0, keepdims=True)
        sums_ref[3:4] = jnp.sum(grad, axis=0, keepdims=True)
        upper_ref[...] = grad
        low = grad.astype(BF16)
        upper_low_ref[...] = low
        upper_low_t_ref[...] = low.T

    @pl.when(step >= groups)
    def _():
        grad_active = mul(upper_low_ref[...], weight(w2_ref, 0, w2_ref.shape[3]))
        hidden = hidden_ref[0]
        cdf = 0.5 * (1.0 + lax.erf(hidden * 0.7071067811865476))
        slope = cdf + hidden * jnp.exp(-0.5 * hidden * hidden) * 0.3989422804014327
        grad_hidden = (grad_active * slope).astype(BF16)
        up_bias_ref[0] = jnp.sum(grad_hidden.astype(F32), axis=0, keepdims=True)
        shape = grad_w2_ref.shape
        grad_w2_ref[...] = mul(upper_low_t_ref[...], active_ref[0]).astype(BF16).reshape(shape)
        grad_w1_ref[...] = mul(low_t_ref[...], grad_hidden).astype(BF16).reshape(shape)
        part = mul(grad_hidden, weight(w1_ref, 0, w1_ref.shape[3]), NT)

        @pl.when(step == groups)
        def _():
            total_ref[...] = part

        @pl.when(step > groups)
        def _():
            total_ref[...] += part

    @pl.when(step == 2 * groups - 1)
    def _():
        scaled, inverse = norm_parts(pre_ref[...])
        grad_middle = upper_ref[...] + total_ref[...]
        grad = norm_back(grad_middle, scaled, inverse, vec_ref[1:2])
        sums_ref[1:2] = jnp.sum(grad_middle * scaled, axis=0, keepdims=True)
        sums_ref[2:3] = jnp.sum(grad_middle, axis=0, keepdims=True)
        sums_ref[0:1] = jnp.sum(grad, axis=0, keepdims=True)
        sums_ref[6:8] = jnp.zeros_like(sums_ref[6:8])
        grad_pre_ref[...] = grad
        low = grad.astype(BF16)
        grad_low_ref[...] = low
        grad_low_t_ref[...] = low.T


def down(pre, cotangent, vectors, active, hidden, w2, w1, low_t):
    rows, width = pre.shape
    groups, units = w2.shape[1], w2.shape[3]
    whole = lambda s: (0, 0)
    both = lambda s: (lax.rem(s, groups), 0, 0)
    late = lambda s: (jnp.maximum(s - groups, 0), 0, 0)
    block = (w2.shape[0], 1) + w2.shape[2:]
    w_both = lambda s: (0, lax.rem(s, groups), 0, 0)
    w_late = lambda s: (0, jnp.maximum(s - groups, 0), 0, 0)
    return pl.pallas_call(
        functools.partial(down_kernel, groups),
        name="down",
        grid=(2 * groups,),
        in_specs=[
            pl.BlockSpec((rows, width), whole),
            pl.BlockSpec((rows, width), whole),
            pl.BlockSpec((8, width), whole),
            pl.BlockSpec((1, rows, units), both),
            pl.BlockSpec((1, rows, units), late),
            pl.BlockSpec(block, w_both),
            pl.BlockSpec(block, w_late),
            pl.BlockSpec((width, rows), whole),
        ],
        out_specs=[
            pl.BlockSpec((rows, width), whole),
            pl.BlockSpec((rows, width), whole),
            pl.BlockSpec((rows, width), whole),
            pl.BlockSpec((width, rows), whole),
            pl.BlockSpec(block, w_late),
            pl.BlockSpec(block, w_late),
            pl.BlockSpec((8, width), whole),
            pl.BlockSpec((1, 1, units), late),
        ],
        out_shape=[
            jax.ShapeDtypeStruct((rows, width), BF16),
            jax.ShapeDtypeStruct((rows, width), F32),
            jax.ShapeDtypeStruct((rows, width), BF16),
            jax.ShapeDtypeStruct((width, rows), BF16),
            jax.ShapeDtypeStruct(w2.shape, BF16),
            jax.ShapeDtypeStruct(w1.shape, BF16),
            jax.ShapeDtypeStruct((8, width), F32),
            jax.ShapeDtypeStruct((groups, 1, units), F32),
        ],
        scratch_shapes=[
            pltpu.VMEM((rows, width), F32),
            pltpu.VMEM((rows, width), F32),
            pltpu.VMEM((rows, width), BF16),
            pltpu.VMEM((width, rows), BF16),
        ],
        cost_estimate=pl.CostEstimate(
            flops=10 * groups * rows * width * units, bytes_accessed=48 << 20, transcendentals=groups * rows * units
        ),
        compiler_params=pltpu.CompilerParams(vmem_limit_bytes=63 << 20),
    )(pre, cotangent, vectors, active, hidden, w2, w1, low_t)


def attend_back_kernel(
    grad_ref,
    grad_t_ref,
    own_t_ref,
    other_t_ref,
    w_ref,
    ctx_ref,
    q_ref,
    k_ref,
    v_ref,
    grad_w_ref,
    grad_own_ref,
    grad_other_ref,
    sums_ref,
    other_total_ref,
):
    group, groups = pl.program_id(0), pl.num_programs(0)
    rows = grad_ref.shape[0]
    step = 256
    grad_context = mul(grad_ref[...], weight(w_ref, 512, 768)).astype(BF16).astype(F32)
    lane = lanes((rows, 128))
    grads = []
    for head in range(3):
        place = 1 + head
        grad_head = head_block(grad_context, place)
        context = head_block(ctx_ref[0].astype(F32), place)
        delta = jnp.sum(jnp.where(lane < HEAD, grad_head * context, 0.0), axis=1, keepdims=True)
        high, middle, low = three_parts(-delta)
        tail = jnp.where(
            lane == HEAD, high, jnp.where(lane == HEAD + 1, middle, jnp.where(lane == HEAD + 2, low, 0.0))
        )
        grad_head = jnp.where(lane < HEAD, grad_head, tail).astype(BF16)
        keys_t = k_ref[head].T
        grad_query = []
        grad_keys = grad_values = None
        for first in range(0, rows, step):
            query_here = q_ref[head, first : first + step, :]
            grad_here = grad_head[first : first + step]
            weights = jnp.exp(mul(k_ref[head], query_here, NT))
            grad_scores = (weights * mul(v_ref[head], grad_here, NT)).astype(BF16)
            values_part = mul(weights.astype(BF16), grad_here)
            keys_part = mul(grad_scores, query_here)
            grad_values = values_part if grad_values is None else grad_values + values_part
            grad_keys = keys_part if grad_keys is None else grad_keys + keys_part
            grad_query.append(mul(keys_t, grad_scores))
        grad_query = jnp.concatenate(grad_query, axis=1).T * SCALE
        grads.append((grad_query, grad_keys, grad_values))
    (q0, k0, v0), (q1, k1, v1), (q2, k2, v2) = grads
    blank = jnp.zeros((rows, 128), F32)
    own = jnp.concatenate(
        [
            pair(q0, q1),
            pair(q2, k0[:rows]),
            pair(k1[:rows], k2[:rows]),
            pair(v0[:rows], v1[:rows]),
            pair(v2[:rows], blank),
        ],
        axis=1,
    )
    other = jnp.concatenate(
        [pair(blank, k0[rows:]), pair(k1[rows:], k2[rows:]), pair(v0[rows:], v1[rows:]), pair(v2[rows:], blank)],
        axis=1,
    )
    own_sum = jnp.sum(own, axis=0, keepdims=True)
    other_sum = jnp.sum(other, axis=0, keepdims=True)
    sums_ref[0, :, 0:128] = own_sum[:, 0:128]
    sums_ref[0, :, 128:640] = own_sum[:, 128:] + other_sum
    own, other = own.astype(BF16), other.astype(BF16)
    grad_w = mul(own_t_ref[...], own)
    grad_w_other = mul(other_t_ref[...], other)
    grad_out = mul(grad_t_ref[...], ctx_ref[0])
    shape = (grad_w_ref.shape[0], 1, grad_w_ref.shape[2])
    grad_w_ref[:, :, :, 0:128] = grad_w[:, 0:128].astype(BF16).reshape(shape + (128,))
    grad_w_ref[:, :, :, 128:512] = (grad_w[:, 128:512] + grad_w_other[:, 0:384]).astype(BF16).reshape(shape + (384,))
    grad_w_ref[:, :, :, 512:640] = (
        (grad_w[:, 512:640] + grad_w_other[:, 384:512] + grad_out[:, 0:128]).astype(BF16).reshape(shape + (128,))
    )
    grad_w_ref[:, :, :, 640:768] = grad_out[:, 128:256].astype(BF16).reshape(shape + (128,))
    own_part = mul(own, weight(w_ref, 0, 640), NT)
    other_part = mul(other, weight(w_ref, 128, 640), NT)

    @pl.when(group == 0)
    def _():
        grad_own_ref[...] = own_part
        other_total_ref[...] = other_part

    @pl.when(group > 0)
    def _():
        grad_own_ref[...] += own_part
        other_total_ref[...] += other_part

    @pl.when(group == groups - 1)
    def _():
        grad_other_ref[...] = other_total_ref[...].astype(BF16)


def attend_back(grad, grad_t, own_t, other_t, weights, ctx, query, keys, values):
    rows, width = grad.shape
    groups = weights.shape[1]
    whole = lambda g: (0, 0)
    by_group = lambda g: (g, 0, 0)
    block = pl.BlockSpec((weights.shape[0], 1) + weights.shape[2:], lambda g: (0, g, 0, 0))
    flops = groups * (3 * 2 * rows * width * 640 + 3 * 10 * rows * SLOT * 128)
    return pl.pallas_call(
        attend_back_kernel,
        name="attend_back",
        grid=(groups,),
        in_specs=[
            pl.BlockSpec((rows, width), whole),
            pl.BlockSpec((width, rows), whole),
            pl.BlockSpec((width, rows), whole),
            pl.BlockSpec((width, rows), whole),
            block,
            pl.BlockSpec((1, rows, 256), by_group),
            pl.BlockSpec((3, rows, 128), by_group),
            pl.BlockSpec((3, SLOT, 128), by_group),
            pl.BlockSpec((3, SLOT, 128), by_group),
        ],
        out_specs=[
            block,
            pl.BlockSpec((rows, width), whole),
            pl.BlockSpec((rows, width), whole),
            pl.BlockSpec((1, 1, 640), by_group),
        ],
        out_shape=[
            jax.ShapeDtypeStruct(weights.shape, BF16),
            jax.ShapeDtypeStruct((rows, width), F32),
            jax.ShapeDtypeStruct((rows, width), BF16),
            jax.ShapeDtypeStruct((groups, 1, 640), F32),
        ],
        scratch_shapes=[pltpu.VMEM((rows, width), F32)],
        cost_estimate=pl.CostEstimate(flops=4 * flops, bytes_accessed=32 << 20, transcendentals=12 * rows * SLOT),
        compiler_params=pltpu.CompilerParams(vmem_limit_bytes=63 << 20),
    )(grad, grad_t, own_t, other_t, weights, ctx, query, keys, values)


CORE, ALONG_X, ALONG_Y = 1, 2, 4
DIAGONAL = ALONG_X | ALONG_Y
COLUMNS = (0, ALONG_X, ALONG_Y, DIAGONAL)


def meet(me, z, depth):
    barrier = pltpu.get_barrier_semaphore()
    for bit in (CORE, ALONG_X, ALONG_Y):
        pl.semaphore_signal(barrier, inc=1, device_id=(me ^ bit, z), device_id_type=MESH)

    @pl.when(z > 0)
    def _():
        pl.semaphore_signal(barrier, inc=1, device_id=(me, z - 1), device_id_type=MESH)

    @pl.when(z < depth - 1)
    def _():
        pl.semaphore_signal(barrier, inc=1, device_id=(me, z + 1), device_id_type=MESH)

    pl.semaphore_wait(barrier, 3 + (z > 0).astype(jnp.int32) + (z < depth - 1).astype(jnp.int32))


def near_first(z, depth):
    yield z, None
    for distance in range(1, depth):
        for place in (z - distance, z + distance):
            yield place, (place >= 0) & (place < depth)


def given(condition, action):
    if condition is None:
        action()
    else:
        pl.when(condition)(action)


def halves(rows):
    return (rows // 2, rows) if rows % 32 == 0 else (rows, rows)


UP, DOWN, X, Y, VIA_Y, VIA_X, C0 = range(7)
GATHER_KINDS = C0 + 4


def gather_kernel(count, depth, *refs):
    locals_, wholes = refs[:count], refs[count : 2 * count]
    send_sem, recv_sem = refs[2 * count :]
    me, z = lax.axis_index("dp"), lax.axis_index("mp")

    def copy(which, kind, place, source, target, to):
        return pltpu.make_async_remote_copy(
            src_ref=source,
            dst_ref=target,
            send_sem=send_sem.at[which, kind, place],
            recv_sem=recv_sem.at[which, kind, place],
            device_id=to,
            device_id_type=MESH,
        )

    meet(me, z, depth)

    def column(which, place, source, owner, kinds):
        whole = wholes[which]
        for kind, to, first, last in kinds:
            view = source if first == 0 and last == source.shape[0] else source.at[first:last]
            copy(which, kind, place, view, whole.at[owner, place, first:last], to).start()

    def arrived(which, kind, place, owner, first, last):
        view = wholes[which].at[owner, place, first:last]
        copy(which, kind, place, view, view, (me, z)).wait_recv()

    def first_stage(which, place, condition):
        rows = locals_[which].shape[0]

        def act():
            own = condition is None
            source = locals_[which] if own else wholes[which].at[me, place]
            if not own:
                pl.when(place < z)(lambda: arrived(which, UP, place, me, 0, rows))
                pl.when(place > z)(lambda: arrived(which, DOWN, place, me, 0, rows))
            up_from = (z < depth - 1) if own else (place < z) & (z < depth - 1)
            down_from = (z > 0) if own else (place > z) & (z > 0)
            pl.when(up_from)(lambda: column(which, place, source, me, [(UP, (me, z + 1), 0, rows)]))
            pl.when(down_from)(lambda: column(which, place, source, me, [(DOWN, (me, z - 1), 0, rows)]))
            column(
                which,
                place,
                source,
                me,
                [
                    (X, (me ^ ALONG_X, z), 0, rows),
                    (Y, (me ^ ALONG_Y, z), 0, rows),
                    (C0, (me ^ CORE, z), 0, rows),
                ],
            )

        given(condition, act)

    def second_stage(which, place, condition):
        rows = locals_[which].shape[0]
        half, _ = halves(rows)

        def act():
            arrived(which, X, place, me ^ ALONG_X, 0, rows)
            source = wholes[which].at[me ^ ALONG_X, place]
            column(
                which,
                place,
                source,
                me ^ ALONG_X,
                [(VIA_Y, (me ^ ALONG_Y, z), 0, half), (C0 + 1, (me ^ CORE, z), 0, rows)],
            )
            arrived(which, Y, place, me ^ ALONG_Y, 0, rows)
            source = wholes[which].at[me ^ ALONG_Y, place]
            kinds = [(C0 + 2, (me ^ CORE, z), 0, rows)]
            if half < rows:
                kinds = [(VIA_X, (me ^ ALONG_X, z), half, rows)] + kinds
            column(which, place, source, me ^ ALONG_Y, kinds)

        given(condition, act)

    def third_stage(which, place, condition):
        rows = locals_[which].shape[0]
        half, _ = halves(rows)

        def act():
            arrived(which, VIA_Y, place, me ^ DIAGONAL, 0, half)
            if half < rows:
                arrived(which, VIA_X, place, me ^ DIAGONAL, half, rows)
            source = wholes[which].at[me ^ DIAGONAL, place]
            column(which, place, source, me ^ DIAGONAL, [(C0 + 3, (me ^ CORE, z), 0, rows)])

        given(condition, act)

    def last_stage(which, place):
        rows = locals_[which].shape[0]
        for number, bit in enumerate(COLUMNS):
            arrived(which, C0 + number, place, me ^ CORE ^ bit, 0, rows)

    order = []
    for which in range(count):
        pltpu.make_async_copy(
            locals_[which], wholes[which].at[me, z], send_sem.at[which, GATHER_KINDS, 0]
        ).start()
        order += [(which,) + item for item in near_first(z, depth)]
    lag = len(order) // count
    for step in range(len(order) + 2 * lag):
        if step < len(order):
            first_stage(*order[step])
        if 0 <= step - lag < len(order):
            second_stage(*order[step - lag])
        if 0 <= step - 2 * lag:
            third_stage(*order[step - 2 * lag])
    for which in range(count):
        rows = locals_[which].shape[0]
        half, _ = halves(rows)
        for place in range(depth):
            last_stage(which, place)
        for place, condition in near_first(z, depth):

            def sent(which=which, place=place, own=condition is None):
                whole = wholes[which].at[me, place]
                pieces = [(X, 0, rows), (Y, 0, rows), (VIA_Y, 0, half)] + [(C0 + n, 0, rows) for n in range(4)]
                if half < rows:
                    pieces.append((VIA_X, half, rows))
                for kind, first, last in pieces:
                    view = whole.at[first:last]
                    copy(which, kind, place, view, view, (me, z)).wait_send()
                up_from = (z < depth - 1) if own else (place < z) & (z < depth - 1)
                down_from = (z > 0) if own else (place > z) & (z > 0)
                pl.when(up_from)(lambda: copy(which, UP, place, whole, whole, (me, z)).wait_send())
                pl.when(down_from)(lambda: copy(which, DOWN, place, whole, whole, (me, z)).wait_send())

            given(condition, sent)
        pltpu.make_async_copy(
            locals_[which], wholes[which].at[me, z], send_sem.at[which, GATHER_KINDS, 0]
        ).wait()


def gather_all(locals_, n_dp, n_mp, number):
    count = len(locals_)
    sems = pltpu.SemaphoreType.DMA((count, GATHER_KINDS + 1, n_mp))
    return pl.pallas_call(
        functools.partial(gather_kernel, count, n_mp),
        name="gather",
        in_specs=[pl.BlockSpec(memory_space=pltpu.VMEM)] * count,
        out_specs=[pl.BlockSpec(memory_space=pl.ANY)] * count,
        out_shape=[jax.ShapeDtypeStruct((n_dp, n_mp) + a.shape, a.dtype) for a in locals_],
        scratch_shapes=[sems, sems],
        compiler_params=pltpu.CompilerParams(collective_id=number, has_side_effects=True),
    )(*locals_)


TO_X, TO_Y, X_LOW, X_HIGH, Y_LOW, Y_HIGH, Z_UP, Z_DOWN, S0 = range(9)
SCATTER_KINDS = S0 + 4


def scatter_kernel(count, depth, *refs):
    partials, outs = refs[:count], refs[count : 2 * count]
    scratch = refs[2 * count : -2]
    send_sem, recv_sem = refs[-2:]
    me, z = lax.axis_index("dp"), lax.axis_index("mp")

    def copy(which, kind, place, source, target, to):
        return pltpu.make_async_remote_copy(
            src_ref=source,
            dst_ref=target,
            send_sem=send_sem.at[which, kind, place],
            recv_sem=recv_sem.at[which, kind, place],
            device_id=to,
            device_id_type=MESH,
        )

    def bufs(which):
        return scratch[4 * which : 4 * which + 4]

    def add(target, *others):
        total = target[...].astype(F32)
        for other in others:
            total = total + other[...].astype(F32)
        target[...] = total.astype(target.dtype)

    meet(me, z, depth)
    started = []

    def start(which, kind, place, source, target, to):
        copy(which, kind, place, source, target, to).start()
        started.append((which, kind, place, source, target))

    def wait(which, kind, place, view):
        copy(which, kind, place, view, view, (me, z)).wait_recv()

    places = [depth - 1, 0] + list(range(1, depth - 1))[::-1]
    order = [(which, place) for which in range(count) for place in places]
    for which, place in order:
        core = bufs(which)[0]
        for number in (3, 1, 2, 0):
            start(
                which,
                S0 + number,
                place,
                partials[which].at[me ^ CORE ^ COLUMNS[number], place],
                core.at[number, place],
                (me ^ CORE, z),
            )

    def first_stage(which, place):
        core, diagonal, sides, _ = bufs(which)
        rows = core.shape[2]
        half, _ = halves(rows)
        to_x, to_y = (me ^ ALONG_X, z), (me ^ ALONG_Y, z)
        for number in (3, 1, 2, 0):
            view = core.at[number, place]
            wait(which, S0 + number, place, view)
            add(view, partials[which].at[me ^ COLUMNS[number], place])
            if number == 3:
                start(which, TO_X, place, view.at[0:half], diagonal.at[place, 0:half], to_x)
                if half < rows:
                    start(which, TO_Y, place, view.at[half:rows], diagonal.at[place, half:rows], to_y)
            if number == 1:
                if half < rows:
                    start(which, X_LOW, place, view.at[0:half], sides.at[0, place, 0:half], to_x)
                else:
                    start(which, X_LOW, place, view, sides.at[0, place], to_x)
            if number == 2 and half < rows:
                start(which, Y_HIGH, place, view.at[half:rows], sides.at[1, place, half:rows], to_y)

    def second_stage(which, place):
        core, diagonal, sides, _ = bufs(which)
        rows = core.shape[2]
        half, _ = halves(rows)
        view = diagonal.at[place, 0:half]
        wait(which, TO_X, place, view)
        mine = core.at[2, place, 0:half]
        add(mine, view)
        start(which, Y_LOW, place, mine, sides.at[1, place, 0:half], (me ^ ALONG_Y, z))
        if half < rows:
            view = diagonal.at[place, half:rows]
            wait(which, TO_Y, place, view)
            mine = core.at[1, place, half:rows]
            add(mine, view)
            start(which, X_HIGH, place, mine, sides.at[0, place, half:rows], (me ^ ALONG_X, z))

    def third_stage(which, place):
        core, _, sides, _ = bufs(which)
        rows = core.shape[2]
        half, _ = halves(rows)
        wait(which, X_LOW, place, sides.at[0, place, 0:half])
        wait(which, Y_LOW, place, sides.at[1, place, 0:half])
        if half < rows:
            wait(which, Y_HIGH, place, sides.at[1, place, half:rows])
            wait(which, X_HIGH, place, sides.at[0, place, half:rows])
        add(core.at[0, place], sides.at[0, place], sides.at[1, place])

    for step in range(len(order) + 4):
        if step < len(order):
            first_stage(*order[step])
        if 0 <= step - 2 < len(order):
            second_stage(*order[step - 2])
        if 0 <= step - 4:
            third_stage(*order[step - 4])

    for which in range(count):
        core, _, _, line = bufs(which)

        def send(kind, place, to, which=which, core=core, line=line):
            way = 0 if kind == Z_UP else 1
            copy(which, kind, place, core.at[0, place], line.at[way, place], (me, to)).start()

        for distance in range(depth - 1, 0, -1):
            above, below = z + distance, z - distance

            @pl.when(above < depth)
            def _(above=above):
                @pl.when(z > 0)
                def _():
                    wait(which, Z_UP, above, line.at[0, above])
                    add(core.at[0, above], line.at[0, above])

                send(Z_UP, above, z + 1)

            @pl.when(below >= 0)
            def _(below=below):
                @pl.when(z < depth - 1)
                def _():
                    wait(which, Z_DOWN, below, line.at[1, below])
                    add(core.at[0, below], line.at[1, below])

                send(Z_DOWN, below, z - 1)

    for which in range(count):
        core, _, _, line = bufs(which)
        outs[which][...] = core[0, z].astype(F32)

        @pl.when(z > 0)
        def _():
            wait(which, Z_UP, z, line.at[0, z])
            outs[which][...] += line[0, z].astype(F32)

        @pl.when(z < depth - 1)
        def _():
            wait(which, Z_DOWN, z, line.at[1, z])
            outs[which][...] += line[1, z].astype(F32)

        for distance in range(depth - 1, 0, -1):
            above, below = z + distance, z - distance

            @pl.when(above < depth)
            def _(above=above):
                copy(which, Z_UP, above, core.at[0, above], line.at[0, above], (me, z)).wait_send()

            @pl.when(below >= 0)
            def _(below=below):
                copy(which, Z_DOWN, below, core.at[0, below], line.at[1, below], (me, z)).wait_send()

    for which, kind, place, source, target in started:
        copy(which, kind, place, source, target, (me, z)).wait_send()


def scatter_all(partials, number):
    count = len(partials)
    n_mp = partials[0].shape[1]
    sems = pltpu.SemaphoreType.DMA((count, SCATTER_KINDS, n_mp))
    scratch = []
    for a in partials:
        block = a.shape[2:]
        scratch += [
            pltpu.VMEM((4, n_mp) + block, a.dtype),
            pltpu.VMEM((n_mp,) + block, a.dtype),
            pltpu.VMEM((2, n_mp) + block, a.dtype),
            pltpu.VMEM((2, n_mp) + block, a.dtype),
        ]
    return pl.pallas_call(
        functools.partial(scatter_kernel, count, n_mp),
        name="scatter",
        in_specs=[pl.BlockSpec(memory_space=pltpu.VMEM)] * count,
        out_specs=[pl.BlockSpec(memory_space=pltpu.VMEM)] * count,
        out_shape=[jax.ShapeDtypeStruct(a.shape[2:], F32) for a in partials],
        scratch_shapes=scratch + [sems, sems],
        compiler_params=pltpu.CompilerParams(
            collective_id=number, has_side_effects=True, vmem_limit_bytes=60 << 20
        ),
    )(*partials)


def blocks(local, mesh_shape):
    return lax.all_gather(local, BOTH, axis=0, tiled=False).reshape(mesh_shape + local.shape)


def gather_first(locals_, mesh_shape):
    if mesh_shape[0] == 8:
        return gather_all(locals_, *mesh_shape, number=1)
    return [blocks(local, mesh_shape) for local in locals_]


def scatter_sums(partials, number):
    if partials[0].shape[0] == 8:
        return scatter_all(partials, number)
    done = []
    for partial in partials:
        flat = partial.reshape((-1,) + partial.shape[3:])
        done.append(lax.psum_scatter(flat, BOTH, scatter_dimension=0, tiled=True).astype(F32))
    return done


def body(
    frames,
    w_qkv,
    b_qv,
    w_out,
    b_out,
    ln1_gain,
    ln1_bias,
    w_ff1,
    b_ff1,
    w_ff2,
    b_ff2,
    ln2_gain,
    ln2_bias,
    cotangent,
    clip_lengths,
    clip_slot,
):
    n_dp, n_mp = lax.axis_size("dp"), lax.axis_size("mp")
    rows, width = frames.shape
    share = b_out.shape[0]

    partner = [(m, m ^ 1) for m in range(n_mp)]
    other = lax.ppermute(frames, "mp", partner)
    packed = jnp.concatenate([w_qkv[0], w_qkv[1], w_qkv[2], w_out.T], axis=1)
    small = jnp.concatenate(
        [b_out, ln1_gain, ln1_bias, b_ff2, ln2_gain, ln2_bias, b_qv.reshape(-1).astype(F32), b_ff1.astype(F32)]
    )
    entries = small.shape[0]
    small = jnp.pad(small, (0, -entries % 1024)).reshape(-1, 128)
    mesh_shape = (n_dp, n_mp)
    w_attn, small = gather_first([packed, small], mesh_shape)
    w1, w2 = blocks(w_ff1, mesh_shape), blocks(w_ff2.T, mesh_shape)
    small = small.reshape(n_dp * n_mp, -1)[:, :entries]
    vectors = small[:, : 6 * share].reshape(n_dp * n_mp, 6, share).transpose(1, 0, 2).reshape(6, width)
    vectors = jnp.concatenate([vectors, jnp.zeros((2, width), F32)])
    ordered = small.reshape(n_dp, n_mp, -1).transpose(1, 0, 2)
    qv = ordered[:, :, 6 * share : 8 * share].reshape(n_mp, n_dp, 2, share).transpose(0, 2, 1, 3)
    qv = qv.reshape(n_mp, 2, 1, n_dp * share)
    heads_width = n_dp * share
    qv_bias = jnp.concatenate(
        [qv[:, 0], jnp.zeros((n_mp, 1, heads_width), F32), qv[:, 1], jnp.zeros((n_mp, 1, HEAD), F32)], axis=2
    )
    up_bias = ordered[:, :, 8 * share :].reshape(n_mp, 1, -1)

    index = lax.axis_index("dp") * n_mp + lax.axis_index("mp")
    slot = index // (SLOT // rows)
    half = index % (SLOT // rows)
    length = jnp.sum(jnp.where(clip_slot == slot, clip_lengths, 0))
    valid = jnp.stack([length - half * rows, length - (1 - half) * rows]).astype(jnp.int32)

    pre_one, ctx, query, keys, values = attend(valid, frames, other, w_attn, qv_bias, vectors[0:1])
    hidden, active, low, low_t = up(pre_one, vectors[1:2], vectors[2:3], w1, up_bias)
    output, grad_pre, grad_low, grad_low_t, grad_w2, grad_w1, sums, grad_up_bias = down(
        pre_one, cotangent, vectors, active, hidden, w2, w1, low_t
    )
    done_w2, done_w1 = scatter_sums([grad_w2, grad_w1], 2)
    grad_w, grad_own, grad_other, head_sums = attend_back(
        grad_low, grad_low_t, frames.T, other.T, w_attn, ctx, query, keys, values
    )
    returned = lax.ppermute(grad_other, "mp", partner)
    grad_input = grad_pre + grad_own + returned.astype(F32)

    sums = sums[:6].reshape(6, n_dp * n_mp, share).transpose(1, 0, 2).reshape(n_dp * n_mp, 6 * share)
    head_sums = jnp.concatenate(
        [head_sums[:, :, :heads_width], head_sums[:, :, 2 * heads_width : 3 * heads_width]], axis=1
    )
    head_sums = head_sums.reshape(n_mp, 2, n_dp, share).transpose(2, 0, 1, 3).reshape(n_dp * n_mp, 2 * share)
    unit_sums = grad_up_bias.reshape(n_mp, n_dp, -1).transpose(1, 0, 2).reshape(n_dp * n_mp, -1)
    small = jnp.concatenate([sums, head_sums, unit_sums], axis=1)
    small = jnp.pad(small, ((0, 0), (0, -entries % 1024))).reshape(mesh_shape + (-1, 128))
    done_w, small = scatter_sums([grad_w, small], 3)
    small = small.reshape(-1)
    (d_out_bias, d_gain1, d_shift1, d_down_bias, d_gain2, d_shift2) = [
        small[i * share : (i + 1) * share] for i in range(6)
    ]
    d_qv = small[6 * share : 8 * share].reshape(2, share)
    d_up_bias = small[8 * share : entries]
    d_qkv = jnp.stack([done_w[:, i * heads_width : (i + 1) * heads_width] for i in range(3)])
    return (
        output,
        grad_input,
        d_qkv,
        d_qv,
        done_w[:, 3 * heads_width :].T,
        d_out_bias,
        d_gain1,
        d_shift1,
        done_w1,
        d_up_bias,
        done_w2.T,
        d_down_bias,
        d_gain2,
        d_shift2,
    )


def solution(mesh):
    rows, vector, group_vector = P(BOTH, None), P(BOTH), P(("mp", "dp"))
    qkv, qv, out, up_spec = P(None, "dp", "mp"), P(None, ("mp", "dp")), P("mp", "dp"), P("dp", "mp")
    weights = (qkv, qv, out, vector, vector, vector, up_spec, group_vector, out, vector, vector, vector)
    return jax.shard_map(
        body,
        mesh=mesh,
        in_specs=(rows,) + weights + (rows, P(), P()),
        out_specs=(rows, rows) + weights,
        check_vma=False,
    )
```

```python
import functools

import jax
import jax.numpy as jnp
from jax import lax
from jax.experimental import pallas as pl
from jax.experimental.pallas import tpu as pltpu
from jax.sharding import PartitionSpec as P

HEAD = 64
SLOT = 1536
EPS = 1e-05
SCALE = 0.125
MASKED = -1e30
BOTH = ("dp", "mp")
F32 = jnp.float32
BF16 = jnp.bfloat16
MESH = pl.DeviceIdType.MESH
NN = (((1,), (0,)), ((), ()))
NT = (((1,), (1,)), ((), ()))


def mul(left, right, dims=NN):
    return lax.dot_general(left, right, dims, preferred_element_type=F32)


def lanes(shape):
    return lax.broadcasted_iota(jnp.int32, shape, 1)


def three_parts(value):
    high = value.astype(BF16).astype(F32)
    rest = value - high
    middle = rest.astype(BF16).astype(F32)
    return high, middle, rest - middle


def head_block(value, place):
    block = value[:, 128 * (place // 2) : 128 * (place // 2) + 128]
    return pltpu.roll(block, HEAD, 1) if place % 2 else block


def pair(low, high):
    return jnp.where(lanes(low.shape) < HEAD, low, pltpu.roll(high, HEAD, 1))


def norm_parts(field):
    mean = jnp.mean(field, axis=-1, keepdims=True)
    centred = field - mean
    spread = jnp.mean(centred * centred, axis=-1, keepdims=True)
    inverse = lax.rsqrt(spread + EPS)
    return centred * inverse, inverse


def norm_back(grad, scaled, inverse, gain):
    inner = grad * gain
    return inverse * (
        inner
        - jnp.mean(inner, axis=-1, keepdims=True)
        - scaled * jnp.mean(inner * scaled, axis=-1, keepdims=True)
    )


def weight(ref, first, last):
    return ref[:, 0, :, first:last].reshape(ref.shape[0] * ref.shape[2], last - first)


def attend_kernel(
    order_ref, valid_ref, own_ref, other_ref, w_ref, qv_bias_ref, out_bias_ref, pre_ref, ctx_ref, q_ref, k_ref, v_ref
):
    group, groups = pl.program_id(0), pl.num_programs(0)
    rows = own_ref.shape[0]
    bias = qv_bias_ref[0]
    projected = mul(own_ref[...], weight(w_ref, 0, 640)) + bias
    projected_other = mul(other_ref[...], weight(w_ref, 128, 640)) + bias[:, 128:]
    lane = lanes((rows, 128))
    row = lax.broadcasted_iota(jnp.int32, (rows, 128), 0)
    contexts = []
    for head in range(3):
        query = jnp.where(
            lane < HEAD, head_block(projected, head).astype(BF16).astype(F32) * SCALE, jnp.where(lane == HEAD, 1.0, 0.0)
        )
        for half, (source, shift) in enumerate(((projected, 0), (projected_other, 2))):
            mask = jnp.where(row < valid_ref[half], 0.0, MASKED)
            tail = jnp.where(lane == HEAD, mask, jnp.where(lane < HEAD + 4, 1.0, 0.0))
            keys = jnp.where(lane < HEAD, head_block(source, 3 + head - shift), tail)
            values = jnp.where(
                lane < HEAD, head_block(source, 6 + head - shift), jnp.where(lane < HEAD + 3, 1.0, 0.0)
            )
            k_ref[head, half * rows : (half + 1) * rows, :] = keys.astype(BF16)
            v_ref[head, half * rows : (half + 1) * rows, :] = values.astype(BF16)
        step = 256
        pieces = []
        for first in range(0, rows, step):
            query_here = query[first : first + step]
            scores = mul(query_here.astype(BF16), k_ref[head], NT)
            peak = jnp.max(scores, axis=1, keepdims=True)
            exps = jnp.exp(scores - peak).astype(BF16)
            mixed = mul(exps, v_ref[head])
            lane_here = lanes((step, 128))
            total = jnp.sum(jnp.where(lane_here == HEAD, mixed, 0.0), axis=1, keepdims=True)
            pieces.append(mixed / total)
            high, middle, low = three_parts(-(peak + jnp.log(total)))
            kept = jnp.where(
                lane_here == HEAD + 1,
                high,
                jnp.where(lane_here == HEAD + 2, middle, jnp.where(lane_here == HEAD + 3, low, query_here)),
            )
            q_ref[head, first : first + step, :] = kept.astype(BF16)
        contexts.append(jnp.concatenate(pieces, axis=0))
    first_half = jnp.where(lane < HEAD, 0.0, pltpu.roll(contexts[0], HEAD, 1)).astype(BF16)
    second_half = pair(contexts[1], contexts[2]).astype(BF16)
    ctx_ref[0, :, 0:128] = first_half
    ctx_ref[0, :, 128:256] = second_half
    part = mul(ctx_ref[0], weight(w_ref, 512, 768), NT)

    @pl.when(group == 0)
    def _():
        pre_ref[...] = part + (out_bias_ref[...] + own_ref[...].astype(F32))

    @pl.when(group > 0)
    def _():
        pre_ref[...] += part


def attend(order, valid, own, other, weights, qv_bias, out_bias):
    rows, width = own.shape
    groups = weights.shape[1]
    whole = lambda g, order, valid: (0, 0)
    by_group = lambda g, order, valid: (g, 0, 0)
    flops = groups * (2 * 2 * rows * width * 640 + 3 * 4 * rows * SLOT * 128)
    return pl.pallas_call(
        attend_kernel,
        name="attend",
        grid_spec=pltpu.PrefetchScalarGridSpec(
            num_scalar_prefetch=2,
            grid=(groups,),
            in_specs=[
                pl.BlockSpec((rows, width), whole),
                pl.BlockSpec((rows, width), whole),
                pl.BlockSpec(
                    (weights.shape[0], 1) + weights.shape[2:], lambda g, order, valid: (0, order[g], 0, 0)
                ),
                pl.BlockSpec((1, 1, 640), lambda g, order, valid: (order[g], 0, 0)),
                pl.BlockSpec((1, width), whole),
            ],
            out_specs=[
                pl.BlockSpec((rows, width), whole),
                pl.BlockSpec((1, rows, 256), by_group),
                pl.BlockSpec((3, rows, 128), by_group),
                pl.BlockSpec((3, SLOT, 128), by_group),
                pl.BlockSpec((3, SLOT, 128), by_group),
            ],
        ),
        out_shape=[
            jax.ShapeDtypeStruct((rows, width), F32),
            jax.ShapeDtypeStruct((groups, rows, 256), BF16),
            jax.ShapeDtypeStruct((3 * groups, rows, 128), BF16),
            jax.ShapeDtypeStruct((3 * groups, SLOT, 128), BF16),
            jax.ShapeDtypeStruct((3 * groups, SLOT, 128), BF16),
        ],
        cost_estimate=pl.CostEstimate(flops=4 * flops, bytes_accessed=24 << 20, transcendentals=12 * rows * SLOT),
        compiler_params=pltpu.CompilerParams(vmem_limit_bytes=60 << 20),
    )(order, valid, own, other, weights, qv_bias, out_bias)


def up_kernel(pre_ref, gain_ref, shift_ref, w_ref, bias_ref, hidden_ref, active_ref, low_ref, low_t_ref):
    @pl.when(pl.program_id(0) == 0)
    def _():
        scaled, _ = norm_parts(pre_ref[...])
        low = (scaled * gain_ref[...] + shift_ref[...]).astype(BF16)
        low_ref[...] = low
        low_t_ref[...] = low.T

    hidden = mul(low_ref[...], weight(w_ref, 0, w_ref.shape[3])) + bias_ref[0]
    hidden_ref[0] = hidden
    active_ref[0] = (hidden * (0.5 * (1.0 + lax.erf(hidden * 0.7071067811865476)))).astype(BF16)


def up(pre, gain, shift, weights, bias):
    rows, width = pre.shape
    groups, units = weights.shape[1], weights.shape[3]
    whole = lambda g: (0, 0)
    by_group = lambda g: (g, 0, 0)
    return pl.pallas_call(
        up_kernel,
        name="up",
        grid=(groups,),
        in_specs=[
            pl.BlockSpec((rows, width), whole),
            pl.BlockSpec((1, width), whole),
            pl.BlockSpec((1, width), whole),
            pl.BlockSpec((weights.shape[0], 1) + weights.shape[2:], lambda g: (0, g, 0, 0)),
            pl.BlockSpec((1, 1, units), by_group),
        ],
        out_specs=[
            pl.BlockSpec((1, rows, units), by_group),
            pl.BlockSpec((1, rows, units), by_group),
            pl.BlockSpec((rows, width), whole),
            pl.BlockSpec((width, rows), whole),
        ],
        out_shape=[
            jax.ShapeDtypeStruct((groups, rows, units), F32),
            jax.ShapeDtypeStruct((groups, rows, units), BF16),
            jax.ShapeDtypeStruct((rows, width), BF16),
            jax.ShapeDtypeStruct((width, rows), BF16),
        ],
        cost_estimate=pl.CostEstimate(
            flops=2 * groups * rows * width * units, bytes_accessed=24 << 20, transcendentals=groups * rows * units
        ),
        compiler_params=pltpu.CompilerParams(vmem_limit_bytes=60 << 20),
    )(pre, gain, shift, weights, bias)


def down_kernel(
    groups,
    pre_ref,
    cot_ref,
    vec_ref,
    active_ref,
    hidden_ref,
    w2_ref,
    w1_ref,
    low_t_ref,
    out_ref,
    grad_pre_ref,
    grad_low_ref,
    grad_low_t_ref,
    grad_ff_ref,
    sums_ref,
    up_bias_ref,
    total_ref,
    upper_ref,
    upper_low_ref,
    upper_low_t_ref,
):
    step = pl.program_id(0)

    @pl.when(step < groups)
    def _():
        part = mul(active_ref[0], weight(w2_ref, 0, w2_ref.shape[3]), NT)

        @pl.when(step == 0)
        def _():
            total_ref[...] = part

        @pl.when(step > 0)
        def _():
            total_ref[...] += part

    @pl.when(step == groups - 1)
    def _():
        gain_one, shift_one = vec_ref[1:2], vec_ref[2:3]
        down_bias, gain_two, shift_two = vec_ref[3:4], vec_ref[4:5], vec_ref[5:6]
        middle = norm_parts(pre_ref[...])[0] * gain_one + shift_one
        scaled, inverse = norm_parts(total_ref[...] + down_bias + middle)
        out_ref[...] = (scaled * gain_two + shift_two).astype(BF16)
        cotangent = cot_ref[...].astype(F32)
        grad = norm_back(cotangent, scaled, inverse, gain_two)
        sums_ref[4:5] = jnp.sum(cotangent * scaled, axis=0, keepdims=True)
        sums_ref[5:6] = jnp.sum(cotangent, axis=0, keepdims=True)
        sums_ref[3:4] = jnp.sum(grad, axis=0, keepdims=True)
        upper_ref[...] = grad
        low = grad.astype(BF16)
        upper_low_ref[...] = low
        upper_low_t_ref[...] = low.T

    @pl.when(step >= groups)
    def _():
        grad_active = mul(upper_low_ref[...], weight(w2_ref, 0, w2_ref.shape[3]))
        hidden = hidden_ref[0]
        cdf = 0.5 * (1.0 + lax.erf(hidden * 0.7071067811865476))
        slope = cdf + hidden * jnp.exp(-0.5 * hidden * hidden) * 0.3989422804014327
        grad_hidden = (grad_active * slope).astype(BF16)
        up_bias_ref[0] = jnp.sum(grad_hidden.astype(F32), axis=0, keepdims=True)
        part_rows = w1_ref.shape[2]
        shape = w1_ref.shape
        grad_ff_ref[:, :, :part_rows] = mul(low_t_ref[...], grad_hidden).astype(BF16).reshape(shape)
        grad_ff_ref[:, :, part_rows:] = mul(upper_low_t_ref[...], active_ref[0]).astype(BF16).reshape(shape)
        part = mul(grad_hidden, weight(w1_ref, 0, w1_ref.shape[3]), NT)

        @pl.when(step == groups)
        def _():
            total_ref[...] = part

        @pl.when(step > groups)
        def _():
            total_ref[...] += part

    @pl.when(step == 2 * groups - 1)
    def _():
        scaled, inverse = norm_parts(pre_ref[...])
        grad_middle = upper_ref[...] + total_ref[...]
        grad = norm_back(grad_middle, scaled, inverse, vec_ref[1:2])
        sums_ref[1:2] = jnp.sum(grad_middle * scaled, axis=0, keepdims=True)
        sums_ref[2:3] = jnp.sum(grad_middle, axis=0, keepdims=True)
        sums_ref[0:1] = jnp.sum(grad, axis=0, keepdims=True)
        sums_ref[6:8] = jnp.zeros_like(sums_ref[6:8])
        grad_pre_ref[...] = grad
        low = grad.astype(BF16)
        grad_low_ref[...] = low
        grad_low_t_ref[...] = low.T


def down(pre, cotangent, vectors, active, hidden, w2, w1, low_t):
    rows, width = pre.shape
    groups, units = w2.shape[1], w2.shape[3]
    whole = lambda s: (0, 0)
    both = lambda s: (lax.rem(s, groups), 0, 0)
    late = lambda s: (jnp.maximum(s - groups, 0), 0, 0)
    block = (w2.shape[0], 1) + w2.shape[2:]
    w_both = lambda s: (0, lax.rem(s, groups), 0, 0)
    w_late = lambda s: (0, jnp.maximum(s - groups, 0), 0, 0)
    return pl.pallas_call(
        functools.partial(down_kernel, groups),
        name="down",
        grid=(2 * groups,),
        in_specs=[
            pl.BlockSpec((rows, width), whole),
            pl.BlockSpec((rows, width), whole),
            pl.BlockSpec((8, width), whole),
            pl.BlockSpec((1, rows, units), both),
            pl.BlockSpec((1, rows, units), late),
            pl.BlockSpec(block, w_both),
            pl.BlockSpec(block, w_late),
            pl.BlockSpec((width, rows), whole),
        ],
        out_specs=[
            pl.BlockSpec((rows, width), whole),
            pl.BlockSpec((rows, width), whole),
            pl.BlockSpec((rows, width), whole),
            pl.BlockSpec((width, rows), whole),
            pl.BlockSpec(block[:2] + (2 * block[2],) + block[3:], w_late),
            pl.BlockSpec((8, width), whole),
            pl.BlockSpec((1, 1, units), late),
        ],
        out_shape=[
            jax.ShapeDtypeStruct((rows, width), BF16),
            jax.ShapeDtypeStruct((rows, width), F32),
            jax.ShapeDtypeStruct((rows, width), BF16),
            jax.ShapeDtypeStruct((width, rows), BF16),
            jax.ShapeDtypeStruct(w1.shape[:2] + (2 * w1.shape[2],) + w1.shape[3:], BF16),
            jax.ShapeDtypeStruct((8, width), F32),
            jax.ShapeDtypeStruct((groups, 1, units), F32),
        ],
        scratch_shapes=[
            pltpu.VMEM((rows, width), F32),
            pltpu.VMEM((rows, width), F32),
            pltpu.VMEM((rows, width), BF16),
            pltpu.VMEM((width, rows), BF16),
        ],
        cost_estimate=pl.CostEstimate(
            flops=10 * groups * rows * width * units, bytes_accessed=48 << 20, transcendentals=groups * rows * units
        ),
        compiler_params=pltpu.CompilerParams(vmem_limit_bytes=63 << 20),
    )(pre, cotangent, vectors, active, hidden, w2, w1, low_t)


def group_back(grad_ref, grad_t_ref, own_t_ref, other_t_ref, weight_of, ctx_ref, q_ref, k_ref, v_ref, after_head):
    rows = grad_ref.shape[0]
    step = 256
    grad_context = mul(grad_ref[...], weight_of(512, 768)).astype(BF16).astype(F32)
    lane = lanes((rows, 128))
    grads = []
    for head in range(3):
        place = 1 + head
        grad_head = head_block(grad_context, place)
        context = head_block(ctx_ref[0].astype(F32), place)
        delta = jnp.sum(jnp.where(lane < HEAD, grad_head * context, 0.0), axis=1, keepdims=True)
        high, middle, low = three_parts(-delta)
        tail = jnp.where(
            lane == HEAD, high, jnp.where(lane == HEAD + 1, middle, jnp.where(lane == HEAD + 2, low, 0.0))
        )
        grad_head = jnp.where(lane < HEAD, grad_head, tail).astype(BF16)
        keys_t = k_ref[head].T
        grad_query = []
        grad_keys = grad_values = None
        for first in range(0, rows, step):
            query_here = q_ref[head, first : first + step, :]
            grad_here = grad_head[first : first + step]
            weights = jnp.exp(mul(k_ref[head], query_here, NT))
            grad_scores = (weights * mul(v_ref[head], grad_here, NT)).astype(BF16)
            values_part = mul(weights.astype(BF16), grad_here)
            keys_part = mul(grad_scores, query_here)
            grad_values = values_part if grad_values is None else grad_values + values_part
            grad_keys = keys_part if grad_keys is None else grad_keys + keys_part
            grad_query.append(mul(keys_t, grad_scores))
        grad_query = jnp.concatenate(grad_query, axis=1).T * SCALE
        grads.append((grad_query, grad_keys, grad_values))
        after_head(head)
    (q0, k0, v0), (q1, k1, v1), (q2, k2, v2) = grads
    blank = jnp.zeros((rows, 128), F32)
    own = jnp.concatenate(
        [
            pair(q0, q1),
            pair(q2, k0[:rows]),
            pair(k1[:rows], k2[:rows]),
            pair(v0[:rows], v1[:rows]),
            pair(v2[:rows], blank),
        ],
        axis=1,
    )
    other = jnp.concatenate(
        [pair(blank, k0[rows:]), pair(k1[rows:], k2[rows:]), pair(v0[rows:], v1[rows:]), pair(v2[rows:], blank)],
        axis=1,
    )
    own_sum = jnp.sum(own, axis=0, keepdims=True)
    other_sum = jnp.sum(other, axis=0, keepdims=True)
    sums = [own_sum[:, 0:128]] + [
        own_sum[:, i : i + 128] + other_sum[:, i - 128 : i] for i in range(128, 640, 128)
    ]
    own, other = own.astype(BF16), other.astype(BF16)
    grad_w = mul(own_t_ref[...], own)
    grad_w_other = mul(other_t_ref[...], other)
    grad_out = mul(grad_t_ref[...], ctx_ref[0])
    columns = [
        grad_w[:, 0:128],
        grad_w[:, 128:512] + grad_w_other[:, 0:384],
        grad_w[:, 512:640] + grad_w_other[:, 384:512] + grad_out[:, 0:128],
        grad_out[:, 128:256],
    ]
    return own, other, sums, columns


def attend_back_kernel(
    grad_ref,
    grad_t_ref,
    own_t_ref,
    other_t_ref,
    w_ref,
    ctx_ref,
    q_ref,
    k_ref,
    v_ref,
    grad_w_ref,
    grad_own_ref,
    grad_other_ref,
    sums_ref,
    other_total_ref,
):
    group, groups = pl.program_id(0), pl.num_programs(0)
    own, other, sums, columns = group_back(
        grad_ref,
        grad_t_ref,
        own_t_ref,
        other_t_ref,
        functools.partial(weight, w_ref),
        ctx_ref,
        q_ref,
        k_ref,
        v_ref,
        lambda head: None,
    )
    for number, piece in enumerate(sums):
        sums_ref[0, :, 128 * number : 128 * number + 128] = piece
    shape = (grad_w_ref.shape[0], 1, grad_w_ref.shape[2])
    first = 0
    for piece in columns:
        last = first + piece.shape[1]
        grad_w_ref[:, :, :, first:last] = piece.astype(BF16).reshape(shape + (last - first,))
        first = last
    own_part = mul(own, weight(w_ref, 0, 640), NT)
    other_part = mul(other, weight(w_ref, 128, 640), NT)

    @pl.when(group == 0)
    def _():
        grad_own_ref[...] = own_part
        other_total_ref[...] = other_part

    @pl.when(group > 0)
    def _():
        grad_own_ref[...] += own_part
        other_total_ref[...] += other_part

    @pl.when(group == groups - 1)
    def _():
        grad_other_ref[...] = other_total_ref[...].astype(BF16)


def attend_back(grad, grad_t, own_t, other_t, weights, ctx, query, keys, values):
    rows, width = grad.shape
    groups = weights.shape[1]
    whole = lambda g: (0, 0)
    by_group = lambda g: (g, 0, 0)
    block = pl.BlockSpec((weights.shape[0], 1) + weights.shape[2:], lambda g: (0, g, 0, 0))
    flops = groups * (3 * 2 * rows * width * 640 + 3 * 10 * rows * SLOT * 128)
    return pl.pallas_call(
        attend_back_kernel,
        name="attend_back",
        grid=(groups,),
        in_specs=[
            pl.BlockSpec((rows, width), whole),
            pl.BlockSpec((width, rows), whole),
            pl.BlockSpec((width, rows), whole),
            pl.BlockSpec((width, rows), whole),
            block,
            pl.BlockSpec((1, rows, 256), by_group),
            pl.BlockSpec((3, rows, 128), by_group),
            pl.BlockSpec((3, SLOT, 128), by_group),
            pl.BlockSpec((3, SLOT, 128), by_group),
        ],
        out_specs=[
            block,
            pl.BlockSpec((rows, width), whole),
            pl.BlockSpec((rows, width), whole),
            pl.BlockSpec((1, 1, 640), by_group),
        ],
        out_shape=[
            jax.ShapeDtypeStruct(weights.shape, BF16),
            jax.ShapeDtypeStruct((rows, width), F32),
            jax.ShapeDtypeStruct((rows, width), BF16),
            jax.ShapeDtypeStruct((groups, 1, 640), F32),
        ],
        scratch_shapes=[pltpu.VMEM((rows, width), F32)],
        cost_estimate=pl.CostEstimate(flops=4 * flops, bytes_accessed=32 << 20, transcendentals=12 * rows * SLOT),
        compiler_params=pltpu.CompilerParams(vmem_limit_bytes=63 << 20),
    )(grad, grad_t, own_t, other_t, weights, ctx, query, keys, values)


CORE, ALONG_X, ALONG_Y = 1, 2, 4
DIAGONAL = ALONG_X | ALONG_Y
COLUMNS = (0, ALONG_X, ALONG_Y, DIAGONAL)


def meet(me, z, depth):
    barrier = pltpu.get_barrier_semaphore()
    for bit in (CORE, ALONG_X, ALONG_Y):
        pl.semaphore_signal(barrier, inc=1, device_id=(me ^ bit, z), device_id_type=MESH)

    @pl.when(z > 0)
    def _():
        pl.semaphore_signal(barrier, inc=1, device_id=(me, z - 1), device_id_type=MESH)

    @pl.when(z < depth - 1)
    def _():
        pl.semaphore_signal(barrier, inc=1, device_id=(me, z + 1), device_id_type=MESH)

    pl.semaphore_wait(barrier, 3 + (z > 0).astype(jnp.int32) + (z < depth - 1).astype(jnp.int32))


def near_first(z, depth):
    yield z, None
    for distance in range(1, depth):
        for place in (z - distance, z + distance):
            yield place, (place >= 0) & (place < depth)


def given(condition, action):
    if condition is None:
        action()
    else:
        pl.when(condition)(action)


def halves(rows):
    return (rows // 2, rows) if rows % 32 == 0 else (rows, rows)


UP, DOWN, X, Y, VIA_Y, VIA_X, C0 = range(7)
GATHER_KINDS = C0 + 4


def gather_kernel(count, depth, *refs):
    locals_, wholes = refs[:count], refs[count : 2 * count]
    send_sem, recv_sem = refs[2 * count :]
    me, z = lax.axis_index("dp"), lax.axis_index("mp")

    def copy(which, kind, place, source, target, to):
        return pltpu.make_async_remote_copy(
            src_ref=source,
            dst_ref=target,
            send_sem=send_sem.at[which, kind, place],
            recv_sem=recv_sem.at[which, kind, place],
            device_id=to,
            device_id_type=MESH,
        )

    meet(me, z, depth)

    def column(which, place, source, owner, kinds):
        whole = wholes[which]
        for kind, to, first, last in kinds:
            view = source if first == 0 and last == source.shape[0] else source.at[first:last]
            copy(which, kind, place, view, whole.at[owner, place, first:last], to).start()

    def arrived(which, kind, place, owner, first, last):
        view = wholes[which].at[owner, place, first:last]
        copy(which, kind, place, view, view, (me, z)).wait_recv()

    def first_stage(which, place, condition):
        rows = locals_[which].shape[0]

        def act():
            own = condition is None
            source = locals_[which] if own else wholes[which].at[me, place]
            if not own:
                pl.when(place < z)(lambda: arrived(which, UP, place, me, 0, rows))
                pl.when(place > z)(lambda: arrived(which, DOWN, place, me, 0, rows))
            up_from = (z < depth - 1) if own else (place < z) & (z < depth - 1)
            down_from = (z > 0) if own else (place > z) & (z > 0)
            pl.when(up_from)(lambda: column(which, place, source, me, [(UP, (me, z + 1), 0, rows)]))
            pl.when(down_from)(lambda: column(which, place, source, me, [(DOWN, (me, z - 1), 0, rows)]))
            column(
                which,
                place,
                source,
                me,
                [
                    (X, (me ^ ALONG_X, z), 0, rows),
                    (Y, (me ^ ALONG_Y, z), 0, rows),
                    (C0, (me ^ CORE, z), 0, rows),
                ],
            )

        given(condition, act)

    def second_stage(which, place, condition):
        rows = locals_[which].shape[0]
        half, _ = halves(rows)

        def act():
            arrived(which, X, place, me ^ ALONG_X, 0, rows)
            source = wholes[which].at[me ^ ALONG_X, place]
            column(
                which,
                place,
                source,
                me ^ ALONG_X,
                [(VIA_Y, (me ^ ALONG_Y, z), 0, half), (C0 + 1, (me ^ CORE, z), 0, rows)],
            )
            arrived(which, Y, place, me ^ ALONG_Y, 0, rows)
            source = wholes[which].at[me ^ ALONG_Y, place]
            kinds = [(C0 + 2, (me ^ CORE, z), 0, rows)]
            if half < rows:
                kinds = [(VIA_X, (me ^ ALONG_X, z), half, rows)] + kinds
            column(which, place, source, me ^ ALONG_Y, kinds)

        given(condition, act)

    def third_stage(which, place, condition):
        rows = locals_[which].shape[0]
        half, _ = halves(rows)

        def act():
            arrived(which, VIA_Y, place, me ^ DIAGONAL, 0, half)
            if half < rows:
                arrived(which, VIA_X, place, me ^ DIAGONAL, half, rows)
            source = wholes[which].at[me ^ DIAGONAL, place]
            column(which, place, source, me ^ DIAGONAL, [(C0 + 3, (me ^ CORE, z), 0, rows)])

        given(condition, act)

    def last_stage(which, place):
        rows = locals_[which].shape[0]
        for number, bit in enumerate(COLUMNS):
            arrived(which, C0 + number, place, me ^ CORE ^ bit, 0, rows)

    order = []
    for which in range(count):
        pltpu.make_async_copy(
            locals_[which], wholes[which].at[me, z], send_sem.at[which, GATHER_KINDS, 0]
        ).start()
        order += [(which,) + item for item in near_first(z, depth)]
    lag = len(order) // count
    for step in range(len(order) + 2 * lag):
        if step < len(order):
            first_stage(*order[step])
        if 0 <= step - lag < len(order):
            second_stage(*order[step - lag])
        if 0 <= step - 2 * lag:
            third_stage(*order[step - 2 * lag])
    for which in range(count):
        rows = locals_[which].shape[0]
        half, _ = halves(rows)
        for place in range(depth):
            last_stage(which, place)
        for place, condition in near_first(z, depth):

            def sent(which=which, place=place, own=condition is None):
                whole = wholes[which].at[me, place]
                pieces = [(X, 0, rows), (Y, 0, rows), (VIA_Y, 0, half)] + [(C0 + n, 0, rows) for n in range(4)]
                if half < rows:
                    pieces.append((VIA_X, half, rows))
                for kind, first, last in pieces:
                    view = whole.at[first:last]
                    copy(which, kind, place, view, view, (me, z)).wait_send()
                up_from = (z < depth - 1) if own else (place < z) & (z < depth - 1)
                down_from = (z > 0) if own else (place > z) & (z > 0)
                pl.when(up_from)(lambda: copy(which, UP, place, whole, whole, (me, z)).wait_send())
                pl.when(down_from)(lambda: copy(which, DOWN, place, whole, whole, (me, z)).wait_send())

            given(condition, sent)
        pltpu.make_async_copy(
            locals_[which], wholes[which].at[me, z], send_sem.at[which, GATHER_KINDS, 0]
        ).wait()


def gather_all(locals_, n_dp, n_mp, number):
    count = len(locals_)
    sems = pltpu.SemaphoreType.DMA((count, GATHER_KINDS + 1, n_mp))
    return pl.pallas_call(
        functools.partial(gather_kernel, count, n_mp),
        name="gather",
        in_specs=[pl.BlockSpec(memory_space=pltpu.VMEM)] * count,
        out_specs=[pl.BlockSpec(memory_space=pl.ANY)] * count,
        out_shape=[jax.ShapeDtypeStruct((n_dp, n_mp) + a.shape, a.dtype) for a in locals_],
        scratch_shapes=[sems, sems],
        compiler_params=pltpu.CompilerParams(collective_id=number, has_side_effects=True),
    )(*locals_)


TO_X, TO_Y, X_LOW, X_HIGH, Y_LOW, Y_HIGH, Z_UP, Z_DOWN, S0 = range(9)
SCATTER_KINDS = S0 + 4


class Reduction:
    def __init__(self, which, me, z, depth, rows, bufs, send_sem, recv_sem):
        self.which, self.me, self.z, self.depth, self.rows = which, me, z, depth, rows
        self.half = halves(rows)[0]
        self.core, self.diagonal, self.sides, self.line = bufs
        self.send_sem, self.recv_sem = send_sem, recv_sem

    def copy(self, kind, place, source, target, to):
        return pltpu.make_async_remote_copy(
            src_ref=source,
            dst_ref=target,
            send_sem=self.send_sem.at[self.which, kind, place],
            recv_sem=self.recv_sem.at[self.which, kind, place],
            device_id=to,
            device_id_type=MESH,
        )

    def start(self, kind, place, source, target, bit):
        self.copy(kind, place, source, target, (self.me ^ bit, self.z)).start()

    def wait(self, kind, place, view):
        self.copy(kind, place, view, view, (self.me, self.z)).wait_recv()

    def add(self, target, *others):
        total = target[...].astype(F32)
        for other in others:
            total = total + other[...].astype(F32)
        target[...] = total.astype(target.dtype)

    def to_core(self, place, theirs):
        for number in (3, 1, 2, 0):
            self.start(S0 + number, place, theirs(number), self.core.at[number, place], CORE)

    def first(self, place, mine):
        half, rows = self.half, self.rows
        for number in (3, 1, 2, 0):
            view = self.core.at[number, place]
            self.wait(S0 + number, place, view)
            self.add(view, mine(number))
            if number == 3:
                self.start(TO_X, place, view.at[0:half], self.diagonal.at[place, 0:half], ALONG_X)
                if half < rows:
                    self.start(TO_Y, place, view.at[half:rows], self.diagonal.at[place, half:rows], ALONG_Y)
            if number == 1:
                self.start(X_LOW, place, view.at[0:half], self.sides.at[0, place, 0:half], ALONG_X)
            if number == 2 and half < rows:
                self.start(Y_HIGH, place, view.at[half:rows], self.sides.at[1, place, half:rows], ALONG_Y)

    def second(self, place):
        half, rows = self.half, self.rows
        view = self.diagonal.at[place, 0:half]
        self.wait(TO_X, place, view)
        mine = self.core.at[2, place, 0:half]
        self.add(mine, view)
        self.start(Y_LOW, place, mine, self.sides.at[1, place, 0:half], ALONG_Y)
        if half < rows:
            view = self.diagonal.at[place, half:rows]
            self.wait(TO_Y, place, view)
            mine = self.core.at[1, place, half:rows]
            self.add(mine, view)
            self.start(X_HIGH, place, mine, self.sides.at[0, place, half:rows], ALONG_X)

    def third(self, place):
        half, rows = self.half, self.rows
        self.wait(X_LOW, place, self.sides.at[0, place, 0:half])
        self.wait(Y_LOW, place, self.sides.at[1, place, 0:half])
        if half < rows:
            self.wait(Y_HIGH, place, self.sides.at[1, place, half:rows])
            self.wait(X_HIGH, place, self.sides.at[0, place, half:rows])
        self.add(self.core.at[0, place], self.sides.at[0, place], self.sides.at[1, place])

    def along(self, kind, place):
        way = 0 if kind == Z_UP else 1
        to = (self.me, self.z + 1 if kind == Z_UP else self.z - 1)
        return self.copy(kind, place, self.core.at[0, place], self.line.at[way, place], to)

    def chain(self, distance):
        z, depth = self.z, self.depth
        above, below = z + distance, z - distance

        @pl.when(above < depth)
        def _():
            @pl.when(z > 0)
            def _():
                self.wait(Z_UP, above, self.line.at[0, above])
                self.add(self.core.at[0, above], self.line.at[0, above])

            self.along(Z_UP, above).start()

        @pl.when(below >= 0)
        def _():
            @pl.when(z < depth - 1)
            def _():
                self.wait(Z_DOWN, below, self.line.at[1, below])
                self.add(self.core.at[0, below], self.line.at[1, below])

            self.along(Z_DOWN, below).start()

    def finish(self, out):
        z, depth = self.z, self.depth
        out[...] = self.core[0, z].astype(F32)

        @pl.when(z > 0)
        def _():
            self.wait(Z_UP, z, self.line.at[0, z])
            out[...] += self.line[0, z].astype(F32)

        @pl.when(z < depth - 1)
        def _():
            self.wait(Z_DOWN, z, self.line.at[1, z])
            out[...] += self.line[1, z].astype(F32)

    def drain(self):
        half, rows = self.half, self.rows
        pieces = [(S0 + number, 0, rows) for number in range(4)]
        pieces += [(TO_X, 0, half), (X_LOW, 0, half), (Y_LOW, 0, half)]
        if half < rows:
            pieces += [(TO_Y, half, rows), (Y_HIGH, half, rows), (X_HIGH, half, rows)]
        for place in range(self.depth):
            for kind, first, last in pieces:
                view = self.core.at[0, place, first:last]
                self.copy(kind, place, view, view, (self.me, self.z)).wait_send()
        for distance in range(1, self.depth):
            above, below = self.z + distance, self.z - distance
            pl.when(above < self.depth)(lambda above=above: self.along(Z_UP, above).wait_send())
            pl.when(below >= 0)(lambda below=below: self.along(Z_DOWN, below).wait_send())


def linked_back_kernel(
    depth,
    grad_ref,
    grad_t_ref,
    own_t_ref,
    other_t_ref,
    early_ref,
    w_hbm,
    ff_hbm,
    ctx_ref,
    q_ref,
    k_ref,
    v_ref,
    ff_out,
    w_out,
    small_out,
    grad_own_ref,
    w_buf,
    w_sem,
    grad_w,
    grad_small,
    ff_mine,
    ff_sem,
    sent,
    received,
    pair_send,
    pair_recv,
    *refs,
):
    send_sem, recv_sem = refs[-2:]
    me, z = lax.axis_index("dp"), lax.axis_index("mp")
    step = pl.program_id(0)
    rows = grad_ref.shape[0]
    part = w_buf.shape[2]
    group_at = lambda s: z ^ (depth - 1 - s)
    group = group_at(step)
    arrays = [(2 * part, refs[0:4]), (part, refs[4:8]), (8, refs[8:12])]
    ff, w, small = [
        Reduction(i, me, z, depth, size, bufs, send_sem, recv_sem) for i, (size, bufs) in enumerate(arrays)
    ]
    places = [depth - 1, 0] + list(range(1, depth - 1))[::-1]

    def load_w(s):
        return pltpu.make_async_copy(w_hbm.at[:, group_at(s)], w_buf.at[group_at(s)], w_sem.at[s])

    def load_ff(turn, number):
        source = ff_hbm.at[me ^ COLUMNS[number], places[turn]]
        return pltpu.make_async_copy(source, ff_mine.at[turn % 2, number], ff_sem.at[turn % 2, number])

    def exchange(place):
        return pltpu.make_async_remote_copy(
            src_ref=sent.at[place],
            dst_ref=received.at[place],
            send_sem=pair_send.at[place],
            recv_sem=pair_recv.at[place],
            device_id=(me, z ^ 1),
            device_id_type=MESH,
        )

    @pl.when(step == 0)
    def _():
        for s in range(depth):
            load_w(s).start()
        for turn in range(2):
            for number in range(4):
                load_ff(turn, number).start()
        meet(me, z, depth)
        for place in places:
            ff.to_core(place, lambda number, place=place: ff_hbm.at[me ^ CORE ^ COLUMNS[number], place])

    for s in range(depth):
        pl.when(step == s)(lambda s=s: load_w(s).wait())

    def ff_first(turn):
        for number in range(4):
            load_ff(turn, number).wait()
        ff.first(places[turn], lambda number: ff_mine.at[turn % 2, number])
        if turn + 2 < depth:
            for number in range(4):
                load_ff(turn + 2, number).start()

    def ff_work(slot):
        if slot < depth:
            ff_first(slot)
        if 0 <= slot - 2 < depth:
            ff.second(places[slot - 2])
        if 0 <= slot - 6 < depth:
            ff.third(places[slot - 6])
        last = 6 + depth - 1
        if last <= slot < last + depth - 1:
            ff.chain(depth - 1 - (slot - last))

    def w_first(s):
        place = group_at(s)
        w.first(place, lambda number: grad_w.at[s, me ^ COLUMNS[number]])
        small.first(place, lambda number: grad_small.at[s, me ^ COLUMNS[number]])

    def w_second(s):
        w.second(group_at(s))
        small.second(group_at(s))

    def w_third(s):
        w.third(group_at(s))
        small.third(group_at(s))

    def take(place):
        exchange(place).wait_recv()
        block = received[place]
        low = lanes((rows, 128)) < HEAD
        zero = jnp.zeros((rows, 128), BF16)
        ends = block[:, 0:128]
        other = jnp.concatenate([jnp.where(low, zero, ends), block[:, 128:384], jnp.where(low, ends, zero)], axis=1)
        view = w_buf.at[place]
        grad_own_ref[...] += mul(other, view[:, :, 128:640].reshape(part * 8, 512), NT)

    def after_head(head):
        for s in range(depth):
            slot = 3 * s + head
            pl.when(step == s)(lambda slot=slot: ff_work(slot))

        @pl.when(step > 0)
        def _():
            [w_first, w_second, w_third][head](step - 1)

    own, other, sums, columns = group_back(
        grad_ref,
        grad_t_ref,
        own_t_ref,
        other_t_ref,
        lambda first, last: w_buf[group, :, :, first:last].reshape(part * 8, last - first),
        ctx_ref,
        q_ref,
        k_ref,
        v_ref,
        after_head,
    )
    sent[group, :, 0:128] = other[:, 0:128] + other[:, 384:512]
    sent[group, :, 128:384] = other[:, 128:384]
    exchange(group).start()
    first = 0
    for piece in columns:
        last = first + piece.shape[1]
        grad_w[step, :, :, first:last] = piece.astype(BF16).reshape(8, part, last - first)
        first = last
    row = lax.broadcasted_iota(jnp.int32, (8, 128), 0)
    late = jnp.zeros((8, 128), F32)
    for number, piece in enumerate(sums):
        late = jnp.where(row == number, piece, late)
    for owner in range(8):
        grad_small[step, owner] = early_ref[owner, group] + late
    w.to_core(group, lambda number: grad_w.at[step, me ^ CORE ^ COLUMNS[number]])
    small.to_core(group, lambda number: grad_small.at[step, me ^ CORE ^ COLUMNS[number]])
    own_part = mul(own, w_buf[group, :, :, 0:640].reshape(part * 8, 640), NT)

    @pl.when(step == 0)
    def _():
        grad_own_ref[...] = own_part

    @pl.when(step > 0)
    def _():
        grad_own_ref[...] += own_part
        take(group_at(step - 1) ^ 1)

    @pl.when(step == depth - 1)
    def _():
        w_first(depth - 1)
        for distance in range(depth - 1, 0, -1):
            w.chain(distance)
            small.chain(distance)
            if distance == depth - 1:
                w_second(depth - 1)
        ff.finish(ff_out)
        w_third(depth - 1)
        w.finish(w_out)
        small.finish(small_out)
        take(group ^ 1)
        for array in (ff, w, small):
            array.drain()
        for place in range(depth):
            exchange(place).wait_send()


def linked_back(grad, grad_t, own_t, other_t, early, weights, grad_ff, ctx, query, keys, values):
    rows, width = grad.shape
    n_dp, groups, part = weights.shape[:3]
    whole = pl.BlockSpec(memory_space=pltpu.VMEM)
    anywhere = pl.BlockSpec(memory_space=pl.ANY)
    by_group = lambda g: (groups - 1 - g, 0, 0)
    flops = groups * (3 * 2 * rows * width * 640 + 3 * 10 * rows * SLOT * 128)
    scratch = []
    for size, columns, kind in ((2 * part, width, BF16), (part, width, BF16), (8, 128, F32)):
        block = (size, columns)
        scratch += [pltpu.VMEM((lead, groups) + block, kind) for lead in (4,)]
        scratch += [pltpu.VMEM((groups,) + block, kind)]
        scratch += [pltpu.VMEM((2, groups) + block, kind)] * 2
    sems = pltpu.SemaphoreType.DMA((3, SCATTER_KINDS, groups))
    pairs = pltpu.SemaphoreType.DMA((groups,))
    return pl.pallas_call(
        functools.partial(linked_back_kernel, groups),
        name="linked_back",
        grid=(groups,),
        in_specs=[whole] * 5
        + [anywhere] * 2
        + [
            pl.BlockSpec((1, rows, 256), by_group),
            pl.BlockSpec((3, rows, 128), by_group),
            pl.BlockSpec((3, SLOT, 128), by_group),
            pl.BlockSpec((3, SLOT, 128), by_group),
        ],
        out_specs=[whole] * 4,
        out_shape=[
            jax.ShapeDtypeStruct((2 * part, width), F32),
            jax.ShapeDtypeStruct((part, width), F32),
            jax.ShapeDtypeStruct((8, 128), F32),
            jax.ShapeDtypeStruct((rows, width), F32),
        ],
        scratch_shapes=[
            pltpu.VMEM((groups, n_dp, part, width), BF16),
            pltpu.SemaphoreType.DMA((groups,)),
            pltpu.VMEM((groups, n_dp, part, width), BF16),
            pltpu.VMEM((groups, n_dp, 8, 128), F32),
            pltpu.VMEM((2, 4, 2 * part, width), BF16),
            pltpu.SemaphoreType.DMA((2, 4)),
            pltpu.VMEM((groups, rows, 384), BF16),
            pltpu.VMEM((groups, rows, 384), BF16),
            pairs,
            pairs,
        ]
        + scratch
        + [sems, sems],
        cost_estimate=pl.CostEstimate(flops=4 * flops, bytes_accessed=48 << 20, transcendentals=12 * rows * SLOT),
        compiler_params=pltpu.CompilerParams(
            collective_id=2, has_side_effects=True, vmem_limit_bytes=67043328
        ),
    )(grad, grad_t, own_t, other_t, early, weights, grad_ff, ctx, query, keys, values)


def blocks(local, mesh_shape):
    return lax.all_gather(local, BOTH, axis=0, tiled=False).reshape(mesh_shape + local.shape)


def gather_first(locals_, mesh_shape):
    if mesh_shape[0] == 8:
        return gather_all(locals_, *mesh_shape, number=1)
    return [blocks(local, mesh_shape) for local in locals_]


def scatter_sums(partial):
    flat = partial.reshape((-1,) + partial.shape[3:])
    return lax.psum_scatter(flat, BOTH, scatter_dimension=0, tiled=True).astype(F32)


def body(
    frames,
    w_qkv,
    b_qv,
    w_out,
    b_out,
    ln1_gain,
    ln1_bias,
    w_ff1,
    b_ff1,
    w_ff2,
    b_ff2,
    ln2_gain,
    ln2_bias,
    cotangent,
    clip_lengths,
    clip_slot,
):
    n_dp, n_mp = lax.axis_size("dp"), lax.axis_size("mp")
    rows, width = frames.shape
    share = b_out.shape[0]

    partner = [(m, m ^ 1) for m in range(n_mp)]
    other = lax.ppermute(frames, "mp", partner)
    packed = jnp.concatenate([w_qkv[0], w_qkv[1], w_qkv[2], w_out.T], axis=1)
    small = jnp.concatenate(
        [b_out, ln1_gain, ln1_bias, b_ff2, ln2_gain, ln2_bias, b_qv.reshape(-1).astype(F32), b_ff1.astype(F32)]
    )
    entries = small.shape[0]
    small = jnp.pad(small, (0, -entries % 1024)).reshape(-1, 128)
    mesh_shape = (n_dp, n_mp)
    w_attn, small = gather_first([packed, small], mesh_shape)
    w1, w2 = blocks(w_ff1, mesh_shape), blocks(w_ff2.T, mesh_shape)
    small = small.reshape(n_dp * n_mp, -1)[:, :entries]
    vectors = small[:, : 6 * share].reshape(n_dp * n_mp, 6, share).transpose(1, 0, 2).reshape(6, width)
    vectors = jnp.concatenate([vectors, jnp.zeros((2, width), F32)])
    ordered = small.reshape(n_dp, n_mp, -1).transpose(1, 0, 2)
    qv = ordered[:, :, 6 * share : 8 * share].reshape(n_mp, n_dp, 2, share).transpose(0, 2, 1, 3)
    qv = qv.reshape(n_mp, 2, 1, n_dp * share)
    heads_width = n_dp * share
    qv_bias = jnp.concatenate(
        [qv[:, 0], jnp.zeros((n_mp, 1, heads_width), F32), qv[:, 1], jnp.zeros((n_mp, 1, HEAD), F32)], axis=2
    )
    up_bias = ordered[:, :, 8 * share :].reshape(n_mp, 1, -1)

    index = lax.axis_index("dp") * n_mp + lax.axis_index("mp")
    slot = index // (SLOT // rows)
    half = index % (SLOT // rows)
    length = jnp.sum(jnp.where(clip_slot == slot, clip_lengths, 0))
    valid = jnp.stack([length - half * rows, length - (1 - half) * rows]).astype(jnp.int32)

    linked = n_dp == 8
    places = jnp.arange(n_mp, dtype=jnp.int32)
    order = (lax.axis_index("mp") ^ places) if linked else places
    pre_one, ctx, query, keys, values = attend(order, valid, frames, other, w_attn, qv_bias, vectors[0:1])
    hidden, active, low, low_t = up(pre_one, vectors[1:2], vectors[2:3], w1, up_bias)
    output, grad_pre, grad_low, grad_low_t, grad_ff, sums, grad_up_bias = down(
        pre_one, cotangent, vectors, active, hidden, w2, w1, low_t
    )
    sums = sums[:6].reshape(6, n_dp * n_mp, share).transpose(1, 0, 2).reshape(n_dp * n_mp, 6 * share)
    unit_sums = grad_up_bias.reshape(n_mp, n_dp, -1).transpose(1, 0, 2).reshape(n_dp * n_mp, -1)
    early = jnp.concatenate([sums, unit_sums], axis=1)
    entries = early.shape[1]
    early = jnp.pad(early, ((0, 0), (0, -entries % 128))).reshape(mesh_shape + (-1, 128))
    early = jnp.pad(early, ((0, 0), (0, 0), (5, 3 - early.shape[2]), (0, 0)))
    kept = (ctx, query, keys, values)
    if linked:
        done_ff, done_w, small, grad_own = linked_back(
            grad_low, grad_low_t, frames.T, other.T, early, w_attn, grad_ff, *kept
        )
        grad_input = grad_pre + grad_own
    else:
        grad_w, grad_own, grad_other, head_sums = attend_back(
            grad_low, grad_low_t, frames.T, other.T, w_attn, *kept
        )
        grad_input = grad_pre + grad_own + lax.ppermute(grad_other, "mp", partner).astype(F32)
        done_ff, done_w = scatter_sums(grad_ff), scatter_sums(grad_w)
        small = scatter_sums(early + jnp.pad(head_sums.reshape(1, n_mp, 5, 128), ((0, 0), (0, 0), (0, 3), (0, 0))))
    part = w_ff1.shape[0]
    small = small.reshape(-1)
    (d_out_bias, d_gain1, d_shift1, d_down_bias, d_gain2, d_shift2) = [
        small[640 + i * share : 640 + (i + 1) * share] for i in range(6)
    ]
    d_up_bias = small[640 + 6 * share : 640 + entries]
    d_qv = jnp.stack(
        [
            lax.dynamic_slice(small, (first + lax.axis_index("dp") * share,), (share,))
            for first in (0, 2 * heads_width)
        ]
    )
    d_qkv = jnp.stack([done_w[:, i * heads_width : (i + 1) * heads_width] for i in range(3)])
    done_w1, done_w2 = done_ff[:part], done_ff[part:]
    return (
        output,
        grad_input,
        d_qkv,
        d_qv,
        done_w[:, 3 * heads_width :].T,
        d_out_bias,
        d_gain1,
        d_shift1,
        done_w1,
        d_up_bias,
        done_w2.T,
        d_down_bias,
        d_gain2,
        d_shift2,
    )


def solution(mesh):
    rows, vector, group_vector = P(BOTH, None), P(BOTH), P(("mp", "dp"))
    qkv, qv, out, up_spec = P(None, "dp", "mp"), P(None, ("mp", "dp")), P("mp", "dp"), P("dp", "mp")
    weights = (qkv, qv, out, vector, vector, vector, up_spec, group_vector, out, vector, vector, vector)
    return jax.shard_map(
        body,
        mesh=mesh,
        in_specs=(rows,) + weights + (rows, P(), P()),
        out_specs=(rows, rows) + weights,
        check_vma=False,
    )
```

```python
import functools

import jax
import jax.numpy as jnp
from jax import lax
from jax.experimental import pallas as pl
from jax.experimental.pallas import tpu as pltpu
from jax.sharding import PartitionSpec as P

HEAD = 64
SLOT = 1536
EPS = 1e-05
SCALE = 0.125
MASKED = -1e30
BOTH = ("dp", "mp")
F32 = jnp.float32
BF16 = jnp.bfloat16
MESH = pl.DeviceIdType.MESH
NN = (((1,), (0,)), ((), ()))
NT = (((1,), (1,)), ((), ()))


def mul(left, right, dims=NN):
    return lax.dot_general(left, right, dims, preferred_element_type=F32)


def lanes(shape):
    return lax.broadcasted_iota(jnp.int32, shape, 1)


def three_parts(value):
    high = value.astype(BF16).astype(F32)
    rest = value - high
    middle = rest.astype(BF16).astype(F32)
    return high, middle, rest - middle


def head_block(value, place):
    block = value[:, 128 * (place // 2) : 128 * (place // 2) + 128]
    return pltpu.roll(block, HEAD, 1) if place % 2 else block


def pair(low, high):
    return jnp.where(lanes(low.shape) < HEAD, low, pltpu.roll(high, HEAD, 1))


def norm_parts(field):
    mean = jnp.mean(field, axis=-1, keepdims=True)
    centred = field - mean
    spread = jnp.mean(centred * centred, axis=-1, keepdims=True)
    inverse = lax.rsqrt(spread + EPS)
    return centred * inverse, inverse


def norm_back(grad, scaled, inverse, gain):
    inner = grad * gain
    return inverse * (
        inner
        - jnp.mean(inner, axis=-1, keepdims=True)
        - scaled * jnp.mean(inner * scaled, axis=-1, keepdims=True)
    )


def weight(ref, first, last):
    return ref[:, 0, :, first:last].reshape(ref.shape[0] * ref.shape[2], last - first)


def attend_kernel(
    order_ref, valid_ref, own_ref, other_ref, w_ref, qv_bias_ref, out_bias_ref, pre_ref, ctx_ref, q_ref, k_ref, v_ref
):
    group, groups = pl.program_id(0), pl.num_programs(0)
    rows = own_ref.shape[0]
    bias = qv_bias_ref[0]
    projected = mul(own_ref[...], weight(w_ref, 0, 640)) + bias
    projected_other = mul(other_ref[...], weight(w_ref, 128, 640)) + bias[:, 128:]
    lane = lanes((rows, 128))
    row = lax.broadcasted_iota(jnp.int32, (rows, 128), 0)
    contexts = []
    for head in range(3):
        query = jnp.where(
            lane < HEAD, head_block(projected, head).astype(BF16).astype(F32) * SCALE, jnp.where(lane == HEAD, 1.0, 0.0)
        )
        for half, (source, shift) in enumerate(((projected, 0), (projected_other, 2))):
            mask = jnp.where(row < valid_ref[half], 0.0, MASKED)
            tail = jnp.where(lane == HEAD, mask, jnp.where(lane < HEAD + 4, 1.0, 0.0))
            keys = jnp.where(lane < HEAD, head_block(source, 3 + head - shift), tail)
            values = jnp.where(
                lane < HEAD, head_block(source, 6 + head - shift), jnp.where(lane < HEAD + 3, 1.0, 0.0)
            )
            k_ref[head, half * rows : (half + 1) * rows, :] = keys.astype(BF16)
            v_ref[head, half * rows : (half + 1) * rows, :] = values.astype(BF16)
        step = 256
        pieces = []
        for first in range(0, rows, step):
            query_here = query[first : first + step]
            scores = mul(query_here.astype(BF16), k_ref[head], NT)
            peak = jnp.max(scores, axis=1, keepdims=True)
            exps = jnp.exp(scores - peak).astype(BF16)
            mixed = mul(exps, v_ref[head])
            lane_here = lanes((step, 128))
            total = jnp.sum(jnp.where(lane_here == HEAD, mixed, 0.0), axis=1, keepdims=True)
            pieces.append(mixed / total)
            high, middle, low = three_parts(-(peak + jnp.log(total)))
            kept = jnp.where(
                lane_here == HEAD + 1,
                high,
                jnp.where(lane_here == HEAD + 2, middle, jnp.where(lane_here == HEAD + 3, low, query_here)),
            )
            q_ref[head, first : first + step, :] = kept.astype(BF16)
        contexts.append(jnp.concatenate(pieces, axis=0))
    first_half = jnp.where(lane < HEAD, 0.0, pltpu.roll(contexts[0], HEAD, 1)).astype(BF16)
    second_half = pair(contexts[1], contexts[2]).astype(BF16)
    ctx_ref[0, :, 0:128] = first_half
    ctx_ref[0, :, 128:256] = second_half
    part = mul(ctx_ref[0], weight(w_ref, 512, 768), NT)

    @pl.when(group == 0)
    def _():
        pre_ref[...] = part + (out_bias_ref[...] + own_ref[...].astype(F32))

    @pl.when(group > 0)
    def _():
        pre_ref[...] += part


def attend(order, valid, own, other, weights, qv_bias, out_bias):
    rows, width = own.shape
    groups = weights.shape[1]
    whole = lambda g, order, valid: (0, 0)
    by_group = lambda g, order, valid: (g, 0, 0)
    flops = groups * (2 * 2 * rows * width * 640 + 3 * 4 * rows * SLOT * 128)
    return pl.pallas_call(
        attend_kernel,
        name="attend",
        grid_spec=pltpu.PrefetchScalarGridSpec(
            num_scalar_prefetch=2,
            grid=(groups,),
            in_specs=[
                pl.BlockSpec((rows, width), whole),
                pl.BlockSpec((rows, width), whole),
                pl.BlockSpec(
                    (weights.shape[0], 1) + weights.shape[2:], lambda g, order, valid: (0, order[g], 0, 0)
                ),
                pl.BlockSpec((1, 1, 640), lambda g, order, valid: (order[g], 0, 0)),
                pl.BlockSpec((1, width), whole),
            ],
            out_specs=[
                pl.BlockSpec((rows, width), whole),
                pl.BlockSpec((1, rows, 256), by_group),
                pl.BlockSpec((3, rows, 128), by_group),
                pl.BlockSpec((3, SLOT, 128), by_group),
                pl.BlockSpec((3, SLOT, 128), by_group),
            ],
        ),
        out_shape=[
            jax.ShapeDtypeStruct((rows, width), F32),
            jax.ShapeDtypeStruct((groups, rows, 256), BF16),
            jax.ShapeDtypeStruct((3 * groups, rows, 128), BF16),
            jax.ShapeDtypeStruct((3 * groups, SLOT, 128), BF16),
            jax.ShapeDtypeStruct((3 * groups, SLOT, 128), BF16),
        ],
        cost_estimate=pl.CostEstimate(flops=4 * flops, bytes_accessed=24 << 20, transcendentals=12 * rows * SLOT),
        compiler_params=pltpu.CompilerParams(vmem_limit_bytes=60 << 20),
    )(order, valid, own, other, weights, qv_bias, out_bias)


def up_kernel(pre_ref, gain_ref, shift_ref, w_ref, bias_ref, hidden_ref, active_ref, low_ref, low_t_ref):
    @pl.when(pl.program_id(0) == 0)
    def _():
        scaled, _ = norm_parts(pre_ref[...])
        low = (scaled * gain_ref[...] + shift_ref[...]).astype(BF16)
        low_ref[...] = low
        low_t_ref[...] = low.T

    hidden = mul(low_ref[...], weight(w_ref, 0, w_ref.shape[3])) + bias_ref[0]
    hidden_ref[0] = hidden
    active_ref[0] = (hidden * (0.5 * (1.0 + lax.erf(hidden * 0.7071067811865476)))).astype(BF16)


def up(pre, gain, shift, weights, bias):
    rows, width = pre.shape
    groups, units = weights.shape[1], weights.shape[3]
    whole = lambda g: (0, 0)
    by_group = lambda g: (g, 0, 0)
    return pl.pallas_call(
        up_kernel,
        name="up",
        grid=(groups,),
        in_specs=[
            pl.BlockSpec((rows, width), whole),
            pl.BlockSpec((1, width), whole),
            pl.BlockSpec((1, width), whole),
            pl.BlockSpec((weights.shape[0], 1) + weights.shape[2:], lambda g: (0, g, 0, 0)),
            pl.BlockSpec((1, 1, units), by_group),
        ],
        out_specs=[
            pl.BlockSpec((1, rows, units), by_group),
            pl.BlockSpec((1, rows, units), by_group),
            pl.BlockSpec((rows, width), whole),
            pl.BlockSpec((width, rows), whole),
        ],
        out_shape=[
            jax.ShapeDtypeStruct((groups, rows, units), F32),
            jax.ShapeDtypeStruct((groups, rows, units), BF16),
            jax.ShapeDtypeStruct((rows, width), BF16),
            jax.ShapeDtypeStruct((width, rows), BF16),
        ],
        cost_estimate=pl.CostEstimate(
            flops=2 * groups * rows * width * units, bytes_accessed=24 << 20, transcendentals=groups * rows * units
        ),
        compiler_params=pltpu.CompilerParams(vmem_limit_bytes=60 << 20),
    )(pre, gain, shift, weights, bias)


def down_kernel(
    groups,
    pre_ref,
    cot_ref,
    vec_ref,
    active_ref,
    hidden_ref,
    w2_ref,
    w1_ref,
    low_t_ref,
    out_ref,
    grad_pre_ref,
    grad_low_ref,
    grad_low_t_ref,
    grad_ff_ref,
    sums_ref,
    up_bias_ref,
    total_ref,
    upper_ref,
    upper_low_ref,
    upper_low_t_ref,
):
    step = pl.program_id(0)

    @pl.when(step < groups)
    def _():
        part = mul(active_ref[0], weight(w2_ref, 0, w2_ref.shape[3]), NT)

        @pl.when(step == 0)
        def _():
            total_ref[...] = part

        @pl.when(step > 0)
        def _():
            total_ref[...] += part

    @pl.when(step == groups - 1)
    def _():
        gain_one, shift_one = vec_ref[1:2], vec_ref[2:3]
        down_bias, gain_two, shift_two = vec_ref[3:4], vec_ref[4:5], vec_ref[5:6]
        middle = norm_parts(pre_ref[...])[0] * gain_one + shift_one
        scaled, inverse = norm_parts(total_ref[...] + down_bias + middle)
        out_ref[...] = (scaled * gain_two + shift_two).astype(BF16)
        cotangent = cot_ref[...].astype(F32)
        grad = norm_back(cotangent, scaled, inverse, gain_two)
        sums_ref[4:5] = jnp.sum(cotangent * scaled, axis=0, keepdims=True)
        sums_ref[5:6] = jnp.sum(cotangent, axis=0, keepdims=True)
        sums_ref[3:4] = jnp.sum(grad, axis=0, keepdims=True)
        upper_ref[...] = grad
        low = grad.astype(BF16)
        upper_low_ref[...] = low
        upper_low_t_ref[...] = low.T

    @pl.when(step >= groups)
    def _():
        grad_active = mul(upper_low_ref[...], weight(w2_ref, 0, w2_ref.shape[3]))
        hidden = hidden_ref[0]
        cdf = 0.5 * (1.0 + lax.erf(hidden * 0.7071067811865476))
        slope = cdf + hidden * jnp.exp(-0.5 * hidden * hidden) * 0.3989422804014327
        grad_hidden = (grad_active * slope).astype(BF16)
        up_bias_ref[0] = jnp.sum(grad_hidden.astype(F32), axis=0, keepdims=True)
        part_rows = w1_ref.shape[2]
        shape = w1_ref.shape
        grad_ff_ref[:, :, :part_rows] = mul(low_t_ref[...], grad_hidden).astype(BF16).reshape(shape)
        grad_ff_ref[:, :, part_rows:] = mul(upper_low_t_ref[...], active_ref[0]).astype(BF16).reshape(shape)
        part = mul(grad_hidden, weight(w1_ref, 0, w1_ref.shape[3]), NT)

        @pl.when(step == groups)
        def _():
            total_ref[...] = part

        @pl.when(step > groups)
        def _():
            total_ref[...] += part

    @pl.when(step == 2 * groups - 1)
    def _():
        scaled, inverse = norm_parts(pre_ref[...])
        grad_middle = upper_ref[...] + total_ref[...]
        grad = norm_back(grad_middle, scaled, inverse, vec_ref[1:2])
        sums_ref[1:2] = jnp.sum(grad_middle * scaled, axis=0, keepdims=True)
        sums_ref[2:3] = jnp.sum(grad_middle, axis=0, keepdims=True)
        sums_ref[0:1] = jnp.sum(grad, axis=0, keepdims=True)
        sums_ref[6:8] = jnp.zeros_like(sums_ref[6:8])
        grad_pre_ref[...] = grad
        low = grad.astype(BF16)
        grad_low_ref[...] = low
        grad_low_t_ref[...] = low.T


def down(pre, cotangent, vectors, active, hidden, w2, w1, low_t):
    rows, width = pre.shape
    groups, units = w2.shape[1], w2.shape[3]
    whole = lambda s: (0, 0)
    both = lambda s: (lax.rem(s, groups), 0, 0)
    late = lambda s: (jnp.maximum(s - groups, 0), 0, 0)
    block = (w2.shape[0], 1) + w2.shape[2:]
    w_both = lambda s: (0, lax.rem(s, groups), 0, 0)
    w_late = lambda s: (0, jnp.maximum(s - groups, 0), 0, 0)
    return pl.pallas_call(
        functools.partial(down_kernel, groups),
        name="down",
        grid=(2 * groups,),
        in_specs=[
            pl.BlockSpec((rows, width), whole),
            pl.BlockSpec((rows, width), whole),
            pl.BlockSpec((8, width), whole),
            pl.BlockSpec((1, rows, units), both),
            pl.BlockSpec((1, rows, units), late),
            pl.BlockSpec(block, w_both),
            pl.BlockSpec(block, w_late),
            pl.BlockSpec((width, rows), whole),
        ],
        out_specs=[
            pl.BlockSpec((rows, width), whole),
            pl.BlockSpec((rows, width), whole),
            pl.BlockSpec((rows, width), whole),
            pl.BlockSpec((width, rows), whole),
            pl.BlockSpec(block[:2] + (2 * block[2],) + block[3:], w_late),
            pl.BlockSpec((8, width), whole),
            pl.BlockSpec((1, 1, units), late),
        ],
        out_shape=[
            jax.ShapeDtypeStruct((rows, width), BF16),
            jax.ShapeDtypeStruct((rows, width), F32),
            jax.ShapeDtypeStruct((rows, width), BF16),
            jax.ShapeDtypeStruct((width, rows), BF16),
            jax.ShapeDtypeStruct(w1.shape[:2] + (2 * w1.shape[2],) + w1.shape[3:], BF16),
            jax.ShapeDtypeStruct((8, width), F32),
            jax.ShapeDtypeStruct((groups, 1, units), F32),
        ],
        scratch_shapes=[
            pltpu.VMEM((rows, width), F32),
            pltpu.VMEM((rows, width), F32),
            pltpu.VMEM((rows, width), BF16),
            pltpu.VMEM((width, rows), BF16),
        ],
        cost_estimate=pl.CostEstimate(
            flops=10 * groups * rows * width * units, bytes_accessed=48 << 20, transcendentals=groups * rows * units
        ),
        compiler_params=pltpu.CompilerParams(vmem_limit_bytes=63 << 20),
    )(pre, cotangent, vectors, active, hidden, w2, w1, low_t)


def group_back(grad_ref, weight_of, ctx_ref, q_ref, k_ref, v_ref, after_head):
    rows = grad_ref.shape[0]
    step = 256
    grad_context = mul(grad_ref[...], weight_of(512, 768)).astype(BF16).astype(F32)
    lane = lanes((rows, 128))
    grads = []
    for head in range(3):
        place = 1 + head
        grad_head = head_block(grad_context, place)
        context = head_block(ctx_ref[0].astype(F32), place)
        delta = jnp.sum(jnp.where(lane < HEAD, grad_head * context, 0.0), axis=1, keepdims=True)
        high, middle, low = three_parts(-delta)
        tail = jnp.where(
            lane == HEAD, high, jnp.where(lane == HEAD + 1, middle, jnp.where(lane == HEAD + 2, low, 0.0))
        )
        grad_head = jnp.where(lane < HEAD, grad_head, tail).astype(BF16)
        keys_t = k_ref[head].T
        grad_query = []
        grad_keys = grad_values = None
        for first in range(0, rows, step):
            query_here = q_ref[head, first : first + step, :]
            grad_here = grad_head[first : first + step]
            weights = jnp.exp(mul(k_ref[head], query_here, NT))
            grad_scores = (weights * mul(v_ref[head], grad_here, NT)).astype(BF16)
            values_part = mul(weights.astype(BF16), grad_here)
            keys_part = mul(grad_scores, query_here)
            grad_values = values_part if grad_values is None else grad_values + values_part
            grad_keys = keys_part if grad_keys is None else grad_keys + keys_part
            grad_query.append(mul(keys_t, grad_scores))
        grad_query = jnp.concatenate(grad_query, axis=1).T * SCALE
        grads.append((grad_query, grad_keys, grad_values))
        after_head(head)
    (q0, k0, v0), (q1, k1, v1), (q2, k2, v2) = grads
    blank = jnp.zeros((rows, 128), F32)
    own = jnp.concatenate(
        [
            pair(q0, q1),
            pair(q2, k0[:rows]),
            pair(k1[:rows], k2[:rows]),
            pair(v0[:rows], v1[:rows]),
            pair(v2[:rows], blank),
        ],
        axis=1,
    )
    other = jnp.concatenate(
        [pair(blank, k0[rows:]), pair(k1[rows:], k2[rows:]), pair(v0[rows:], v1[rows:]), pair(v2[rows:], blank)],
        axis=1,
    )
    own_sum = jnp.sum(own, axis=0, keepdims=True)
    other_sum = jnp.sum(other, axis=0, keepdims=True)
    sums = [own_sum[:, 0:128]] + [
        own_sum[:, i : i + 128] + other_sum[:, i - 128 : i] for i in range(128, 640, 128)
    ]
    return own.astype(BF16), other.astype(BF16), sums


def weight_grads(grad_t_ref, own_t_ref, other_t_ref, ctx_ref, own, other):
    grad_w = mul(own_t_ref[...], own)
    grad_w_other = mul(other_t_ref[...], other)
    grad_out = mul(grad_t_ref[...], ctx_ref[0])
    return [
        grad_w[:, 0:128],
        grad_w[:, 128:512] + grad_w_other[:, 0:384],
        grad_w[:, 512:640] + grad_w_other[:, 384:512] + grad_out[:, 0:128],
        grad_out[:, 128:256],
    ]


def attend_back_kernel(
    grad_ref,
    grad_t_ref,
    own_t_ref,
    other_t_ref,
    w_ref,
    ctx_ref,
    q_ref,
    k_ref,
    v_ref,
    grad_w_ref,
    grad_own_ref,
    grad_other_ref,
    sums_ref,
    other_total_ref,
):
    group, groups = pl.program_id(0), pl.num_programs(0)
    own, other, sums = group_back(
        grad_ref, functools.partial(weight, w_ref), ctx_ref, q_ref, k_ref, v_ref, lambda head: None
    )
    columns = weight_grads(grad_t_ref, own_t_ref, other_t_ref, ctx_ref, own, other)
    for number, piece in enumerate(sums):
        sums_ref[0, :, 128 * number : 128 * number + 128] = piece
    shape = (grad_w_ref.shape[0], 1, grad_w_ref.shape[2])
    first = 0
    for piece in columns:
        last = first + piece.shape[1]
        grad_w_ref[:, :, :, first:last] = piece.astype(BF16).reshape(shape + (last - first,))
        first = last
    own_part = mul(own, weight(w_ref, 0, 640), NT)
    other_part = mul(other, weight(w_ref, 128, 640), NT)

    @pl.when(group == 0)
    def _():
        grad_own_ref[...] = own_part
        other_total_ref[...] = other_part

    @pl.when(group > 0)
    def _():
        grad_own_ref[...] += own_part
        other_total_ref[...] += other_part

    @pl.when(group == groups - 1)
    def _():
        grad_other_ref[...] = other_total_ref[...].astype(BF16)


def attend_back(grad, grad_t, own_t, other_t, weights, ctx, query, keys, values):
    rows, width = grad.shape
    groups = weights.shape[1]
    whole = lambda g: (0, 0)
    by_group = lambda g: (g, 0, 0)
    block = pl.BlockSpec((weights.shape[0], 1) + weights.shape[2:], lambda g: (0, g, 0, 0))
    flops = groups * (3 * 2 * rows * width * 640 + 3 * 10 * rows * SLOT * 128)
    return pl.pallas_call(
        attend_back_kernel,
        name="attend_back",
        grid=(groups,),
        in_specs=[
            pl.BlockSpec((rows, width), whole),
            pl.BlockSpec((width, rows), whole),
            pl.BlockSpec((width, rows), whole),
            pl.BlockSpec((width, rows), whole),
            block,
            pl.BlockSpec((1, rows, 256), by_group),
            pl.BlockSpec((3, rows, 128), by_group),
            pl.BlockSpec((3, SLOT, 128), by_group),
            pl.BlockSpec((3, SLOT, 128), by_group),
        ],
        out_specs=[
            block,
            pl.BlockSpec((rows, width), whole),
            pl.BlockSpec((rows, width), whole),
            pl.BlockSpec((1, 1, 640), by_group),
        ],
        out_shape=[
            jax.ShapeDtypeStruct(weights.shape, BF16),
            jax.ShapeDtypeStruct((rows, width), F32),
            jax.ShapeDtypeStruct((rows, width), BF16),
            jax.ShapeDtypeStruct((groups, 1, 640), F32),
        ],
        scratch_shapes=[pltpu.VMEM((rows, width), F32)],
        cost_estimate=pl.CostEstimate(flops=4 * flops, bytes_accessed=32 << 20, transcendentals=12 * rows * SLOT),
        compiler_params=pltpu.CompilerParams(vmem_limit_bytes=63 << 20),
    )(grad, grad_t, own_t, other_t, weights, ctx, query, keys, values)


CORE, ALONG_X, ALONG_Y = 1, 2, 4
DIAGONAL = ALONG_X | ALONG_Y
COLUMNS = (0, ALONG_X, ALONG_Y, DIAGONAL)


def meet(me, z, depth):
    barrier = pltpu.get_barrier_semaphore()
    for bit in (CORE, ALONG_X, ALONG_Y):
        pl.semaphore_signal(barrier, inc=1, device_id=(me ^ bit, z), device_id_type=MESH)

    @pl.when(z > 0)
    def _():
        pl.semaphore_signal(barrier, inc=1, device_id=(me, z - 1), device_id_type=MESH)

    @pl.when(z < depth - 1)
    def _():
        pl.semaphore_signal(barrier, inc=1, device_id=(me, z + 1), device_id_type=MESH)

    pl.semaphore_wait(barrier, 3 + (z > 0).astype(jnp.int32) + (z < depth - 1).astype(jnp.int32))


def near_first(z, depth):
    yield z, None
    for distance in range(1, depth):
        for place in (z - distance, z + distance):
            yield place, (place >= 0) & (place < depth)


def given(condition, action):
    if condition is None:
        action()
    else:
        pl.when(condition)(action)


def halves(rows):
    return (rows // 2, rows) if rows % 32 == 0 else (rows, rows)


UP, DOWN, X, Y, VIA_Y, VIA_X, C0 = range(7)
GATHER_KINDS = C0 + 4


def gather_kernel(count, depth, *refs):
    locals_, wholes = refs[:count], refs[count : 2 * count]
    send_sem, recv_sem = refs[2 * count :]
    me, z = lax.axis_index("dp"), lax.axis_index("mp")

    def copy(which, kind, place, source, target, to):
        return pltpu.make_async_remote_copy(
            src_ref=source,
            dst_ref=target,
            send_sem=send_sem.at[which, kind, place],
            recv_sem=recv_sem.at[which, kind, place],
            device_id=to,
            device_id_type=MESH,
        )

    meet(me, z, depth)

    def column(which, place, source, owner, kinds):
        whole = wholes[which]
        for kind, to, first, last in kinds:
            view = source if first == 0 and last == source.shape[0] else source.at[first:last]
            copy(which, kind, place, view, whole.at[owner, place, first:last], to).start()

    def arrived(which, kind, place, owner, first, last):
        view = wholes[which].at[owner, place, first:last]
        copy(which, kind, place, view, view, (me, z)).wait_recv()

    def first_stage(which, place, condition):
        rows = locals_[which].shape[0]

        def act():
            own = condition is None
            source = locals_[which] if own else wholes[which].at[me, place]
            if not own:
                pl.when(place < z)(lambda: arrived(which, UP, place, me, 0, rows))
                pl.when(place > z)(lambda: arrived(which, DOWN, place, me, 0, rows))
            up_from = (z < depth - 1) if own else (place < z) & (z < depth - 1)
            down_from = (z > 0) if own else (place > z) & (z > 0)
            pl.when(up_from)(lambda: column(which, place, source, me, [(UP, (me, z + 1), 0, rows)]))
            pl.when(down_from)(lambda: column(which, place, source, me, [(DOWN, (me, z - 1), 0, rows)]))
            column(
                which,
                place,
                source,
                me,
                [
                    (X, (me ^ ALONG_X, z), 0, rows),
                    (Y, (me ^ ALONG_Y, z), 0, rows),
                    (C0, (me ^ CORE, z), 0, rows),
                ],
            )

        given(condition, act)

    def second_stage(which, place, condition):
        rows = locals_[which].shape[0]
        half, _ = halves(rows)

        def act():
            arrived(which, X, place, me ^ ALONG_X, 0, rows)
            source = wholes[which].at[me ^ ALONG_X, place]
            column(
                which,
                place,
                source,
                me ^ ALONG_X,
                [(VIA_Y, (me ^ ALONG_Y, z), 0, half), (C0 + 1, (me ^ CORE, z), 0, rows)],
            )
            arrived(which, Y, place, me ^ ALONG_Y, 0, rows)
            source = wholes[which].at[me ^ ALONG_Y, place]
            kinds = [(C0 + 2, (me ^ CORE, z), 0, rows)]
            if half < rows:
                kinds = [(VIA_X, (me ^ ALONG_X, z), half, rows)] + kinds
            column(which, place, source, me ^ ALONG_Y, kinds)

        given(condition, act)

    def third_stage(which, place, condition):
        rows = locals_[which].shape[0]
        half, _ = halves(rows)

        def act():
            arrived(which, VIA_Y, place, me ^ DIAGONAL, 0, half)
            if half < rows:
                arrived(which, VIA_X, place, me ^ DIAGONAL, half, rows)
            source = wholes[which].at[me ^ DIAGONAL, place]
            column(which, place, source, me ^ DIAGONAL, [(C0 + 3, (me ^ CORE, z), 0, rows)])

        given(condition, act)

    def last_stage(which, place):
        rows = locals_[which].shape[0]
        for number, bit in enumerate(COLUMNS):
            arrived(which, C0 + number, place, me ^ CORE ^ bit, 0, rows)

    order = []
    for which in range(count):
        pltpu.make_async_copy(
            locals_[which], wholes[which].at[me, z], send_sem.at[which, GATHER_KINDS, 0]
        ).start()
        order += [(which,) + item for item in near_first(z, depth)]
    lag = len(order) // count
    for step in range(len(order) + 2 * lag):
        if step < len(order):
            first_stage(*order[step])
        if 0 <= step - lag < len(order):
            second_stage(*order[step - lag])
        if 0 <= step - 2 * lag:
            third_stage(*order[step - 2 * lag])
    for which in range(count):
        rows = locals_[which].shape[0]
        half, _ = halves(rows)
        for place in range(depth):
            last_stage(which, place)
        for place, condition in near_first(z, depth):

            def sent(which=which, place=place, own=condition is None):
                whole = wholes[which].at[me, place]
                pieces = [(X, 0, rows), (Y, 0, rows), (VIA_Y, 0, half)] + [(C0 + n, 0, rows) for n in range(4)]
                if half < rows:
                    pieces.append((VIA_X, half, rows))
                for kind, first, last in pieces:
                    view = whole.at[first:last]
                    copy(which, kind, place, view, view, (me, z)).wait_send()
                up_from = (z < depth - 1) if own else (place < z) & (z < depth - 1)
                down_from = (z > 0) if own else (place > z) & (z > 0)
                pl.when(up_from)(lambda: copy(which, UP, place, whole, whole, (me, z)).wait_send())
                pl.when(down_from)(lambda: copy(which, DOWN, place, whole, whole, (me, z)).wait_send())

            given(condition, sent)
        pltpu.make_async_copy(
            locals_[which], wholes[which].at[me, z], send_sem.at[which, GATHER_KINDS, 0]
        ).wait()


def gather_all(locals_, n_dp, n_mp, number):
    count = len(locals_)
    sems = pltpu.SemaphoreType.DMA((count, GATHER_KINDS + 1, n_mp))
    return pl.pallas_call(
        functools.partial(gather_kernel, count, n_mp),
        name="gather",
        in_specs=[pl.BlockSpec(memory_space=pltpu.VMEM)] * count,
        out_specs=[pl.BlockSpec(memory_space=pl.ANY)] * count,
        out_shape=[jax.ShapeDtypeStruct((n_dp, n_mp) + a.shape, a.dtype) for a in locals_],
        scratch_shapes=[sems, sems],
        compiler_params=pltpu.CompilerParams(collective_id=number, has_side_effects=True),
    )(*locals_)


TO_X, TO_Y, X_LOW, X_HIGH, Y_LOW, Y_HIGH, Z_UP, Z_DOWN, S0 = range(9)
SCATTER_KINDS = S0 + 4


class Reduction:
    def __init__(self, which, me, z, depth, rows, bufs, send_sem, recv_sem):
        self.which, self.me, self.z, self.depth, self.rows = which, me, z, depth, rows
        self.half = halves(rows)[0]
        self.core, self.diagonal, self.sides, self.line = bufs
        self.send_sem, self.recv_sem = send_sem, recv_sem

    def copy(self, kind, place, source, target, to):
        return pltpu.make_async_remote_copy(
            src_ref=source,
            dst_ref=target,
            send_sem=self.send_sem.at[self.which, kind, place],
            recv_sem=self.recv_sem.at[self.which, kind, place],
            device_id=to,
            device_id_type=MESH,
        )

    def start(self, kind, place, source, target, bit):
        self.copy(kind, place, source, target, (self.me ^ bit, self.z)).start()

    def wait(self, kind, place, view):
        self.copy(kind, place, view, view, (self.me, self.z)).wait_recv()

    def add(self, target, *others):
        total = target[...].astype(F32)
        for other in others:
            total = total + other[...].astype(F32)
        target[...] = total.astype(target.dtype)

    def to_core(self, place, theirs, numbers=(3, 1, 2, 0)):
        for number in numbers:
            self.start(S0 + number, place, theirs(number), self.core.at[number, place], CORE)

    def first(self, place, mine):
        half, rows = self.half, self.rows
        for number in (3, 1, 2):
            view = self.core.at[number, place]
            self.wait(S0 + number, place, view)
            self.add(view, mine(number))
            if number == 3:
                self.start(TO_X, place, view.at[0:half], self.diagonal.at[place, 0:half], ALONG_X)
                if half < rows:
                    self.start(TO_Y, place, view.at[half:rows], self.diagonal.at[place, half:rows], ALONG_Y)
            if number == 1:
                self.start(X_LOW, place, view.at[0:half], self.sides.at[0, place, 0:half], ALONG_X)
            if number == 2 and half < rows:
                self.start(Y_HIGH, place, view.at[half:rows], self.sides.at[1, place, half:rows], ALONG_Y)

    def second(self, place):
        half, rows = self.half, self.rows
        view = self.diagonal.at[place, 0:half]
        self.wait(TO_X, place, view)
        mine = self.core.at[2, place, 0:half]
        self.add(mine, view)
        self.start(Y_LOW, place, mine, self.sides.at[1, place, 0:half], ALONG_Y)
        if half < rows:
            view = self.diagonal.at[place, half:rows]
            self.wait(TO_Y, place, view)
            mine = self.core.at[1, place, half:rows]
            self.add(mine, view)
            self.start(X_HIGH, place, mine, self.sides.at[0, place, half:rows], ALONG_X)

    def third(self, place, mine):
        half, rows = self.half, self.rows
        self.wait(S0, place, self.core.at[0, place])
        self.wait(X_LOW, place, self.sides.at[0, place, 0:half])
        self.wait(Y_LOW, place, self.sides.at[1, place, 0:half])
        if half < rows:
            self.wait(Y_HIGH, place, self.sides.at[1, place, half:rows])
            self.wait(X_HIGH, place, self.sides.at[0, place, half:rows])
        self.add(self.core.at[0, place], mine(0), self.sides.at[0, place], self.sides.at[1, place])

    def along(self, kind, place):
        way = 0 if kind == Z_UP else 1
        to = (self.me, self.z + 1 if kind == Z_UP else self.z - 1)
        return self.copy(kind, place, self.core.at[0, place], self.line.at[way, place], to)

    def hop(self, place, number):
        for kind, here in ((Z_UP, number), (Z_DOWN, self.depth - 1 - number)):
            if (here < place) if kind == Z_UP else (here > place):

                @pl.when(self.z == here)
                def _(kind=kind):
                    if number > 0:
                        view = self.line.at[0 if kind == Z_UP else 1, place]
                        self.wait(kind, place, view)
                        self.add(self.core.at[0, place], view)
                    self.along(kind, place).start()

    def chain(self, distance):
        z, depth = self.z, self.depth
        above, below = z + distance, z - distance

        @pl.when(above < depth)
        def _():
            @pl.when(z > 0)
            def _():
                self.wait(Z_UP, above, self.line.at[0, above])
                self.add(self.core.at[0, above], self.line.at[0, above])

            self.along(Z_UP, above).start()

        @pl.when(below >= 0)
        def _():
            @pl.when(z < depth - 1)
            def _():
                self.wait(Z_DOWN, below, self.line.at[1, below])
                self.add(self.core.at[0, below], self.line.at[1, below])

            self.along(Z_DOWN, below).start()

    def finish(self, out):
        z, depth = self.z, self.depth
        out[...] = self.core[0, z].astype(F32)

        @pl.when(z > 0)
        def _():
            self.wait(Z_UP, z, self.line.at[0, z])
            out[...] += self.line[0, z].astype(F32)

        @pl.when(z < depth - 1)
        def _():
            self.wait(Z_DOWN, z, self.line.at[1, z])
            out[...] += self.line[1, z].astype(F32)

    def drain(self):
        half, rows = self.half, self.rows
        pieces = [(S0 + number, 0, rows) for number in range(4)]
        pieces += [(TO_X, 0, half), (X_LOW, 0, half), (Y_LOW, 0, half)]
        if half < rows:
            pieces += [(TO_Y, half, rows), (Y_HIGH, half, rows), (X_HIGH, half, rows)]
        for place in range(self.depth):
            for kind, first, last in pieces:
                view = self.core.at[0, place, first:last]
                self.copy(kind, place, view, view, (self.me, self.z)).wait_send()
        for distance in range(1, self.depth):
            above, below = self.z + distance, self.z - distance
            pl.when(above < self.depth)(lambda above=above: self.along(Z_UP, above).wait_send())
            pl.when(below >= 0)(lambda below=below: self.along(Z_DOWN, below).wait_send())


def linked_back_kernel(
    depth,
    grad_ref,
    grad_t_ref,
    own_t_ref,
    other_t_ref,
    early_ref,
    w_hbm,
    ff_hbm,
    ctx_ref,
    q_ref,
    k_ref,
    v_ref,
    ff_out,
    w_out,
    small_out,
    grad_own_ref,
    w_buf,
    w_sem,
    grad_w,
    grad_small,
    ff_mine,
    ff_sem,
    ff_own,
    ff_own_sem,
    grad_heads,
    grad_queries,
    others,
    other_total,
    sent,
    received,
    pair_send,
    pair_recv,
    *refs,
):
    send_sem, recv_sem = refs[-2:]
    me, z = lax.axis_index("dp"), lax.axis_index("mp")
    step = pl.program_id(0)
    turn = lax.rem(step, depth)
    rows = grad_ref.shape[0]
    part = w_buf.shape[2]
    width = 8 * part
    group_at = lambda s: z ^ (depth - 1 - s)
    group = group_at(turn)
    arrays = [(2 * part, refs[0:4]), (part, refs[4:8]), (8, refs[8:12])]
    ff, w, small = [
        Reduction(i, me, z, depth, size, bufs, send_sem, recv_sem) for i, (size, bufs) in enumerate(arrays)
    ]
    places = [depth - 1, 0] + list(range(1, depth - 1))[::-1]
    lane = lanes((rows, 128))

    def load_w(s):
        return pltpu.make_async_copy(w_hbm.at[:, group_at(s)], w_buf.at[group_at(s)], w_sem.at[s])

    def load_ff(number, column):
        source = ff_hbm.at[me ^ COLUMNS[column], places[number]]
        return pltpu.make_async_copy(source, ff_mine.at[number % 2, column - 1], ff_sem.at[number % 2, column - 1])

    def load_ff_own(place):
        return pltpu.make_async_copy(ff_hbm.at[me, place], ff_own.at[place], ff_own_sem.at[place])

    exchange = pltpu.make_async_remote_copy(
        src_ref=sent,
        dst_ref=received,
        send_sem=pair_send,
        recv_sem=pair_recv,
        device_id=(me, z ^ 1),
        device_id_type=MESH,
    )

    @pl.when(step == 0)
    def _():
        for s in range(depth):
            load_w(s).start()
        for number in range(2):
            for column in (3, 1, 2):
                load_ff(number, column).start()
        meet(me, z, depth)
        theirs = lambda place: lambda column: ff_hbm.at[me ^ CORE ^ COLUMNS[column], place]
        for place in places:
            ff.to_core(place, theirs(place), (3, 1, 2))
        for place in places:
            ff.to_core(place, theirs(place), (0,))
            load_ff_own(place).start()

    for s in range(depth):
        pl.when(step == s)(lambda s=s: load_w(s).wait())

    def ff_first(number):
        for column in (3, 1, 2):
            load_ff(number, column).wait()
        ff.first(places[number], lambda column: ff_mine.at[number % 2, column - 1])
        if number + 2 < depth:
            for column in (3, 1, 2):
                load_ff(number + 2, column).start()

    def ff_third(number):
        place = places[number]
        load_ff_own(place).wait()
        ff.third(place, lambda column: ff_own.at[place])

    work = {}

    def plan(slot, action, *arguments):
        work.setdefault(slot, []).append((action, arguments))

    end = 6 * depth
    for number, slots in enumerate(((1, 5, 9), (2, 8, 13), (4, 12, 17), (5, 15, 20))):
        plan(slots[0], ff_first, number)
        plan(slots[1], ff.second, places[number])
        plan(slots[2], ff_third, number)
        for hop in range(depth - 1):
            plan(min(slots[2] + 4 * hop, end + (number == 3) * (hop - 1)), ff.hop, places[number], hop)

    def do(slot):
        for action, arguments in work.get(slot, ()):
            action(*arguments)

    def w_first(s):
        place = group_at(s)
        w.first(place, lambda column: grad_w.at[s, me ^ COLUMNS[column]])
        small.first(place, lambda column: grad_small.at[s, me ^ COLUMNS[column]])

    def w_second(s):
        w.second(group_at(s))
        small.second(group_at(s))

    def w_third(s):
        place = group_at(s)
        w.third(place, lambda column: grad_w.at[s, me ^ COLUMNS[column]])
        small.third(place, lambda column: grad_small.at[s, me ^ COLUMNS[column]])

    def w_chain(distance):
        w.chain(distance)
        small.chain(distance)

    def after_head(head):
        for s in range(2 * depth):
            if 3 * s + head in work:
                pl.when(step == s)(lambda slot=3 * s + head: do(slot))
        pl.when(step > depth)(lambda: (w_first, w_second, w_third)[head](step - depth - 1))
        if head == 2:
            for s in range(depth - 1):
                pl.when(step == depth + 1 + s)(lambda s=s: w_chain(depth - 1 - s))

    def weight_of(first, last):
        return w_buf[group, :, :, first:last].reshape(width, last - first)

    @pl.when(step < depth)
    def _():
        grad_context = mul(grad_ref[...], weight_of(512, 768)).astype(BF16).astype(F32)
        for head in range(3):
            grad_head = head_block(grad_context, 1 + head)
            context = head_block(ctx_ref[0].astype(F32), 1 + head)
            delta = jnp.sum(jnp.where(lane < HEAD, grad_head * context, 0.0), axis=1, keepdims=True)
            high, middle, low = three_parts(-delta)
            tail = jnp.where(
                lane == HEAD, high, jnp.where(lane == HEAD + 1, middle, jnp.where(lane == HEAD + 2, low, 0.0))
            )
            grad_heads[turn, head] = jnp.where(lane < HEAD, grad_head, tail).astype(BF16)

    grads = []
    chunk = 256
    for head in range(3):
        keys_t = k_ref[head].T
        grad_query = []
        grad_keys = grad_values = None
        for first in range(0, rows, chunk):
            query_here = q_ref[head, first : first + chunk, :]
            grad_here = grad_heads[turn, head, first : first + chunk, :]
            weights = jnp.exp(mul(k_ref[head], query_here, NT))
            grad_scores = (weights * mul(v_ref[head], grad_here, NT)).astype(BF16)
            values_part = mul(weights.astype(BF16), grad_here)
            keys_part = mul(grad_scores, query_here)
            grad_values = values_part if grad_values is None else grad_values + values_part
            grad_keys = keys_part if grad_keys is None else grad_keys + keys_part
            grad_query.append(mul(keys_t, grad_scores))
        grads.append((jnp.concatenate(grad_query, axis=1).T * SCALE, grad_keys, grad_values))
        after_head(head)
    (q0, k0, v0), (q1, k1, v1), (q2, k2, v2) = grads
    blank = jnp.zeros((rows, 128), F32)
    k12, v01 = pair(k1, k2), pair(v0, v1)

    @pl.when(step < depth)
    def _():
        grad_queries[turn, :, 0:128] = pair(q0, q1)
        grad_queries[turn, :, 128:256] = q2
        other = jnp.concatenate([pair(blank, k0), k12, v01, pair(v2, blank)], axis=1).astype(BF16)
        others[turn] = other
        other_part = mul(other, weight_of(128, 640), NT)

        @pl.when(step == 0)
        def _():
            other_total[...] = other_part

        @pl.when(step > 0)
        def _():
            other_total[...] += other_part

        @pl.when(step == depth - 1)
        def _():
            sent[...] = other_total[...].astype(BF16)
            exchange.start()

    @pl.when(step >= depth)
    def _():
        q01 = pair(q0, q1) + grad_queries[turn, :, 0:128]
        q2_all = q2 + grad_queries[turn, :, 128:256]
        own = jnp.concatenate([q01, pair(q2_all, k0), k12, v01, pair(v2, blank)], axis=1)
        other = others[turn]
        own_sum = jnp.sum(own, axis=0, keepdims=True)
        other_sum = jnp.sum(other.astype(F32), axis=0, keepdims=True)
        row = lax.broadcasted_iota(jnp.int32, (8, 128), 0)
        late = jnp.where(row == 0, own_sum[:, 0:128], 0.0)
        for number in range(1, 5):
            piece = own_sum[:, 128 * number : 128 * number + 128] + other_sum[:, 128 * number - 128 : 128 * number]
            late = jnp.where(row == number, piece, late)
        for owner in range(8):
            grad_small[turn, owner] = early_ref[owner, group] + late
        own = own.astype(BF16)
        first = 0
        for piece in weight_grads(grad_t_ref, own_t_ref, other_t_ref, ctx_ref, own, other):
            last = first + piece.shape[1]
            grad_w[turn, :, :, first:last] = piece.astype(BF16).reshape(8, part, last - first)
            first = last
        w.to_core(group, lambda column: grad_w.at[turn, me ^ CORE ^ COLUMNS[column]])
        small.to_core(group, lambda column: grad_small.at[turn, me ^ CORE ^ COLUMNS[column]])
        own_part = mul(own, weight_of(0, 640), NT)

        @pl.when(step == depth)
        def _():
            grad_own_ref[...] = own_part

        @pl.when(step > depth)
        def _():
            grad_own_ref[...] += own_part

    @pl.when(step == 2 * depth - 1)
    def _():
        w_first(depth - 1)
        do(end)
        exchange.wait_recv()
        grad_own_ref[...] += received[...].astype(F32)
        w_second(depth - 1)
        do(end + 1)
        w_third(depth - 1)
        ff.finish(ff_out)
        w.finish(w_out)
        small.finish(small_out)
        for array in (ff, w, small):
            array.drain()
        exchange.wait_send()


def linked_back(grad, grad_t, own_t, other_t, early, weights, grad_ff, ctx, query, keys, values):
    rows, width = grad.shape
    n_dp, groups, part = weights.shape[:3]
    whole = pl.BlockSpec(memory_space=pltpu.VMEM)
    anywhere = pl.BlockSpec(memory_space=pl.ANY)
    by_group = lambda g: (groups - 1 - lax.rem(g, groups), 0, 0)
    by_half = lambda g: (groups - 1 - lax.rem(g, groups), 1 - g // groups, 0)
    flops = groups * (3 * 2 * rows * width * 640 + 3 * 10 * rows * SLOT * 128)
    scratch = []
    for size, columns, kind in ((2 * part, width, BF16), (part, width, BF16), (8, 128, F32)):
        block = (size, columns)
        scratch += [
            pltpu.VMEM((4, groups) + block, kind),
            pltpu.VMEM((groups,) + block, kind),
            pltpu.VMEM((2, groups) + block, kind),
            pltpu.VMEM((2, groups) + block, kind),
        ]
    sems = pltpu.SemaphoreType.DMA((3, SCATTER_KINDS, groups))
    return pl.pallas_call(
        functools.partial(linked_back_kernel, groups),
        name="linked_back",
        grid=(2 * groups,),
        in_specs=[whole] * 5
        + [anywhere] * 2
        + [
            pl.BlockSpec((1, rows, 256), by_group),
            pl.BlockSpec((3, rows, 128), by_group),
            pl.BlockSpec((3, rows, 128), by_half),
            pl.BlockSpec((3, rows, 128), by_half),
        ],
        out_specs=[whole] * 4,
        out_shape=[
            jax.ShapeDtypeStruct((2 * part, width), F32),
            jax.ShapeDtypeStruct((part, width), F32),
            jax.ShapeDtypeStruct((8, 128), F32),
            jax.ShapeDtypeStruct((rows, width), F32),
        ],
        scratch_shapes=[
            pltpu.VMEM((groups, n_dp, part, width), BF16),
            pltpu.SemaphoreType.DMA((groups,)),
            pltpu.VMEM((groups, n_dp, part, width), BF16),
            pltpu.VMEM((groups, n_dp, 8, 128), F32),
            pltpu.VMEM((2, 3, 2 * part, width), BF16),
            pltpu.SemaphoreType.DMA((2, 3)),
            pltpu.VMEM((groups, 2 * part, width), BF16),
            pltpu.SemaphoreType.DMA((groups,)),
            pltpu.VMEM((groups, 3, rows, 128), BF16),
            pltpu.VMEM((groups, rows, 256), F32),
            pltpu.VMEM((groups, rows, 512), BF16),
            pltpu.VMEM((rows, width), F32),
            pltpu.VMEM((rows, width), BF16),
            pltpu.VMEM((rows, width), BF16),
            pltpu.SemaphoreType.DMA,
            pltpu.SemaphoreType.DMA,
        ]
        + scratch
        + [sems, sems],
        cost_estimate=pl.CostEstimate(flops=4 * flops, bytes_accessed=48 << 20, transcendentals=12 * rows * SLOT),
        compiler_params=pltpu.CompilerParams(
            collective_id=2, has_side_effects=True, vmem_limit_bytes=67043328
        ),
    )(grad, grad_t, own_t, other_t, early, weights, grad_ff, ctx, query, keys, values)


def blocks(local, mesh_shape):
    return lax.all_gather(local, BOTH, axis=0, tiled=False).reshape(mesh_shape + local.shape)


def gather_first(locals_, mesh_shape):
    if mesh_shape[0] == 8:
        return gather_all(locals_, *mesh_shape, number=1)
    return [blocks(local, mesh_shape) for local in locals_]


def scatter_sums(partial):
    flat = partial.reshape((-1,) + partial.shape[3:])
    return lax.psum_scatter(flat, BOTH, scatter_dimension=0, tiled=True).astype(F32)


def body(
    frames,
    w_qkv,
    b_qv,
    w_out,
    b_out,
    ln1_gain,
    ln1_bias,
    w_ff1,
    b_ff1,
    w_ff2,
    b_ff2,
    ln2_gain,
    ln2_bias,
    cotangent,
    clip_lengths,
    clip_slot,
):
    n_dp, n_mp = lax.axis_size("dp"), lax.axis_size("mp")
    rows, width = frames.shape
    share = b_out.shape[0]

    partner = [(m, m ^ 1) for m in range(n_mp)]
    other = lax.ppermute(frames, "mp", partner)
    packed = jnp.concatenate([w_qkv[0], w_qkv[1], w_qkv[2], w_out.T], axis=1)
    small = jnp.concatenate(
        [b_out, ln1_gain, ln1_bias, b_ff2, ln2_gain, ln2_bias, b_qv.reshape(-1).astype(F32), b_ff1.astype(F32)]
    )
    entries = small.shape[0]
    small = jnp.pad(small, (0, -entries % 1024)).reshape(-1, 128)
    mesh_shape = (n_dp, n_mp)
    w_attn, small = gather_first([packed, small], mesh_shape)
    w1, w2 = blocks(w_ff1, mesh_shape), blocks(w_ff2.T, mesh_shape)
    small = small.reshape(n_dp * n_mp, -1)[:, :entries]
    vectors = small[:, : 6 * share].reshape(n_dp * n_mp, 6, share).transpose(1, 0, 2).reshape(6, width)
    vectors = jnp.concatenate([vectors, jnp.zeros((2, width), F32)])
    ordered = small.reshape(n_dp, n_mp, -1).transpose(1, 0, 2)
    qv = ordered[:, :, 6 * share : 8 * share].reshape(n_mp, n_dp, 2, share).transpose(0, 2, 1, 3)
    qv = qv.reshape(n_mp, 2, 1, n_dp * share)
    heads_width = n_dp * share
    qv_bias = jnp.concatenate(
        [qv[:, 0], jnp.zeros((n_mp, 1, heads_width), F32), qv[:, 1], jnp.zeros((n_mp, 1, HEAD), F32)], axis=2
    )
    up_bias = ordered[:, :, 8 * share :].reshape(n_mp, 1, -1)

    index = lax.axis_index("dp") * n_mp + lax.axis_index("mp")
    slot = index // (SLOT // rows)
    half = index % (SLOT // rows)
    length = jnp.sum(jnp.where(clip_slot == slot, clip_lengths, 0))
    valid = jnp.stack([length - half * rows, length - (1 - half) * rows]).astype(jnp.int32)

    linked = n_dp == 8
    places = jnp.arange(n_mp, dtype=jnp.int32)
    order = (lax.axis_index("mp") ^ places) if linked else places
    pre_one, ctx, query, keys, values = attend(order, valid, frames, other, w_attn, qv_bias, vectors[0:1])
    hidden, active, low, low_t = up(pre_one, vectors[1:2], vectors[2:3], w1, up_bias)
    output, grad_pre, grad_low, grad_low_t, grad_ff, sums, grad_up_bias = down(
        pre_one, cotangent, vectors, active, hidden, w2, w1, low_t
    )
    sums = sums[:6].reshape(6, n_dp * n_mp, share).transpose(1, 0, 2).reshape(n_dp * n_mp, 6 * share)
    unit_sums = grad_up_bias.reshape(n_mp, n_dp, -1).transpose(1, 0, 2).reshape(n_dp * n_mp, -1)
    early = jnp.concatenate([sums, unit_sums], axis=1)
    entries = early.shape[1]
    early = jnp.pad(early, ((0, 0), (0, -entries % 128))).reshape(mesh_shape + (-1, 128))
    early = jnp.pad(early, ((0, 0), (0, 0), (5, 3 - early.shape[2]), (0, 0)))
    kept = (ctx, query, keys, values)
    if linked:
        done_ff, done_w, small, grad_own = linked_back(
            grad_low, grad_low_t, frames.T, other.T, early, w_attn, grad_ff, *kept
        )
        grad_input = grad_pre + grad_own
    else:
        grad_w, grad_own, grad_other, head_sums = attend_back(
            grad_low, grad_low_t, frames.T, other.T, w_attn, *kept
        )
        grad_input = grad_pre + grad_own + lax.ppermute(grad_other, "mp", partner).astype(F32)
        done_ff, done_w = scatter_sums(grad_ff), scatter_sums(grad_w)
        small = scatter_sums(early + jnp.pad(head_sums.reshape(1, n_mp, 5, 128), ((0, 0), (0, 0), (0, 3), (0, 0))))
    part = w_ff1.shape[0]
    small = small.reshape(-1)
    (d_out_bias, d_gain1, d_shift1, d_down_bias, d_gain2, d_shift2) = [
        small[640 + i * share : 640 + (i + 1) * share] for i in range(6)
    ]
    d_up_bias = small[640 + 6 * share : 640 + entries]
    d_qv = jnp.stack(
        [
            lax.dynamic_slice(small, (first + lax.axis_index("dp") * share,), (share,))
            for first in (0, 2 * heads_width)
        ]
    )
    d_qkv = jnp.stack([done_w[:, i * heads_width : (i + 1) * heads_width] for i in range(3)])
    done_w1, done_w2 = done_ff[:part], done_ff[part:]
    return (
        output,
        grad_input,
        d_qkv,
        d_qv,
        done_w[:, 3 * heads_width :].T,
        d_out_bias,
        d_gain1,
        d_shift1,
        done_w1,
        d_up_bias,
        done_w2.T,
        d_down_bias,
        d_gain2,
        d_shift2,
    )


def solution(mesh):
    rows, vector, group_vector = P(BOTH, None), P(BOTH), P(("mp", "dp"))
    qkv, qv, out, up_spec = P(None, "dp", "mp"), P(None, ("mp", "dp")), P("mp", "dp"), P("dp", "mp")
    weights = (qkv, qv, out, vector, vector, vector, up_spec, group_vector, out, vector, vector, vector)
    return jax.shard_map(
        body,
        mesh=mesh,
        in_specs=(rows,) + weights + (rows, P(), P()),
        out_specs=(rows, rows) + weights,
        check_vma=False,
    )
```

```python
import functools

import jax
import jax.numpy as jnp
from jax import lax
from jax.experimental import pallas as pl
from jax.experimental.pallas import tpu as pltpu
from jax.sharding import PartitionSpec as P

HEAD = 64
SLOT = 1536
EPS = 1e-05
SCALE = 0.125
MASKED = -1e30
BOTH = ("dp", "mp")
F32 = jnp.float32
BF16 = jnp.bfloat16
MESH = pl.DeviceIdType.MESH
NN = (((1,), (0,)), ((), ()))
NT = (((1,), (1,)), ((), ()))


def mul(left, right, dims=NN):
    return lax.dot_general(left, right, dims, preferred_element_type=F32)


def lanes(shape):
    return lax.broadcasted_iota(jnp.int32, shape, 1)


def three_parts(value):
    high = value.astype(BF16).astype(F32)
    rest = value - high
    middle = rest.astype(BF16).astype(F32)
    return high, middle, rest - middle


def head_block(value, place):
    block = value[:, 128 * (place // 2) : 128 * (place // 2) + 128]
    return pltpu.roll(block, HEAD, 1) if place % 2 else block


def pair(low, high):
    return jnp.where(lanes(low.shape) < HEAD, low, pltpu.roll(high, HEAD, 1))


def norm_parts(field):
    mean = jnp.mean(field, axis=-1, keepdims=True)
    centred = field - mean
    spread = jnp.mean(centred * centred, axis=-1, keepdims=True)
    inverse = lax.rsqrt(spread + EPS)
    return centred * inverse, inverse


def norm_back(grad, scaled, inverse, gain):
    inner = grad * gain
    return inverse * (
        inner
        - jnp.mean(inner, axis=-1, keepdims=True)
        - scaled * jnp.mean(inner * scaled, axis=-1, keepdims=True)
    )


def weight(ref, first, last):
    return ref[:, 0, :, first:last].reshape(ref.shape[0] * ref.shape[2], last - first)


def attend_group(bias, weight_of, valid_ref, own_ref, other_ref, ctx_ref, q_ref, k_ref, v_ref, after_head):
    rows = own_ref.shape[0]
    projected = mul(own_ref[...], weight_of(0, 640)) + bias
    projected_other = mul(other_ref[...], weight_of(128, 640)) + bias[:, 128:]
    lane = lanes((rows, 128))
    row = lax.broadcasted_iota(jnp.int32, (rows, 128), 0)
    contexts = []
    for head in range(3):
        query = jnp.where(
            lane < HEAD, head_block(projected, head).astype(BF16).astype(F32) * SCALE, jnp.where(lane == HEAD, 1.0, 0.0)
        )
        for half, (source, shift) in enumerate(((projected, 0), (projected_other, 2))):
            mask = jnp.where(row < valid_ref[half], 0.0, MASKED)
            tail = jnp.where(lane == HEAD, mask, jnp.where(lane < HEAD + 4, 1.0, 0.0))
            keys = jnp.where(lane < HEAD, head_block(source, 3 + head - shift), tail)
            values = jnp.where(
                lane < HEAD, head_block(source, 6 + head - shift), jnp.where(lane < HEAD + 3, 1.0, 0.0)
            )
            k_ref[head, half * rows : (half + 1) * rows, :] = keys.astype(BF16)
            v_ref[head, half * rows : (half + 1) * rows, :] = values.astype(BF16)
        step = 256
        pieces = []
        for first in range(0, rows, step):
            query_here = query[first : first + step]
            scores = mul(query_here.astype(BF16), k_ref[head], NT)
            peak = jnp.max(scores, axis=1, keepdims=True)
            exps = jnp.exp(scores - peak).astype(BF16)
            mixed = mul(exps, v_ref[head])
            lane_here = lanes((step, 128))
            total = jnp.sum(jnp.where(lane_here == HEAD, mixed, 0.0), axis=1, keepdims=True)
            pieces.append(mixed / total)
            high, middle, low = three_parts(-(peak + jnp.log(total)))
            kept = jnp.where(
                lane_here == HEAD + 1,
                high,
                jnp.where(lane_here == HEAD + 2, middle, jnp.where(lane_here == HEAD + 3, low, query_here)),
            )
            q_ref[head, first : first + step, :] = kept.astype(BF16)
        contexts.append(jnp.concatenate(pieces, axis=0))
        after_head(head)
    first_half = jnp.where(lane < HEAD, 0.0, pltpu.roll(contexts[0], HEAD, 1)).astype(BF16)
    second_half = pair(contexts[1], contexts[2]).astype(BF16)
    ctx_ref[0, :, 0:128] = first_half
    ctx_ref[0, :, 128:256] = second_half
    return mul(ctx_ref[0], weight_of(512, 768), NT)


def attend_kernel(
    order_ref, valid_ref, own_ref, other_ref, w_ref, qv_bias_ref, out_bias_ref, pre_ref, ctx_ref, q_ref, k_ref, v_ref
):
    group = pl.program_id(0)
    weight_of = functools.partial(weight, w_ref)
    kept = (ctx_ref, q_ref, k_ref, v_ref)
    part = attend_group(qv_bias_ref[0], weight_of, valid_ref, own_ref, other_ref, *kept, lambda head: None)

    @pl.when(group == 0)
    def _():
        pre_ref[...] = part + (out_bias_ref[...] + own_ref[...].astype(F32))

    @pl.when(group > 0)
    def _():
        pre_ref[...] += part


def attend(order, valid, own, other, weights, qv_bias, out_bias):
    rows, width = own.shape
    groups = weights.shape[1]
    whole = lambda g, order, valid: (0, 0)
    by_group = lambda g, order, valid: (g, 0, 0)
    flops = groups * (2 * 2 * rows * width * 640 + 3 * 4 * rows * SLOT * 128)
    return pl.pallas_call(
        attend_kernel,
        name="attend",
        grid_spec=pltpu.PrefetchScalarGridSpec(
            num_scalar_prefetch=2,
            grid=(groups,),
            in_specs=[
                pl.BlockSpec((rows, width), whole),
                pl.BlockSpec((rows, width), whole),
                pl.BlockSpec(
                    (weights.shape[0], 1) + weights.shape[2:], lambda g, order, valid: (0, order[g], 0, 0)
                ),
                pl.BlockSpec((1, 1, 640), lambda g, order, valid: (order[g], 0, 0)),
                pl.BlockSpec((1, width), whole),
            ],
            out_specs=[
                pl.BlockSpec((rows, width), whole),
                pl.BlockSpec((1, rows, 256), by_group),
                pl.BlockSpec((3, rows, 128), by_group),
                pl.BlockSpec((3, SLOT, 128), by_group),
                pl.BlockSpec((3, SLOT, 128), by_group),
            ],
        ),
        out_shape=[
            jax.ShapeDtypeStruct((rows, width), F32),
            jax.ShapeDtypeStruct((groups, rows, 256), BF16),
            jax.ShapeDtypeStruct((3 * groups, rows, 128), BF16),
            jax.ShapeDtypeStruct((3 * groups, SLOT, 128), BF16),
            jax.ShapeDtypeStruct((3 * groups, SLOT, 128), BF16),
        ],
        cost_estimate=pl.CostEstimate(flops=4 * flops, bytes_accessed=24 << 20, transcendentals=12 * rows * SLOT),
        compiler_params=pltpu.CompilerParams(vmem_limit_bytes=60 << 20),
    )(order, valid, own, other, weights, qv_bias, out_bias)


def up_kernel(pre_ref, gain_ref, shift_ref, w_ref, bias_ref, hidden_ref, active_ref, low_ref, low_t_ref):
    @pl.when(pl.program_id(0) == 0)
    def _():
        scaled, _ = norm_parts(pre_ref[...])
        low = (scaled * gain_ref[...] + shift_ref[...]).astype(BF16)
        low_ref[...] = low
        low_t_ref[...] = low.T

    hidden = mul(low_ref[...], weight(w_ref, 0, w_ref.shape[3])) + bias_ref[0]
    hidden_ref[0] = hidden
    active_ref[0] = (hidden * (0.5 * (1.0 + lax.erf(hidden * 0.7071067811865476)))).astype(BF16)


def up(pre, gain, shift, weights, bias):
    rows, width = pre.shape
    groups, units = weights.shape[1], weights.shape[3]
    whole = lambda g: (0, 0)
    by_group = lambda g: (g, 0, 0)
    return pl.pallas_call(
        up_kernel,
        name="up",
        grid=(groups,),
        in_specs=[
            pl.BlockSpec((rows, width), whole),
            pl.BlockSpec((1, width), whole),
            pl.BlockSpec((1, width), whole),
            pl.BlockSpec((weights.shape[0], 1) + weights.shape[2:], lambda g: (0, g, 0, 0)),
            pl.BlockSpec((1, 1, units), by_group),
        ],
        out_specs=[
            pl.BlockSpec((1, rows, units), by_group),
            pl.BlockSpec((1, rows, units), by_group),
            pl.BlockSpec((rows, width), whole),
            pl.BlockSpec((width, rows), whole),
        ],
        out_shape=[
            jax.ShapeDtypeStruct((groups, rows, units), F32),
            jax.ShapeDtypeStruct((groups, rows, units), BF16),
            jax.ShapeDtypeStruct((rows, width), BF16),
            jax.ShapeDtypeStruct((width, rows), BF16),
        ],
        cost_estimate=pl.CostEstimate(
            flops=2 * groups * rows * width * units, bytes_accessed=24 << 20, transcendentals=groups * rows * units
        ),
        compiler_params=pltpu.CompilerParams(vmem_limit_bytes=60 << 20),
    )(pre, gain, shift, weights, bias)


def down_kernel(
    groups,
    pre_ref,
    cot_ref,
    vec_ref,
    active_ref,
    hidden_ref,
    w2_ref,
    w1_ref,
    low_t_ref,
    out_ref,
    grad_pre_ref,
    grad_low_ref,
    grad_low_t_ref,
    grad_ff_ref,
    sums_ref,
    up_bias_ref,
    total_ref,
    upper_ref,
    upper_low_ref,
    upper_low_t_ref,
):
    step = pl.program_id(0)

    @pl.when(step < groups)
    def _():
        part = mul(active_ref[0], weight(w2_ref, 0, w2_ref.shape[3]), NT)

        @pl.when(step == 0)
        def _():
            total_ref[...] = part

        @pl.when(step > 0)
        def _():
            total_ref[...] += part

    @pl.when(step == groups - 1)
    def _():
        gain_one, shift_one = vec_ref[1:2], vec_ref[2:3]
        down_bias, gain_two, shift_two = vec_ref[3:4], vec_ref[4:5], vec_ref[5:6]
        middle = norm_parts(pre_ref[...])[0] * gain_one + shift_one
        scaled, inverse = norm_parts(total_ref[...] + down_bias + middle)
        out_ref[...] = (scaled * gain_two + shift_two).astype(BF16)
        cotangent = cot_ref[...].astype(F32)
        grad = norm_back(cotangent, scaled, inverse, gain_two)
        sums_ref[4:5] = jnp.sum(cotangent * scaled, axis=0, keepdims=True)
        sums_ref[5:6] = jnp.sum(cotangent, axis=0, keepdims=True)
        sums_ref[3:4] = jnp.sum(grad, axis=0, keepdims=True)
        upper_ref[...] = grad
        low = grad.astype(BF16)
        upper_low_ref[...] = low
        upper_low_t_ref[...] = low.T

    @pl.when(step >= groups)
    def _():
        grad_active = mul(upper_low_ref[...], weight(w2_ref, 0, w2_ref.shape[3]))
        hidden = hidden_ref[0]
        cdf = 0.5 * (1.0 + lax.erf(hidden * 0.7071067811865476))
        slope = cdf + hidden * jnp.exp(-0.5 * hidden * hidden) * 0.3989422804014327
        grad_hidden = (grad_active * slope).astype(BF16)
        up_bias_ref[0] = jnp.sum(grad_hidden.astype(F32), axis=0, keepdims=True)
        part_rows = w1_ref.shape[2]
        shape = w1_ref.shape
        grad_ff_ref[:, :, :part_rows] = mul(low_t_ref[...], grad_hidden).astype(BF16).reshape(shape)
        grad_ff_ref[:, :, part_rows:] = mul(upper_low_t_ref[...], active_ref[0]).astype(BF16).reshape(shape)
        part = mul(grad_hidden, weight(w1_ref, 0, w1_ref.shape[3]), NT)

        @pl.when(step == groups)
        def _():
            total_ref[...] = part

        @pl.when(step > groups)
        def _():
            total_ref[...] += part

    @pl.when(step == 2 * groups - 1)
    def _():
        scaled, inverse = norm_parts(pre_ref[...])
        grad_middle = upper_ref[...] + total_ref[...]
        grad = norm_back(grad_middle, scaled, inverse, vec_ref[1:2])
        sums_ref[1:2] = jnp.sum(grad_middle * scaled, axis=0, keepdims=True)
        sums_ref[2:3] = jnp.sum(grad_middle, axis=0, keepdims=True)
        sums_ref[0:1] = jnp.sum(grad, axis=0, keepdims=True)
        sums_ref[6:8] = jnp.zeros_like(sums_ref[6:8])
        grad_pre_ref[...] = grad
        low = grad.astype(BF16)
        grad_low_ref[...] = low
        grad_low_t_ref[...] = low.T


def down(pre, cotangent, vectors, active, hidden, w2, w1, low_t):
    rows, width = pre.shape
    groups, units = w2.shape[1], w2.shape[3]
    whole = lambda s: (0, 0)
    both = lambda s: (lax.rem(s, groups), 0, 0)
    late = lambda s: (jnp.maximum(s - groups, 0), 0, 0)
    block = (w2.shape[0], 1) + w2.shape[2:]
    w_both = lambda s: (0, lax.rem(s, groups), 0, 0)
    w_late = lambda s: (0, jnp.maximum(s - groups, 0), 0, 0)
    return pl.pallas_call(
        functools.partial(down_kernel, groups),
        name="down",
        grid=(2 * groups,),
        in_specs=[
            pl.BlockSpec((rows, width), whole),
            pl.BlockSpec((rows, width), whole),
            pl.BlockSpec((8, width), whole),
            pl.BlockSpec((1, rows, units), both),
            pl.BlockSpec((1, rows, units), late),
            pl.BlockSpec(block, w_both),
            pl.BlockSpec(block, w_late),
            pl.BlockSpec((width, rows), whole),
        ],
        out_specs=[
            pl.BlockSpec((rows, width), whole),
            pl.BlockSpec((rows, width), whole),
            pl.BlockSpec((rows, width), whole),
            pl.BlockSpec((width, rows), whole),
            pl.BlockSpec(block[:2] + (2 * block[2],) + block[3:], w_late),
            pl.BlockSpec((8, width), whole),
            pl.BlockSpec((1, 1, units), late),
        ],
        out_shape=[
            jax.ShapeDtypeStruct((rows, width), BF16),
            jax.ShapeDtypeStruct((rows, width), F32),
            jax.ShapeDtypeStruct((rows, width), BF16),
            jax.ShapeDtypeStruct((width, rows), BF16),
            jax.ShapeDtypeStruct(w1.shape[:2] + (2 * w1.shape[2],) + w1.shape[3:], BF16),
            jax.ShapeDtypeStruct((8, width), F32),
            jax.ShapeDtypeStruct((groups, 1, units), F32),
        ],
        scratch_shapes=[
            pltpu.VMEM((rows, width), F32),
            pltpu.VMEM((rows, width), F32),
            pltpu.VMEM((rows, width), BF16),
            pltpu.VMEM((width, rows), BF16),
        ],
        cost_estimate=pl.CostEstimate(
            flops=10 * groups * rows * width * units, bytes_accessed=48 << 20, transcendentals=groups * rows * units
        ),
        compiler_params=pltpu.CompilerParams(vmem_limit_bytes=63 << 20),
    )(pre, cotangent, vectors, active, hidden, w2, w1, low_t)


def group_back(grad_ref, weight_of, ctx_ref, q_ref, k_ref, v_ref, after_head):
    rows = grad_ref.shape[0]
    step = 256
    grad_context = mul(grad_ref[...], weight_of(512, 768)).astype(BF16).astype(F32)
    lane = lanes((rows, 128))
    grads = []
    for head in range(3):
        place = 1 + head
        grad_head = head_block(grad_context, place)
        context = head_block(ctx_ref[0].astype(F32), place)
        delta = jnp.sum(jnp.where(lane < HEAD, grad_head * context, 0.0), axis=1, keepdims=True)
        high, middle, low = three_parts(-delta)
        tail = jnp.where(
            lane == HEAD, high, jnp.where(lane == HEAD + 1, middle, jnp.where(lane == HEAD + 2, low, 0.0))
        )
        grad_head = jnp.where(lane < HEAD, grad_head, tail).astype(BF16)
        keys_t = k_ref[head].T
        grad_query = []
        grad_keys = grad_values = None
        for first in range(0, rows, step):
            query_here = q_ref[head, first : first + step, :]
            grad_here = grad_head[first : first + step]
            weights = jnp.exp(mul(k_ref[head], query_here, NT))
            grad_scores = (weights * mul(v_ref[head], grad_here, NT)).astype(BF16)
            values_part = mul(weights.astype(BF16), grad_here)
            keys_part = mul(grad_scores, query_here)
            grad_values = values_part if grad_values is None else grad_values + values_part
            grad_keys = keys_part if grad_keys is None else grad_keys + keys_part
            grad_query.append(mul(keys_t, grad_scores))
        grad_query = jnp.concatenate(grad_query, axis=1).T * SCALE
        grads.append((grad_query, grad_keys, grad_values))
        after_head(head)
    (q0, k0, v0), (q1, k1, v1), (q2, k2, v2) = grads
    blank = jnp.zeros((rows, 128), F32)
    own = jnp.concatenate(
        [
            pair(q0, q1),
            pair(q2, k0[:rows]),
            pair(k1[:rows], k2[:rows]),
            pair(v0[:rows], v1[:rows]),
            pair(v2[:rows], blank),
        ],
        axis=1,
    )
    other = jnp.concatenate(
        [pair(blank, k0[rows:]), pair(k1[rows:], k2[rows:]), pair(v0[rows:], v1[rows:]), pair(v2[rows:], blank)],
        axis=1,
    )
    own_sum = jnp.sum(own, axis=0, keepdims=True)
    other_sum = jnp.sum(other, axis=0, keepdims=True)
    sums = [own_sum[:, 0:128]] + [
        own_sum[:, i : i + 128] + other_sum[:, i - 128 : i] for i in range(128, 640, 128)
    ]
    return own.astype(BF16), other.astype(BF16), sums


def weight_grads(grad_t_ref, own_t_ref, other_t_ref, ctx_ref, own, other):
    grad_w = mul(own_t_ref[...], own)
    grad_w_other = mul(other_t_ref[...], other)
    grad_out = mul(grad_t_ref[...], ctx_ref[0])
    return [
        grad_w[:, 0:128],
        grad_w[:, 128:512] + grad_w_other[:, 0:384],
        grad_w[:, 512:640] + grad_w_other[:, 384:512] + grad_out[:, 0:128],
        grad_out[:, 128:256],
    ]


def attend_back_kernel(
    grad_ref,
    grad_t_ref,
    own_t_ref,
    other_t_ref,
    w_ref,
    ctx_ref,
    q_ref,
    k_ref,
    v_ref,
    grad_w_ref,
    grad_own_ref,
    grad_other_ref,
    sums_ref,
    other_total_ref,
):
    group, groups = pl.program_id(0), pl.num_programs(0)
    own, other, sums = group_back(
        grad_ref, functools.partial(weight, w_ref), ctx_ref, q_ref, k_ref, v_ref, lambda head: None
    )
    columns = weight_grads(grad_t_ref, own_t_ref, other_t_ref, ctx_ref, own, other)
    for number, piece in enumerate(sums):
        sums_ref[0, :, 128 * number : 128 * number + 128] = piece
    shape = (grad_w_ref.shape[0], 1, grad_w_ref.shape[2])
    first = 0
    for piece in columns:
        last = first + piece.shape[1]
        grad_w_ref[:, :, :, first:last] = piece.astype(BF16).reshape(shape + (last - first,))
        first = last
    own_part = mul(own, weight(w_ref, 0, 640), NT)
    other_part = mul(other, weight(w_ref, 128, 640), NT)

    @pl.when(group == 0)
    def _():
        grad_own_ref[...] = own_part
        other_total_ref[...] = other_part

    @pl.when(group > 0)
    def _():
        grad_own_ref[...] += own_part
        other_total_ref[...] += other_part

    @pl.when(group == groups - 1)
    def _():
        grad_other_ref[...] = other_total_ref[...].astype(BF16)


def attend_back(grad, grad_t, own_t, other_t, weights, ctx, query, keys, values):
    rows, width = grad.shape
    groups = weights.shape[1]
    whole = lambda g: (0, 0)
    by_group = lambda g: (g, 0, 0)
    block = pl.BlockSpec((weights.shape[0], 1) + weights.shape[2:], lambda g: (0, g, 0, 0))
    flops = groups * (3 * 2 * rows * width * 640 + 3 * 10 * rows * SLOT * 128)
    return pl.pallas_call(
        attend_back_kernel,
        name="attend_back",
        grid=(groups,),
        in_specs=[
            pl.BlockSpec((rows, width), whole),
            pl.BlockSpec((width, rows), whole),
            pl.BlockSpec((width, rows), whole),
            pl.BlockSpec((width, rows), whole),
            block,
            pl.BlockSpec((1, rows, 256), by_group),
            pl.BlockSpec((3, rows, 128), by_group),
            pl.BlockSpec((3, SLOT, 128), by_group),
            pl.BlockSpec((3, SLOT, 128), by_group),
        ],
        out_specs=[
            block,
            pl.BlockSpec((rows, width), whole),
            pl.BlockSpec((rows, width), whole),
            pl.BlockSpec((1, 1, 640), by_group),
        ],
        out_shape=[
            jax.ShapeDtypeStruct(weights.shape, BF16),
            jax.ShapeDtypeStruct((rows, width), F32),
            jax.ShapeDtypeStruct((rows, width), BF16),
            jax.ShapeDtypeStruct((groups, 1, 640), F32),
        ],
        scratch_shapes=[pltpu.VMEM((rows, width), F32)],
        cost_estimate=pl.CostEstimate(flops=4 * flops, bytes_accessed=32 << 20, transcendentals=12 * rows * SLOT),
        compiler_params=pltpu.CompilerParams(vmem_limit_bytes=63 << 20),
    )(grad, grad_t, own_t, other_t, weights, ctx, query, keys, values)


CORE, ALONG_X, ALONG_Y = 1, 2, 4
DIAGONAL = ALONG_X | ALONG_Y
COLUMNS = (0, ALONG_X, ALONG_Y, DIAGONAL)


def meet(me, z, depth):
    barrier = pltpu.get_barrier_semaphore()
    for bit in (CORE, ALONG_X, ALONG_Y):
        pl.semaphore_signal(barrier, inc=1, device_id=(me ^ bit, z), device_id_type=MESH)

    @pl.when(z > 0)
    def _():
        pl.semaphore_signal(barrier, inc=1, device_id=(me, z - 1), device_id_type=MESH)

    @pl.when(z < depth - 1)
    def _():
        pl.semaphore_signal(barrier, inc=1, device_id=(me, z + 1), device_id_type=MESH)

    pl.semaphore_wait(barrier, 3 + (z > 0).astype(jnp.int32) + (z < depth - 1).astype(jnp.int32))


def near_first(z, depth):
    yield z, None
    for distance in range(1, depth):
        for place in (z - distance, z + distance):
            yield place, (place >= 0) & (place < depth)


def near_at(z, depth, distance):
    for place in (z - distance, z + distance):
        yield place, (place >= 0) & (place < depth)


def given(condition, action):
    if condition is None:
        action()
    else:
        pl.when(condition)(action)


def halves(rows):
    return (rows // 2, rows) if rows % 32 == 0 else (rows, rows)


UP, DOWN, X, Y, VIA_Y, VIA_X, C0 = range(7)
GATHER_KINDS = C0 + 4


def gather_stages(depth, locals_, wholes, send_sem, recv_sem):
    me, z = lax.axis_index("dp"), lax.axis_index("mp")

    def copy(which, kind, place, source, target, to):
        return pltpu.make_async_remote_copy(
            src_ref=source,
            dst_ref=target,
            send_sem=send_sem.at[which, kind, place],
            recv_sem=recv_sem.at[which, kind, place],
            device_id=to,
            device_id_type=MESH,
        )

    def column(which, place, source, owner, kinds):
        whole = wholes[which]
        for kind, to, first, last in kinds:
            view = source if first == 0 and last == source.shape[0] else source.at[first:last]
            copy(which, kind, place, view, whole.at[owner, place, first:last], to).start()

    def arrived(which, kind, place, owner, first, last):
        view = wholes[which].at[owner, place, first:last]
        copy(which, kind, place, view, view, (me, z)).wait_recv()

    def first_stage(which, place, condition):
        rows = locals_[which].shape[0]

        def act():
            own = condition is None
            source = locals_[which] if own else wholes[which].at[me, place]
            if not own:
                pl.when(place < z)(lambda: arrived(which, UP, place, me, 0, rows))
                pl.when(place > z)(lambda: arrived(which, DOWN, place, me, 0, rows))
            up_from = (z < depth - 1) if own else (place < z) & (z < depth - 1)
            down_from = (z > 0) if own else (place > z) & (z > 0)
            pl.when(up_from)(lambda: column(which, place, source, me, [(UP, (me, z + 1), 0, rows)]))
            pl.when(down_from)(lambda: column(which, place, source, me, [(DOWN, (me, z - 1), 0, rows)]))
            column(
                which,
                place,
                source,
                me,
                [
                    (X, (me ^ ALONG_X, z), 0, rows),
                    (Y, (me ^ ALONG_Y, z), 0, rows),
                    (C0, (me ^ CORE, z), 0, rows),
                ],
            )

        given(condition, act)

    def second_stage(which, place, condition):
        rows = locals_[which].shape[0]
        half, _ = halves(rows)

        def act():
            arrived(which, X, place, me ^ ALONG_X, 0, rows)
            source = wholes[which].at[me ^ ALONG_X, place]
            column(
                which,
                place,
                source,
                me ^ ALONG_X,
                [(VIA_Y, (me ^ ALONG_Y, z), 0, half), (C0 + 1, (me ^ CORE, z), 0, rows)],
            )
            arrived(which, Y, place, me ^ ALONG_Y, 0, rows)
            source = wholes[which].at[me ^ ALONG_Y, place]
            kinds = [(C0 + 2, (me ^ CORE, z), 0, rows)]
            if half < rows:
                kinds = [(VIA_X, (me ^ ALONG_X, z), half, rows)] + kinds
            column(which, place, source, me ^ ALONG_Y, kinds)

        given(condition, act)

    def third_stage(which, place, condition):
        rows = locals_[which].shape[0]
        half, _ = halves(rows)

        def act():
            arrived(which, VIA_Y, place, me ^ DIAGONAL, 0, half)
            if half < rows:
                arrived(which, VIA_X, place, me ^ DIAGONAL, half, rows)
            source = wholes[which].at[me ^ DIAGONAL, place]
            column(which, place, source, me ^ DIAGONAL, [(C0 + 3, (me ^ CORE, z), 0, rows)])

        given(condition, act)

    def last_stage(which, place):
        rows = locals_[which].shape[0]
        for number, bit in enumerate(COLUMNS):
            arrived(which, C0 + number, place, me ^ CORE ^ bit, 0, rows)

    def begin(which):
        pltpu.make_async_copy(
            locals_[which], wholes[which].at[me, z], send_sem.at[which, GATHER_KINDS, 0]
        ).start()

    def finish(which):
        rows = locals_[which].shape[0]
        half, _ = halves(rows)
        for place in range(depth):
            last_stage(which, place)
        for place, condition in near_first(z, depth):

            def sent(place=place, own=condition is None):
                whole = wholes[which].at[me, place]
                pieces = [(X, 0, rows), (Y, 0, rows), (VIA_Y, 0, half)] + [(C0 + n, 0, rows) for n in range(4)]
                if half < rows:
                    pieces.append((VIA_X, half, rows))
                for kind, first, last in pieces:
                    view = whole.at[first:last]
                    copy(which, kind, place, view, view, (me, z)).wait_send()
                up_from = (z < depth - 1) if own else (place < z) & (z < depth - 1)
                down_from = (z > 0) if own else (place > z) & (z > 0)
                pl.when(up_from)(lambda: copy(which, UP, place, whole, whole, (me, z)).wait_send())
                pl.when(down_from)(lambda: copy(which, DOWN, place, whole, whole, (me, z)).wait_send())

            given(condition, sent)
        pltpu.make_async_copy(
            locals_[which], wholes[which].at[me, z], send_sem.at[which, GATHER_KINDS, 0]
        ).wait()

    return begin, first_stage, second_stage, third_stage, finish


def gather_kernel(count, depth, *refs):
    locals_, wholes = refs[:count], refs[count : 2 * count]
    me, z = lax.axis_index("dp"), lax.axis_index("mp")
    meet(me, z, depth)
    begin, first, second, third, finish = gather_stages(depth, locals_, wholes, *refs[2 * count :])
    order = []
    for which in range(count):
        begin(which)
        order += [(which,) + item for item in near_first(z, depth)]
    lag = len(order) // count
    for step in range(len(order) + 2 * lag):
        if step < len(order):
            first(*order[step])
        if 0 <= step - lag < len(order):
            second(*order[step - lag])
        if 0 <= step - 2 * lag:
            third(*order[step - 2 * lag])
    for which in range(count):
        finish(which)


FIRST_AT = {1: [(0, 1)], 2: [(1, 1)], 3: [(0, 2)], 4: [(1, 2)], 5: [(0, 3)], 6: [(1, 3)]}
SECOND_AT = {2: [(0, 0)], 3: [(1, 0)], 5: [(0, 1)], 8: [(1, 1)], 9: [(0, 2)], 10: [(1, 2), (0, 3)], 11: [(1, 3)]}
THIRD_AT = {6: [(0, 0)], 7: [(1, 0)], 9: [(0, 1)], 11: [(1, 1)], 12: [(0, 2), (1, 2), (0, 3), (1, 3)]}


def linked_attend_kernel(
    depth,
    valid_ref,
    own_ref,
    other_ref,
    qv_bias_ref,
    out_bias_ref,
    w1_ref,
    w2_ref,
    w_hbm,
    pre_ref,
    ctx_ref,
    q_ref,
    k_ref,
    v_ref,
    w1_out,
    w2_out,
    w_buf,
    w_sem,
    send_sem,
    recv_sem,
):
    me, z = lax.axis_index("dp"), lax.axis_index("mp")
    step = pl.program_id(0)
    group = z ^ step
    part, width = w_buf.shape[2:]

    def load_w(s):
        return pltpu.make_async_copy(w_hbm.at[:, z ^ s], w_buf.at[s], w_sem.at[s])

    begin, first, second, third, finish = gather_stages(depth, (w1_ref, w2_ref), (w1_out, w2_out), send_sem, recv_sem)

    def around(stage, which, distance):
        for place, condition in near_first(z, depth) if distance == 0 else near_at(z, depth, distance):
            if distance == 0 and condition is not None:
                break
            stage(which, place, condition)

    def do(slot):
        for stage, plan in ((first, FIRST_AT), (second, SECOND_AT), (third, THIRD_AT)):
            for which, distance in plan.get(slot, ()):
                around(stage, which, distance)

    @pl.when(step == 0)
    def _():
        for s in range(depth):
            load_w(s).start()
        meet(me, z, depth)
        for which in range(2):
            begin(which)
            around(first, which, 0)

    for s in range(depth):
        pl.when(step == s)(lambda s=s: load_w(s).wait())

    def after_head(head):
        for s in range(depth):
            pl.when(step == s)(lambda s=s: do(3 * s + head))

    part_sum = attend_group(
        qv_bias_ref[group],
        lambda low, high: w_buf[step, :, :, low:high].reshape(8 * part, high - low),
        valid_ref,
        own_ref,
        other_ref,
        ctx_ref,
        q_ref,
        k_ref,
        v_ref,
        after_head,
    )

    @pl.when(step == 0)
    def _():
        pre_ref[...] = part_sum + (out_bias_ref[...] + own_ref[...].astype(F32))

    @pl.when(step > 0)
    def _():
        pre_ref[...] += part_sum

    @pl.when(step == depth - 1)
    def _():
        do(3 * depth)
        for which in range(2):
            finish(which)


def linked_attend(valid, own, other, weights, qv_bias, out_bias, w1, w2):
    rows, width = own.shape
    n_dp, groups, part = weights.shape[:3]
    whole = pl.BlockSpec(memory_space=pltpu.VMEM)
    anywhere = pl.BlockSpec(memory_space=pl.ANY)
    by_group = lambda g: (g, 0, 0)
    flops = groups * (2 * 2 * rows * width * 640 + 3 * 4 * rows * SLOT * 128)
    sems = pltpu.SemaphoreType.DMA((2, GATHER_KINDS + 1, groups))
    return pl.pallas_call(
        functools.partial(linked_attend_kernel, groups),
        name="linked_attend",
        grid=(groups,),
        in_specs=[pl.BlockSpec(memory_space=pltpu.SMEM)] + [whole] * 6 + [anywhere],
        out_specs=[
            whole,
            pl.BlockSpec((1, rows, 256), by_group),
            pl.BlockSpec((3, rows, 128), by_group),
            pl.BlockSpec((3, SLOT, 128), by_group),
            pl.BlockSpec((3, SLOT, 128), by_group),
            anywhere,
            anywhere,
        ],
        out_shape=[
            jax.ShapeDtypeStruct((rows, width), F32),
            jax.ShapeDtypeStruct((groups, rows, 256), BF16),
            jax.ShapeDtypeStruct((3 * groups, rows, 128), BF16),
            jax.ShapeDtypeStruct((3 * groups, SLOT, 128), BF16),
            jax.ShapeDtypeStruct((3 * groups, SLOT, 128), BF16),
            jax.ShapeDtypeStruct((n_dp, groups) + w1.shape, BF16),
            jax.ShapeDtypeStruct((n_dp, groups) + w2.shape, BF16),
        ],
        scratch_shapes=[
            pltpu.VMEM((groups, n_dp, part, width), BF16),
            pltpu.SemaphoreType.DMA((groups,)),
            sems,
            sems,
        ],
        cost_estimate=pl.CostEstimate(flops=4 * flops, bytes_accessed=36 << 20, transcendentals=12 * rows * SLOT),
        compiler_params=pltpu.CompilerParams(collective_id=3, has_side_effects=True, vmem_limit_bytes=60 << 20),
    )(valid, own, other, qv_bias, out_bias, w1, w2, weights)


def gather_all(locals_, n_dp, n_mp, number):
    count = len(locals_)
    sems = pltpu.SemaphoreType.DMA((count, GATHER_KINDS + 1, n_mp))
    return pl.pallas_call(
        functools.partial(gather_kernel, count, n_mp),
        name="gather",
        in_specs=[pl.BlockSpec(memory_space=pltpu.VMEM)] * count,
        out_specs=[pl.BlockSpec(memory_space=pl.ANY)] * count,
        out_shape=[jax.ShapeDtypeStruct((n_dp, n_mp) + a.shape, a.dtype) for a in locals_],
        scratch_shapes=[sems, sems],
        compiler_params=pltpu.CompilerParams(collective_id=number, has_side_effects=True),
    )(*locals_)


TO_X, TO_Y, X_LOW, X_HIGH, Y_LOW, Y_HIGH, Z_UP, Z_DOWN, S0 = range(9)
SCATTER_KINDS = S0 + 4


class Reduction:
    def __init__(self, which, me, z, depth, rows, bufs, send_sem, recv_sem):
        self.which, self.me, self.z, self.depth, self.rows = which, me, z, depth, rows
        self.half = halves(rows)[0]
        self.core, self.diagonal, self.sides, self.line = bufs
        self.send_sem, self.recv_sem = send_sem, recv_sem

    def copy(self, kind, place, source, target, to):
        return pltpu.make_async_remote_copy(
            src_ref=source,
            dst_ref=target,
            send_sem=self.send_sem.at[self.which, kind, place],
            recv_sem=self.recv_sem.at[self.which, kind, place],
            device_id=to,
            device_id_type=MESH,
        )

    def start(self, kind, place, source, target, bit):
        self.copy(kind, place, source, target, (self.me ^ bit, self.z)).start()

    def wait(self, kind, place, view):
        self.copy(kind, place, view, view, (self.me, self.z)).wait_recv()

    def add(self, target, *others):
        total = target[...].astype(F32)
        for other in others:
            total = total + other[...].astype(F32)
        target[...] = total.astype(target.dtype)

    def to_core(self, place, theirs, numbers=(3, 1, 2, 0)):
        for number in numbers:
            self.start(S0 + number, place, theirs(number), self.core.at[number, place], CORE)

    def first(self, place, mine):
        half, rows = self.half, self.rows
        for number in (3, 1, 2):
            view = self.core.at[number, place]
            self.wait(S0 + number, place, view)
            self.add(view, mine(number))
            if number == 3:
                self.start(TO_X, place, view.at[0:half], self.diagonal.at[place, 0:half], ALONG_X)
                if half < rows:
                    self.start(TO_Y, place, view.at[half:rows], self.diagonal.at[place, half:rows], ALONG_Y)
            if number == 1:
                self.start(X_LOW, place, view.at[0:half], self.sides.at[0, place, 0:half], ALONG_X)
            if number == 2 and half < rows:
                self.start(Y_HIGH, place, view.at[half:rows], self.sides.at[1, place, half:rows], ALONG_Y)

    def second(self, place):
        half, rows = self.half, self.rows
        view = self.diagonal.at[place, 0:half]
        self.wait(TO_X, place, view)
        mine = self.core.at[2, place, 0:half]
        self.add(mine, view)
        self.start(Y_LOW, place, mine, self.sides.at[1, place, 0:half], ALONG_Y)
        if half < rows:
            view = self.diagonal.at[place, half:rows]
            self.wait(TO_Y, place, view)
            mine = self.core.at[1, place, half:rows]
            self.add(mine, view)
            self.start(X_HIGH, place, mine, self.sides.at[0, place, half:rows], ALONG_X)

    def third(self, place, mine):
        half, rows = self.half, self.rows
        self.wait(S0, place, self.core.at[0, place])
        self.wait(X_LOW, place, self.sides.at[0, place, 0:half])
        self.wait(Y_LOW, place, self.sides.at[1, place, 0:half])
        if half < rows:
            self.wait(Y_HIGH, place, self.sides.at[1, place, half:rows])
            self.wait(X_HIGH, place, self.sides.at[0, place, half:rows])
        self.add(self.core.at[0, place], mine(0), self.sides.at[0, place], self.sides.at[1, place])

    def along(self, kind, place):
        way = 0 if kind == Z_UP else 1
        to = (self.me, self.z + 1 if kind == Z_UP else self.z - 1)
        return self.copy(kind, place, self.core.at[0, place], self.line.at[way, place], to)

    def hop(self, place, number):
        for kind, here in ((Z_UP, number), (Z_DOWN, self.depth - 1 - number)):
            if (here < place) if kind == Z_UP else (here > place):

                @pl.when(self.z == here)
                def _(kind=kind):
                    if number > 0:
                        view = self.line.at[0 if kind == Z_UP else 1, place]
                        self.wait(kind, place, view)
                        self.add(self.core.at[0, place], view)
                    self.along(kind, place).start()

    def chain(self, distance):
        z, depth = self.z, self.depth
        above, below = z + distance, z - distance

        @pl.when(above < depth)
        def _():
            @pl.when(z > 0)
            def _():
                self.wait(Z_UP, above, self.line.at[0, above])
                self.add(self.core.at[0, above], self.line.at[0, above])

            self.along(Z_UP, above).start()

        @pl.when(below >= 0)
        def _():
            @pl.when(z < depth - 1)
            def _():
                self.wait(Z_DOWN, below, self.line.at[1, below])
                self.add(self.core.at[0, below], self.line.at[1, below])

            self.along(Z_DOWN, below).start()

    def finish(self, out):
        z, depth = self.z, self.depth
        out[...] = self.core[0, z].astype(F32)

        @pl.when(z > 0)
        def _():
            self.wait(Z_UP, z, self.line.at[0, z])
            out[...] += self.line[0, z].astype(F32)

        @pl.when(z < depth - 1)
        def _():
            self.wait(Z_DOWN, z, self.line.at[1, z])
            out[...] += self.line[1, z].astype(F32)

    def drain(self):
        half, rows = self.half, self.rows
        pieces = [(S0 + number, 0, rows) for number in range(4)]
        pieces += [(TO_X, 0, half), (X_LOW, 0, half), (Y_LOW, 0, half)]
        if half < rows:
            pieces += [(TO_Y, half, rows), (Y_HIGH, half, rows), (X_HIGH, half, rows)]
        for place in range(self.depth):
            for kind, first, last in pieces:
                view = self.core.at[0, place, first:last]
                self.copy(kind, place, view, view, (self.me, self.z)).wait_send()
        for distance in range(1, self.depth):
            above, below = self.z + distance, self.z - distance
            pl.when(above < self.depth)(lambda above=above: self.along(Z_UP, above).wait_send())
            pl.when(below >= 0)(lambda below=below: self.along(Z_DOWN, below).wait_send())


def linked_back_kernel(
    depth,
    grad_ref,
    grad_t_ref,
    own_t_ref,
    other_t_ref,
    early_ref,
    w_hbm,
    ff_hbm,
    ctx_ref,
    q_ref,
    k_ref,
    v_ref,
    ff_out,
    w_out,
    small_out,
    grad_own_ref,
    w_buf,
    w_sem,
    grad_w,
    grad_small,
    ff_mine,
    ff_sem,
    ff_own,
    ff_own_sem,
    grad_heads,
    grad_queries,
    others,
    other_total,
    sent,
    received,
    pair_send,
    pair_recv,
    *refs,
):
    send_sem, recv_sem = refs[-2:]
    me, z = lax.axis_index("dp"), lax.axis_index("mp")
    step = pl.program_id(0)
    turn = lax.rem(step, depth)
    rows = grad_ref.shape[0]
    part = w_buf.shape[2]
    width = 8 * part
    group_at = lambda s: z ^ (depth - 1 - s)
    group = group_at(turn)
    arrays = [(2 * part, refs[0:4]), (part, refs[4:8]), (8, refs[8:12])]
    ff, w, small = [
        Reduction(i, me, z, depth, size, bufs, send_sem, recv_sem) for i, (size, bufs) in enumerate(arrays)
    ]
    places = [depth - 1, 0] + list(range(1, depth - 1))[::-1]
    lane = lanes((rows, 128))

    def load_w(s):
        return pltpu.make_async_copy(w_hbm.at[:, group_at(s)], w_buf.at[group_at(s)], w_sem.at[s])

    def load_ff(number, column):
        source = ff_hbm.at[me ^ COLUMNS[column], places[number]]
        return pltpu.make_async_copy(source, ff_mine.at[number % 2, column - 1], ff_sem.at[number % 2, column - 1])

    def load_ff_own(place):
        return pltpu.make_async_copy(ff_hbm.at[me, place], ff_own.at[place], ff_own_sem.at[place])

    exchange = pltpu.make_async_remote_copy(
        src_ref=sent,
        dst_ref=received,
        send_sem=pair_send,
        recv_sem=pair_recv,
        device_id=(me, z ^ 1),
        device_id_type=MESH,
    )

    @pl.when(step == 0)
    def _():
        for s in range(depth):
            load_w(s).start()
        for number in range(2):
            for column in (3, 1, 2):
                load_ff(number, column).start()
        meet(me, z, depth)
        theirs = lambda place: lambda column: ff_hbm.at[me ^ CORE ^ COLUMNS[column], place]
        for place in places:
            ff.to_core(place, theirs(place), (3, 1, 2))
        for place in places:
            ff.to_core(place, theirs(place), (0,))
            load_ff_own(place).start()

    for s in range(depth):
        pl.when(step == s)(lambda s=s: load_w(s).wait())

    def ff_first(number):
        for column in (3, 1, 2):
            load_ff(number, column).wait()
        ff.first(places[number], lambda column: ff_mine.at[number % 2, column - 1])
        if number + 2 < depth:
            for column in (3, 1, 2):
                load_ff(number + 2, column).start()

    def ff_third(number):
        place = places[number]
        load_ff_own(place).wait()
        ff.third(place, lambda column: ff_own.at[place])

    work = {}

    def plan(slot, action, *arguments):
        work.setdefault(slot, []).append((action, arguments))

    end = 6 * depth
    for number, slots in enumerate(((1, 5, 9), (2, 8, 13), (4, 12, 17), (5, 15, 20))):
        plan(slots[0], ff_first, number)
        plan(slots[1], ff.second, places[number])
        plan(slots[2], ff_third, number)
        for hop in range(depth - 1):
            plan(min(slots[2] + 4 * hop, end + (number == 3) * (hop - 1)), ff.hop, places[number], hop)

    def do(slot):
        for action, arguments in work.get(slot, ()):
            action(*arguments)

    def w_first(s):
        place = group_at(s)
        w.first(place, lambda column: grad_w.at[s, me ^ COLUMNS[column]])
        small.first(place, lambda column: grad_small.at[s, me ^ COLUMNS[column]])

    def w_second(s):
        w.second(group_at(s))
        small.second(group_at(s))

    def w_third(s):
        place = group_at(s)
        w.third(place, lambda column: grad_w.at[s, me ^ COLUMNS[column]])
        small.third(place, lambda column: grad_small.at[s, me ^ COLUMNS[column]])

    def w_chain(distance):
        w.chain(distance)
        small.chain(distance)

    def after_head(head):
        for s in range(2 * depth):
            if 3 * s + head in work:
                pl.when(step == s)(lambda slot=3 * s + head: do(slot))
        pl.when(step > depth)(lambda: (w_first, w_second, w_third)[head](step - depth - 1))
        if head == 2:
            for s in range(depth - 1):
                pl.when(step == depth + 1 + s)(lambda s=s: w_chain(depth - 1 - s))

    def weight_of(first, last):
        return w_buf[group, :, :, first:last].reshape(width, last - first)

    @pl.when(step < depth)
    def _():
        grad_context = mul(grad_ref[...], weight_of(512, 768)).astype(BF16).astype(F32)
        for head in range(3):
            grad_head = head_block(grad_context, 1 + head)
            context = head_block(ctx_ref[0].astype(F32), 1 + head)
            delta = jnp.sum(jnp.where(lane < HEAD, grad_head * context, 0.0), axis=1, keepdims=True)
            high, middle, low = three_parts(-delta)
            tail = jnp.where(
                lane == HEAD, high, jnp.where(lane == HEAD + 1, middle, jnp.where(lane == HEAD + 2, low, 0.0))
            )
            grad_heads[turn, head] = jnp.where(lane < HEAD, grad_head, tail).astype(BF16)

    grads = []
    chunk = 256
    for head in range(3):
        keys_t = k_ref[head].T
        grad_query = []
        grad_keys = grad_values = None
        for first in range(0, rows, chunk):
            query_here = q_ref[head, first : first + chunk, :]
            grad_here = grad_heads[turn, head, first : first + chunk, :]
            weights = jnp.exp(mul(k_ref[head], query_here, NT))
            grad_scores = (weights * mul(v_ref[head], grad_here, NT)).astype(BF16)
            values_part = mul(weights.astype(BF16), grad_here)
            keys_part = mul(grad_scores, query_here)
            grad_values = values_part if grad_values is None else grad_values + values_part
            grad_keys = keys_part if grad_keys is None else grad_keys + keys_part
            grad_query.append(mul(keys_t, grad_scores))
        grads.append((jnp.concatenate(grad_query, axis=1).T * SCALE, grad_keys, grad_values))
        after_head(head)
    (q0, k0, v0), (q1, k1, v1), (q2, k2, v2) = grads
    blank = jnp.zeros((rows, 128), F32)
    k12, v01 = pair(k1, k2), pair(v0, v1)

    @pl.when(step < depth)
    def _():
        grad_queries[turn, :, 0:128] = pair(q0, q1)
        grad_queries[turn, :, 128:256] = q2
        other = jnp.concatenate([pair(blank, k0), k12, v01, pair(v2, blank)], axis=1).astype(BF16)
        others[turn] = other
        other_part = mul(other, weight_of(128, 640), NT)

        @pl.when(step == 0)
        def _():
            other_total[...] = other_part

        @pl.when(step > 0)
        def _():
            other_total[...] += other_part

        @pl.when(step == depth - 1)
        def _():
            sent[...] = other_total[...].astype(BF16)
            exchange.start()

    @pl.when(step >= depth)
    def _():
        q01 = pair(q0, q1) + grad_queries[turn, :, 0:128]
        q2_all = q2 + grad_queries[turn, :, 128:256]
        own = jnp.concatenate([q01, pair(q2_all, k0), k12, v01, pair(v2, blank)], axis=1)
        other = others[turn]
        own_sum = jnp.sum(own, axis=0, keepdims=True)
        other_sum = jnp.sum(other.astype(F32), axis=0, keepdims=True)
        row = lax.broadcasted_iota(jnp.int32, (8, 128), 0)
        late = jnp.where(row == 0, own_sum[:, 0:128], 0.0)
        for number in range(1, 5):
            piece = own_sum[:, 128 * number : 128 * number + 128] + other_sum[:, 128 * number - 128 : 128 * number]
            late = jnp.where(row == number, piece, late)
        for owner in range(8):
            grad_small[turn, owner] = early_ref[owner, group] + late
        own = own.astype(BF16)
        first = 0
        for piece in weight_grads(grad_t_ref, own_t_ref, other_t_ref, ctx_ref, own, other):
            last = first + piece.shape[1]
            grad_w[turn, :, :, first:last] = piece.astype(BF16).reshape(8, part, last - first)
            first = last
        w.to_core(group, lambda column: grad_w.at[turn, me ^ CORE ^ COLUMNS[column]])
        small.to_core(group, lambda column: grad_small.at[turn, me ^ CORE ^ COLUMNS[column]])
        own_part = mul(own, weight_of(0, 640), NT)

        @pl.when(step == depth)
        def _():
            grad_own_ref[...] = own_part

        @pl.when(step > depth)
        def _():
            grad_own_ref[...] += own_part

    @pl.when(step == 2 * depth - 1)
    def _():
        w_first(depth - 1)
        do(end)
        exchange.wait_recv()
        grad_own_ref[...] += received[...].astype(F32)
        w_second(depth - 1)
        do(end + 1)
        w_third(depth - 1)
        ff.finish(ff_out)
        w.finish(w_out)
        small.finish(small_out)
        for array in (ff, w, small):
            array.drain()
        exchange.wait_send()


def linked_back(grad, grad_t, own_t, other_t, early, weights, grad_ff, ctx, query, keys, values):
    rows, width = grad.shape
    n_dp, groups, part = weights.shape[:3]
    whole = pl.BlockSpec(memory_space=pltpu.VMEM)
    anywhere = pl.BlockSpec(memory_space=pl.ANY)
    by_group = lambda g: (groups - 1 - lax.rem(g, groups), 0, 0)
    by_half = lambda g: (groups - 1 - lax.rem(g, groups), 1 - g // groups, 0)
    flops = groups * (3 * 2 * rows * width * 640 + 3 * 10 * rows * SLOT * 128)
    scratch = []
    for size, columns, kind in ((2 * part, width, BF16), (part, width, BF16), (8, 128, F32)):
        block = (size, columns)
        scratch += [
            pltpu.VMEM((4, groups) + block, kind),
            pltpu.VMEM((groups,) + block, kind),
            pltpu.VMEM((2, groups) + block, kind),
            pltpu.VMEM((2, groups) + block, kind),
        ]
    sems = pltpu.SemaphoreType.DMA((3, SCATTER_KINDS, groups))
    return pl.pallas_call(
        functools.partial(linked_back_kernel, groups),
        name="linked_back",
        grid=(2 * groups,),
        in_specs=[whole] * 5
        + [anywhere] * 2
        + [
            pl.BlockSpec((1, rows, 256), by_group),
            pl.BlockSpec((3, rows, 128), by_group),
            pl.BlockSpec((3, rows, 128), by_half),
            pl.BlockSpec((3, rows, 128), by_half),
        ],
        out_specs=[whole] * 4,
        out_shape=[
            jax.ShapeDtypeStruct((2 * part, width), F32),
            jax.ShapeDtypeStruct((part, width), F32),
            jax.ShapeDtypeStruct((8, 128), F32),
            jax.ShapeDtypeStruct((rows, width), F32),
        ],
        scratch_shapes=[
            pltpu.VMEM((groups, n_dp, part, width), BF16),
            pltpu.SemaphoreType.DMA((groups,)),
            pltpu.VMEM((groups, n_dp, part, width), BF16),
            pltpu.VMEM((groups, n_dp, 8, 128), F32),
            pltpu.VMEM((2, 3, 2 * part, width), BF16),
            pltpu.SemaphoreType.DMA((2, 3)),
            pltpu.VMEM((groups, 2 * part, width), BF16),
            pltpu.SemaphoreType.DMA((groups,)),
            pltpu.VMEM((groups, 3, rows, 128), BF16),
            pltpu.VMEM((groups, rows, 256), F32),
            pltpu.VMEM((groups, rows, 512), BF16),
            pltpu.VMEM((rows, width), F32),
            pltpu.VMEM((rows, width), BF16),
            pltpu.VMEM((rows, width), BF16),
            pltpu.SemaphoreType.DMA,
            pltpu.SemaphoreType.DMA,
        ]
        + scratch
        + [sems, sems],
        cost_estimate=pl.CostEstimate(flops=4 * flops, bytes_accessed=48 << 20, transcendentals=12 * rows * SLOT),
        compiler_params=pltpu.CompilerParams(
            collective_id=2, has_side_effects=True, vmem_limit_bytes=67043328
        ),
    )(grad, grad_t, own_t, other_t, early, weights, grad_ff, ctx, query, keys, values)


def blocks(local, mesh_shape):
    return lax.all_gather(local, BOTH, axis=0, tiled=False).reshape(mesh_shape + local.shape)


def gather_first(locals_, mesh_shape):
    if mesh_shape[0] == 8:
        return gather_all(locals_, *mesh_shape, number=1)
    return [blocks(local, mesh_shape) for local in locals_]


def scatter_sums(partial):
    flat = partial.reshape((-1,) + partial.shape[3:])
    return lax.psum_scatter(flat, BOTH, scatter_dimension=0, tiled=True).astype(F32)


def body(
    frames,
    w_qkv,
    b_qv,
    w_out,
    b_out,
    ln1_gain,
    ln1_bias,
    w_ff1,
    b_ff1,
    w_ff2,
    b_ff2,
    ln2_gain,
    ln2_bias,
    cotangent,
    clip_lengths,
    clip_slot,
):
    n_dp, n_mp = lax.axis_size("dp"), lax.axis_size("mp")
    rows, width = frames.shape
    share = b_out.shape[0]

    partner = [(m, m ^ 1) for m in range(n_mp)]
    other = lax.ppermute(frames, "mp", partner)
    packed = jnp.concatenate([w_qkv[0], w_qkv[1], w_qkv[2], w_out.T], axis=1)
    small = jnp.concatenate(
        [b_out, ln1_gain, ln1_bias, b_ff2, ln2_gain, ln2_bias, b_qv.reshape(-1).astype(F32), b_ff1.astype(F32)]
    )
    entries = small.shape[0]
    small = jnp.pad(small, (0, -entries % 1024)).reshape(-1, 128)
    mesh_shape = (n_dp, n_mp)
    w_attn, small = gather_first([packed, small], mesh_shape)
    small = small.reshape(n_dp * n_mp, -1)[:, :entries]
    vectors = small[:, : 6 * share].reshape(n_dp * n_mp, 6, share).transpose(1, 0, 2).reshape(6, width)
    vectors = jnp.concatenate([vectors, jnp.zeros((2, width), F32)])
    ordered = small.reshape(n_dp, n_mp, -1).transpose(1, 0, 2)
    qv = ordered[:, :, 6 * share : 8 * share].reshape(n_mp, n_dp, 2, share).transpose(0, 2, 1, 3)
    qv = qv.reshape(n_mp, 2, 1, n_dp * share)
    heads_width = n_dp * share
    qv_bias = jnp.concatenate(
        [qv[:, 0], jnp.zeros((n_mp, 1, heads_width), F32), qv[:, 1], jnp.zeros((n_mp, 1, HEAD), F32)], axis=2
    )
    up_bias = ordered[:, :, 8 * share :].reshape(n_mp, 1, -1)

    index = lax.axis_index("dp") * n_mp + lax.axis_index("mp")
    slot = index // (SLOT // rows)
    half = index % (SLOT // rows)
    length = jnp.sum(jnp.where(clip_slot == slot, clip_lengths, 0))
    valid = jnp.stack([length - half * rows, length - (1 - half) * rows]).astype(jnp.int32)

    linked = n_dp == 8
    if linked:
        pre_one, ctx, query, keys, values, w1, w2 = linked_attend(
            valid, frames, other, w_attn, qv_bias, vectors[0:1], w_ff1, w_ff2.T
        )
    else:
        w1, w2 = blocks(w_ff1, mesh_shape), blocks(w_ff2.T, mesh_shape)
        order = jnp.arange(n_mp, dtype=jnp.int32)
        pre_one, ctx, query, keys, values = attend(order, valid, frames, other, w_attn, qv_bias, vectors[0:1])
    hidden, active, low, low_t = up(pre_one, vectors[1:2], vectors[2:3], w1, up_bias)
    output, grad_pre, grad_low, grad_low_t, grad_ff, sums, grad_up_bias = down(
        pre_one, cotangent, vectors, active, hidden, w2, w1, low_t
    )
    sums = sums[:6].reshape(6, n_dp * n_mp, share).transpose(1, 0, 2).reshape(n_dp * n_mp, 6 * share)
    unit_sums = grad_up_bias.reshape(n_mp, n_dp, -1).transpose(1, 0, 2).reshape(n_dp * n_mp, -1)
    early = jnp.concatenate([sums, unit_sums], axis=1)
    entries = early.shape[1]
    early = jnp.pad(early, ((0, 0), (0, -entries % 128))).reshape(mesh_shape + (-1, 128))
    early = jnp.pad(early, ((0, 0), (0, 0), (5, 3 - early.shape[2]), (0, 0)))
    kept = (ctx, query, keys, values)
    if linked:
        done_ff, done_w, small, grad_own = linked_back(
            grad_low, grad_low_t, frames.T, other.T, early, w_attn, grad_ff, *kept
        )
        grad_input = grad_pre + grad_own
    else:
        grad_w, grad_own, grad_other, head_sums = attend_back(
            grad_low, grad_low_t, frames.T, other.T, w_attn, *kept
        )
        grad_input = grad_pre + grad_own + lax.ppermute(grad_other, "mp", partner).astype(F32)
        done_ff, done_w = scatter_sums(grad_ff), scatter_sums(grad_w)
        small = scatter_sums(early + jnp.pad(head_sums.reshape(1, n_mp, 5, 128), ((0, 0), (0, 0), (0, 3), (0, 0))))
    part = w_ff1.shape[0]
    small = small.reshape(-1)
    (d_out_bias, d_gain1, d_shift1, d_down_bias, d_gain2, d_shift2) = [
        small[640 + i * share : 640 + (i + 1) * share] for i in range(6)
    ]
    d_up_bias = small[640 + 6 * share : 640 + entries]
    d_qv = jnp.stack(
        [
            lax.dynamic_slice(small, (first + lax.axis_index("dp") * share,), (share,))
            for first in (0, 2 * heads_width)
        ]
    )
    d_qkv = jnp.stack([done_w[:, i * heads_width : (i + 1) * heads_width] for i in range(3)])
    done_w1, done_w2 = done_ff[:part], done_ff[part:]
    return (
        output,
        grad_input,
        d_qkv,
        d_qv,
        done_w[:, 3 * heads_width :].T,
        d_out_bias,
        d_gain1,
        d_shift1,
        done_w1,
        d_up_bias,
        done_w2.T,
        d_down_bias,
        d_gain2,
        d_shift2,
    )


def solution(mesh):
    rows, vector, group_vector = P(BOTH, None), P(BOTH), P(("mp", "dp"))
    qkv, qv, out, up_spec = P(None, "dp", "mp"), P(None, ("mp", "dp")), P("mp", "dp"), P("dp", "mp")
    weights = (qkv, qv, out, vector, vector, vector, up_spec, group_vector, out, vector, vector, vector)
    return jax.shard_map(
        body,
        mesh=mesh,
        in_specs=(rows,) + weights + (rows, P(), P()),
        out_specs=(rows, rows) + weights,
        check_vma=False,
    )
```
